256 devices in a mesh: dir: 2 (over x_hi), slab: 64 (over y, x_lo, z), tile: 2 (over core).
Axes of the slice: x: 4 (x_hi: 2, x_lo: 2; x = x_hi * 2 + x_lo), y: 4, z: 8, core: 2. Of those that a mesh axis runs over, the one named last changes fastest.
Arguments:
- voxels: float32 [4, 512, 64, 512], P(None, 'slab', 'tile'), may hold values from -2.5 to 2.5
- offsets: int32 [2, 64, 512], P('dir', 'tile'), may hold values from 0 to 511
- heading: int32 [2, 64, 512], P('dir', 'tile'), may hold values from 0 to 1
- cotangent: float32 [2, 3, 64, 512], P('dir', None, 'tile'), may hold values from -6 to 6
Outputs:
- image: float32 [2, 3, 64, 512], P('dir', None, 'tile', 'slab')
- voxel_grad: float32 [4, 512, 64, 512], P(None, 'slab', 'tile', 'dir')
The draws below stay inside these ranges and needn't reach their ends.
Inputs may be any that keep to these rules, and one draw needn't show every extreme that they name: `offsets`: A code packs three sub-cell positions as p + 8 * m + 8 * 8 * n (p along depth, m along rows, n along columns).
All inputs are finite; a program needn't handle non-finite values.
Results may differ from the reference program's by a relative error of at most 0.0003.
Values sent between devices are 32-bit elements; how exact they have to be, the bound alone decides.
A program may use at most 64 MiB of HBM per device.

```python
import jax
import jax.numpy as jnp
from jax import lax

CHANNELS = 4
LEVELS = 8
NX = 512
GROUPS = 2
NZ = 512
NY = 64


def with_ends(drawn, stream_key, smallest, high):
    longest = drawn.shape.index(max(drawn.shape))
    spots = []
    for shift in (0, 1):
        where = [jax.random.randint(jax.random.fold_in(stream_key, axis), (), 0, length) for axis, length in enumerate(drawn.shape)]
        where[longest] = (where[longest] + shift) % drawn.shape[longest]
        spots.append(tuple(where))
    return drawn.at[spots[0]].set(smallest).at[spots[1]].set(high)


def level_of(key, shape, cuts, least, top_value):
    level = 1.0
    for dim, shards_of in cuts:
        steps = jax.random.uniform(jax.random.fold_in(jax.random.fold_in(key, 6), dim), (shards_of,), jnp.float32, least / len(cuts), top_value / len(cuts))
        level = level * jnp.repeat(jnp.exp(steps), shape[dim] // shards_of).reshape((-1,) + (1,) * (len(shape) - 1 - dim))
    return level


def bell_draw(rng, extent, width, bound, cuts=(), kind=jnp.bfloat16):
    loudness = level_of(rng, extent, cuts, -0.22, 0.18) if cuts else 1.0
    entries = jax.random.normal(rng, extent, jnp.float32) * width * loudness
    return jnp.minimum(jnp.maximum(entries, -bound), bound).astype(kind)


def setup_inputs(seed: int = 0) -> dict:
    seeds = jax.random.split(jax.random.key(seed), 5)
    return {
        "voxels": jnp.clip(jax.random.uniform(seeds[0], (CHANNELS, NZ, NY, NX), jnp.float32, -2.5, 2.5) * level_of(seeds[0], (CHANNELS, NZ, NY, NX), ((1, 64), (2, 2)), -0.4, 0.0), -2.5, 2.5),
        "offsets": with_ends(jax.random.randint(seeds[1], (GROUPS, NY, NX), 0, LEVELS * LEVELS * LEVELS), jax.random.fold_in(seeds[1], 1), 0, (LEVELS * LEVELS * LEVELS) - 1).astype(jnp.int32),
        "heading": with_ends(jax.random.randint(seeds[2], (GROUPS, NY, NX), 0, 2), jax.random.fold_in(seeds[2], 1), 0, 1).astype(jnp.int32),
        "cotangent": bell_draw(seeds[3], (GROUPS, 3, NY, NX), 1.0, 6.0, ((0, 2), (2, 2)), jnp.float32),
    }


def tap_weights(codes):
    level = LEVELS
    fz = (codes % level).astype(jnp.float32)
    fy = (codes // level % level).astype(jnp.float32)
    fx = (codes // (level * level)).astype(jnp.float32)

    def three(raw):
        f = (raw + 0.5) / level - 0.5
        return (jnp.maximum(-f, 0.0), 1.0 - jnp.abs(f), jnp.maximum(f, 0.0))
    return (three(fz), three(fy), three(fx))

def sample(vox, weights):
    wz, wy, wx = weights
    depth, rows, cols = (vox.shape[1], vox.shape[2], vox.shape[3])
    padded = jnp.pad(vox, ((0, 0), (1, 1), (1, 1), (1, 1)))
    plane = None
    for b in range(3):
        for e in range(3):
            term = wy[b] * wx[e] * padded[:, :, b:b + rows, e:e + cols]
            plane = term if plane is None else plane + term
    values = None
    for a in range(3):
        term = wz[a] * plane[:, a:a + depth]
        values = term if values is None else values + term
    return values

def render(vox, weights, head):
    values = sample(vox, weights)
    scale = 2.0 / NZ
    sigma = jax.nn.softplus(values[0]) * scale
    colour = jax.nn.sigmoid(values[1:])
    alpha = 1.0 - jnp.exp(-sigma)
    ahead = jnp.cumsum(sigma, axis=0) - sigma
    total = lax.optimization_barrier(jnp.sum(sigma, axis=0))
    front = jnp.where(head == 0, ahead, total - ahead - sigma)
    return lax.optimization_barrier(jnp.sum(jnp.exp(-front) * alpha * colour, axis=1))

def reference(voxels, offsets, heading, cotangent):

    def one(carry, items):
        codes, head, cot = items
        weights = tap_weights(codes)
        image, pull = jax.vjp(lambda grid: render(grid, weights, head), voxels)
        grad, = pull(cot * NZ)
        return (carry + grad, image)
    total, images = lax.scan(one, jnp.zeros_like(voxels), (offsets, heading, cotangent))
    return (images, total)
```

```python
import functools

import jax
import jax.numpy as jnp
from jax import lax
from jax.experimental import pallas as pl
from jax.experimental.pallas import tpu as pltpu
from jax.sharding import Mesh
from jax.sharding import PartitionSpec as P

LEVELS = 8
AXES = ("dir", "sy", "sx", "sz", "tile")
SLAB = ("sy", "sx", "sz")
MESH = pl.DeviceIdType.MESH
ANY = pl.BlockSpec(memory_space=pl.ANY)
VM = pl.BlockSpec(memory_space=pltpu.VMEM)


def places():
    return {a: lax.axis_index(a) for a in AXES}


def slab_index(me):
    sx, sz = lax.axis_size("sx"), lax.axis_size("sz")
    return (me["sy"] * sx + me["sx"]) * sz + me["sz"]


def at_slab(me, step):
    sy, sx, sz = (lax.axis_size(a) for a in SLAB)
    s = lax.rem(slab_index(me) + step + sy * sx * sz, sy * sx * sz)
    return dict(me, sy=s // (sx * sz), sx=(s // sz) % sx, sz=s % sz)


def ident(place):
    return tuple(place[a] for a in AXES)


def greet(peers):
    barrier = pltpu.get_barrier_semaphore()
    for peer in peers:
        pl.semaphore_signal(barrier, inc=1, device_id=ident(peer), device_id_type=MESH)
    pl.semaphore_wait(barrier, len(peers))


def push(src, dst, send, recv, peer):
    return pltpu.make_async_remote_copy(
        src_ref=src, dst_ref=dst, send_sem=send, recv_sem=recv,
        device_id=ident(peer), device_id_type=MESH,
    )


def halo_kernel(win, half, vox, codes, head, cot,
                zp, zn, rh, zpr, znr, oc, oh, oct_, send, recv):
    me = places()
    d, t = me["dir"], me["tile"]
    prev, nxt = at_slab(me, -1), at_slab(me, 1)
    flip = lambda p: dict(p, tile=1 - p["tile"])
    mate = dict(me, dir=1 - d, sx=lax.axis_size("sx") - 1 - me["sx"])
    greet([prev, nxt, flip(me), flip(prev), flip(nxt), mate])
    planes, rows = vox.shape[1], vox.shape[2]
    cols = pl.ds(pl.multiple_of(d * (half - (win - half)), win - half), win)
    edge = pl.ds(pl.multiple_of((1 - t) * (rows - 8), 8), 8)
    theirs = pl.ds(pl.multiple_of((1 - d) * half, half), half)
    jobs = [
        (vox.at[:, planes - 1, :, cols], zp, nxt),
        (vox.at[:, 0, :, cols], zn, prev),
        (codes.at[0, :, theirs], oc, mate),
        (head.at[0, :, theirs], oh, mate),
        (vox.at[:, planes - 1, edge, cols], zpr, flip(nxt)),
        (vox.at[:, 0, edge, cols], znr, flip(prev)),
        (vox.at[:, :, edge, cols], rh, flip(me)),
        (cot.at[0, :, :, theirs], oct_, mate),
    ]
    copies = [push(a, b, send.at[i], recv.at[i], p) for i, (a, b, p) in enumerate(jobs)]
    for copy in copies:
        copy.start()
    for copy in copies:
        copy.wait()


def exchange_halos(voxels, offsets, heading, cotangent):
    ch, planes, rows, total = voxels.shape
    half = total // 2
    win = half + half // 2
    f32 = lambda *s: jax.ShapeDtypeStruct(s, jnp.float32)
    i32 = lambda *s: jax.ShapeDtypeStruct(s, jnp.int32)
    return pl.pallas_call(
        functools.partial(halo_kernel, win, half),
        out_shape=(f32(ch, rows, win), f32(ch, rows, win), f32(ch, planes, 8, win),
                   f32(ch, 8, win), f32(ch, 8, win),
                   i32(rows, half), i32(rows, half), f32(3, rows, half)),
        in_specs=[ANY] * 4,
        out_specs=(ANY,) * 8,
        scratch_shapes=[pltpu.SemaphoreType.DMA((8,)), pltpu.SemaphoreType.DMA((8,))],
        compiler_params=pltpu.CompilerParams(collective_id=0, has_side_effects=True),
    )(voxels, offsets, heading, cotangent)


def scan_kernel(dl, im, hd, rb, img, rdl, rim, gm, ret, part, rpart,
                s1, r1, s2, r2, s3, r3, s4, r4, s5, r5):
    me = places()
    nsy, nsx, nz = (lax.axis_size(a) for a in SLAB)
    ng = nsy * nsx
    blocks = ng // 2
    z = me["sz"]
    gi = me["sy"] * nsx + me["sx"]
    d = me["dir"]
    lanes = dl.shape[-1]
    rows = lanes // 4

    zpeer = [dict(me, sz=lax.rem(z + i, nz)) for i in range(1, nz)]
    gpeer = []
    for i in range(1, ng):
        g = lax.rem(gi + i, ng)
        gpeer.append(dict(me, sy=g // nsx, sx=g % nsx))
    across = []
    for i in range(ng):
        g = lax.rem(gi + i, ng)
        across.append(dict(me, dir=1 - d, sy=g // nsx, sx=g % nsx))
    greet(zpeer + gpeer + across)

    first = [push(dl.at[p["sz"]], rdl.at[z], s1.at[i], r1.at[i], p) for i, p in enumerate(zpeer)]
    for c in first:
        c.start()
    late = [push(im.at[p["sz"]], rim.at[z], s2.at[i], r2.at[i], p) for i, p in enumerate(zpeer)]
    for c in late:
        c.start()
    rdl[z] = dl[z]
    rim[z] = im[z]
    ahead = hd[z] == 0
    lane = lax.broadcasted_iota(jnp.int32, ahead.shape, 2)
    is_d = (lane // rows) % 2 == 0
    for c in first:
        c.wait()
    roll = lambda a, n: pltpu.roll(a, n % lanes, 2)

    def directed(parts):
        lows, total = [], jnp.zeros_like(parts[0])
        for p in parts:
            lows.append(total)
            total = total + p
        highs, back = [], jnp.zeros_like(parts[0])
        for p in reversed(parts):
            highs.append(back)
            back = back + p
        highs = highs[::-1]
        before = [jnp.where(ahead, a, b) for a, b in zip(lows, highs)]
        after = [jnp.where(ahead, b, a) for a, b in zip(lows, highs)]
        return before, after, total

    tiles = [rdl[i] for i in range(nz)]
    before, _, dsum = directed(tiles)
    reach = [jnp.exp(-b) for b in before]
    pulled = [roll(r, rows) * t for r, t in zip(reach, tiles)]
    _, behind, lsum = directed(pulled)
    gm[gi] = jnp.where(is_d, dsum, lsum)
    second = [push(gm.at[gi], gm.at[gi], s3.at[i], r3.at[i], p) for i, p in enumerate(gpeer)]
    for c in second:
        c.start()
    for c in second:
        c.wait()
    groups = [gm[i] for i in range(ng)]
    gbefore, _, _ = directed(groups)
    greach = [jnp.exp(-b) for b in gbefore]
    gpull = [roll(r, rows) * t for r, t in zip(greach, groups)]
    _, gafter, _ = directed(gpull)
    mine = jnp.zeros_like(dsum)
    rest = jnp.zeros_like(dsum)
    for i in range(ng):
        mine = jnp.where(gi == i, greach[i], mine)
        rest = jnp.where(gi == i, gafter[i], rest)
    mine_l = roll(mine, rows)
    full = []
    for i in range(nz):
        r = mine * reach[i]
        full.append(r)
        ret[i] = jnp.where(is_d, r, rest + mine_l * behind[i])
    back = [push(ret.at[p["sz"]], rb.at[z], s4.at[i], r4.at[i], p) for i, p in enumerate(zpeer)]
    for c in back:
        c.start()
    rb[z] = ret[z]
    for c in late:
        c.wait()
    quarter = lane // rows
    for b in range(2):
        total = jnp.zeros_like(dsum)
        for i in range(nz):
            src = full[i]
            spread = roll(src, -2 * b * rows)
            spread = jnp.where(quarter == 1, roll(src, (1 - 2 * b) * rows), spread)
            spread = jnp.where(quarter == 2, roll(src, (2 - 2 * b) * rows), spread)
            total = total + spread * rim[i, b]
        part[b] = total
    half_of_me = gi // blocks
    out = []
    for b in range(2):
        for m in range(blocks):
            g = blocks * d + m
            peer = dict(me, dir=d if b == 0 else 1 - d, sy=g // nsx, sx=g % nsx)
            out.append(push(part.at[b, m], rpart.at[gi], s5.at[b * blocks + m], r5.at[gi], peer))
    for b in range(2):
        for m in range(blocks):
            copy = out[b * blocks + m]
            if b == 0:
                itself = gi == blocks * d + m

                @pl.when(itself)
                def _():
                    rpart[gi] = part[0, m]

                @pl.when(jnp.logical_not(itself))
                def _():
                    copy.start()
            else:
                copy.start()
    for b in range(2):
        for m in range(blocks):
            copy = out[b * blocks + m]
            if b == 0:
                @pl.when(gi != blocks * d + m)
                def _():
                    copy.wait_send()
            else:
                copy.wait_send()
    for i in range(ng):
        arrive = push(part.at[0, 0], rpart.at[i], s5.at[0], r5.at[i], dict(me, dir=1 - d))

        @pl.when(jnp.logical_or(half_of_me != d, gi != i))
        def _():
            arrive.wait_recv()
    total = rpart[0]
    for i in range(1, ng):
        total = total + rpart[i]
    img[...] = total
    for c in back:
        c.wait()


def scan_slabs(dl, im, hd):
    nz, m, c8, lanes = dl.shape
    nsy, nsx = lax.axis_size("sy"), lax.axis_size("sx")
    ng = nsy * nsx
    f32 = lambda *s: pltpu.VMEM(s, jnp.float32)
    dma = pltpu.SemaphoreType.DMA
    return pl.pallas_call(
        scan_kernel,
        out_shape=(jax.ShapeDtypeStruct(dl.shape, jnp.float32),
                   jax.ShapeDtypeStruct((c8, lanes), jnp.float32)),
        in_specs=[VM] * 3,
        out_specs=(VM, VM),
        scratch_shapes=[
            f32(*dl.shape), f32(*im.shape), f32(ng, m, c8, lanes), f32(*dl.shape),
            f32(2, m, c8, lanes), f32(ng, c8, lanes),
            dma((nz - 1,)), dma((nz - 1,)), dma((nz - 1,)), dma((nz - 1,)),
            dma((ng - 1,)), dma((ng - 1,)), dma((nz - 1,)), dma((nz - 1,)),
            dma((ng,)), dma((ng,)),
        ],
        compiler_params=pltpu.CompilerParams(collective_id=1, has_side_effects=True),
    )(dl, im, hd)


def spill_kernel(zup, zdn, line, pack, fp, fn, rline, rpack, send, recv):
    me = places()
    prev, nxt = at_slab(me, -1), at_slab(me, 1)
    flip = lambda p: dict(p, tile=1 - p["tile"])
    over = lambda p: dict(p, dir=1 - p["dir"])
    near = [prev, me, nxt]
    greet([prev, nxt] + [flip(p) for p in near] + [over(p) for p in near]
          + [over(flip(p)) for p in near])
    jobs = [(zup, fp, nxt), (zdn, fn, prev)]
    for i, p in enumerate(near):
        jobs.append((line, rline.at[2 - i], flip(p)))
    for i, p in enumerate(near):
        jobs.append((pack, rpack.at[2 - i, 0], over(p)))
        jobs.append((pack, rpack.at[2 - i, 1], over(flip(p))))
    copies = [push(a, b, send.at[i], recv.at[i], p) for i, (a, b, p) in enumerate(jobs)]
    for copy in copies:
        copy.start()
    for copy in copies:
        copy.wait()


def exchange_spill(zup, zdn, line, pack):
    s = jax.ShapeDtypeStruct
    return pl.pallas_call(
        spill_kernel,
        out_shape=(s(zup.shape, jnp.float32), s(zdn.shape, jnp.float32),
                   s((3,) + line.shape, jnp.float32), s((3, 2) + pack.shape, jnp.float32)),
        in_specs=[VM] * 4,
        out_specs=(VM,) * 4,
        scratch_shapes=[pltpu.SemaphoreType.DMA((11,)), pltpu.SemaphoreType.DMA((11,))],
        compiler_params=pltpu.CompilerParams(collective_id=2, has_side_effects=True),
    )(zup, zdn, line, pack)


def tap_weights(codes):
    level = LEVELS
    fz = (codes % level).astype(jnp.float32)
    fy = (codes // level % level).astype(jnp.float32)
    fx = (codes // (level * level)).astype(jnp.float32)

    def three(raw):
        f = (raw + 0.5) / level - 0.5
        return (jnp.maximum(-f, 0.0), 1.0 - jnp.abs(f), jnp.maximum(f, 0.0))

    return (three(fz), three(fy), three(fx))


def to_tiles(stacked, nz):
    lanes, cols = stacked.shape
    tiles = stacked.T.reshape(cols // 8 // nz, nz, 8, lanes)
    return jnp.moveaxis(tiles, 1, 0)


def from_tiles(tiles):
    nz, m, c8, lanes = tiles.shape
    return jnp.moveaxis(tiles, 0, 1).reshape(m * nz * c8, lanes).T


def per_device(voxels, offsets, heading, cotangent):
    ch, planes, rows, total = voxels.shape
    nz = lax.axis_size("sz")
    slabs = lax.axis_size(SLAB)
    depth = planes * slabs
    scale = 2.0 / depth
    half = total // 2
    ext = half // 2
    win = half + ext
    me = places()
    d, t, s = me["dir"], me["tile"], slab_index(me)
    zp, zn, rh, zpr, znr, oc, oh, oct_ = exchange_halos(voxels, offsets, heading, cotangent)

    own = lambda a: lax.dynamic_slice_in_dim(a[0], d * half, half, axis=a.ndim - 2)
    codes = jnp.stack([own(offsets), oc])
    head = jnp.stack([own(heading), oh])
    pull = jnp.stack([own(cotangent), oct_]) * depth
    forward = head == 0

    zp = jnp.where(s > 0, zp, 0.0)
    zpr = jnp.where(s > 0, zpr, 0.0)
    zn = jnp.where(s < slabs - 1, zn, 0.0)
    znr = jnp.where(s < slabs - 1, znr, 0.0)
    core = lax.dynamic_slice_in_dim(voxels, d * (half - ext), win, axis=3)
    body = jnp.concatenate([zp[:, None], core, zn[:, None]], axis=1)
    side = jnp.concatenate([zpr[:, None], rh, znr[:, None]], axis=1)
    top = jnp.where(t == 1, side[:, :, 7:8], 0.0)
    low = jnp.where(t == 0, side[:, :, 0:1], 0.0)
    grid = jnp.concatenate([top, body, low], axis=2)
    grid = jnp.pad(grid, ((0, 0), (0, 0), (0, 0), (1, 1)))
    grid = lax.dynamic_slice_in_dim(grid, d * (half - ext), half + 2, axis=3)

    wz, wy, wx = tap_weights(codes)
    plane = None
    for b in range(3):
        for e in range(3):
            term = (wy[b] * wx[e])[:, None, None] * grid[None, :, :, b:b + rows, e:e + half]
            plane = term if plane is None else plane + term
    values = None
    for a in range(3):
        term = wz[a][:, None, None] * plane[:, :, a:a + planes]
        values = term if values is None else values + term
    sigma = jax.nn.softplus(values[:, 0]) * scale
    colour = jax.nn.sigmoid(values[:, 1:])
    alpha = 1.0 - jnp.exp(-sigma)
    ahead = jnp.cumsum(sigma, axis=1) - sigma
    depth_sum = jnp.sum(sigma, axis=1)
    front = jnp.where(forward[:, None], ahead, depth_sum[:, None] - ahead - sigma)
    through = jnp.exp(-front)
    glow = through * alpha
    local_image = jnp.sum(glow[:, None] * colour, axis=2)
    shade = jnp.sum(pull[:, :, None] * colour, axis=1)
    local_pull = jnp.sum(pull * local_image, axis=1)

    stacked = jnp.stack([depth_sum, local_pull], axis=1).reshape(4 * rows, half)
    dl = to_tiles(stacked, nz)
    blank = jnp.zeros_like(depth_sum)[:, None]
    images = jnp.concatenate([local_image, blank], axis=1).reshape(2, 4 * rows, half)
    im = jnp.stack([to_tiles(images[0], nz), to_tiles(images[1], nz)], axis=1)
    hd = to_tiles(jnp.stack([head, head], axis=1).reshape(4 * rows, half), nz)
    rb, img = scan_slabs(dl, im, hd)
    image = img.T.reshape(4, rows, 8)[None, :3]
    rb = from_tiles(rb).reshape(2, 2, rows, half)
    reach, rest = rb[:, 0], rb[:, 1]

    lit = reach[:, None] * glow
    share = lit * shade
    share_before = jnp.cumsum(share, axis=1) - share
    share_sum = jnp.sum(share, axis=1)
    behind = rest[:, None] + jnp.where(
        forward[:, None], share_sum[:, None] - share_before - share, share_before
    )
    d_sigma = reach[:, None] * (through - glow) * shade - behind
    grad_density = d_sigma * jax.nn.sigmoid(values[:, 0]) * scale
    grad_colour = pull[:, :, None] * lit[:, None] * colour * (1.0 - colour)
    grads = jnp.concatenate([grad_density[:, None], grad_colour], axis=1)

    padded = jnp.pad(grads, ((0, 0), (0, 0), (2, 2), (0, 0), (0, 0)))
    column = None
    for a in range(3):
        term = wz[a][:, None, None] * padded[:, :, 2 - a:2 - a + planes + 2]
        column = term if column is None else column + term
    wide = None
    for b in range(3):
        for e in range(3):
            term = jnp.sum((wy[b] * wx[e])[:, None, None] * column, axis=0)
            term = jnp.pad(term, ((0, 0), (0, 0), (b, 2 - b), (e, 2 - e)))
            wide = term if wide is None else wide + term
    inner = wide[:, :, 1:rows + 1, 1:half + 1]
    line = jnp.where(t == 0, wide[:, :, rows + 1], wide[:, :, 0])
    edge = jnp.where(d == 0, wide[..., half + 1], wide[..., 0])
    far = jnp.where(t == 0, edge[:, :, rows + 1], edge[:, :, 0])
    packs = ch * (planes + 2)
    pack = jnp.concatenate([edge[:, :, 1:rows + 1], far[:, :, None]], axis=2)
    pack = pack.reshape(packs, rows + 1).T
    pack = jnp.pad(pack, ((0, 7), (0, 128 - packs)))
    line = line[:, :, 1:half + 1].reshape(packs, half)

    fp, fn, rline, rpack = exchange_spill(inner[:, -1], inner[:, 0], line, pack)
    has_prev, has_next = s > 0, s < slabs - 1
    grad = inner[:, 1:-1]
    grad = grad.at[:, 0].add(jnp.where(has_prev, fp, 0.0))
    grad = grad.at[:, -1].add(jnp.where(has_next, fn, 0.0))
    rline = rline.reshape(3, ch, planes + 2, half)
    row = rline[1, :, 1:-1]
    row = row.at[:, 0].add(jnp.where(has_prev, rline[0, :, -1], 0.0))
    row = row.at[:, -1].add(jnp.where(has_next, rline[2, :, 0], 0.0))
    rpack = rpack[..., :rows + 1, :packs].reshape(3, 2, rows + 1, ch, planes + 2)
    rim = rpack[1, :, :, :, 1:-1]
    rim = rim.at[..., 0].add(jnp.where(has_prev, rpack[0, ..., -1], 0.0))
    rim = rim.at[..., -1].add(jnp.where(has_next, rpack[2, ..., 0], 0.0))
    touch = (1 - t) * (rows - 1)
    grad = jnp.where(
        lax.broadcasted_iota(jnp.int32, grad.shape, 2) == touch, grad + row[:, :, None], grad
    )
    col = rim[0, :rows]
    col = jnp.where(
        lax.broadcasted_iota(jnp.int32, col.shape, 0) == touch, col + rim[1, rows], col
    )
    col = jnp.moveaxis(col, 0, -1)
    seam = (1 - d) * (half - 1)
    grad = jnp.where(
        lax.broadcasted_iota(jnp.int32, grad.shape, 3) == seam, grad + col[..., None], grad
    )
    return (image, grad)


def solution(mesh):
    n = mesh.devices.size
    shape = (2, 4, 2, 8, 2) if n == 256 else (2, 2, 1, 2, 2)
    finer = Mesh(mesh.devices.reshape(shape), AXES)
    return jax.shard_map(
        per_device,
        mesh=finer,
        in_specs=(
            P(None, SLAB, "tile", None),
            P("dir", "tile", None),
            P("dir", "tile", None),
            P("dir", None, "tile", None),
        ),
        out_specs=(P("dir", None, "tile", SLAB), P(None, SLAB, "tile", "dir")),
        check_vma=False,
    )
```

```python
import functools
from types import SimpleNamespace
from typing import NamedTuple

import jax
import jax.numpy as jnp
from jax import lax
from jax.experimental import pallas as pl
from jax.experimental.pallas import tpu as pltpu
from jax.sharding import Mesh
from jax.sharding import PartitionSpec as P

LEVELS = 8
AXES = ("dir", "sy", "sx", "sz", "tile")
SLAB = AXES[1:4]
MESH = pl.DeviceIdType.MESH
ANY = pl.BlockSpec(memory_space=pl.ANY)
VM = pl.BlockSpec(memory_space=pltpu.VMEM)


class Place(NamedTuple):
    dir: int
    sy: int
    sx: int
    sz: int
    tile: int


def places():
    return Place(*[lax.axis_index(a) for a in AXES])


def slab_index(me):
    _, _, sx, sz, _ = (lax.axis_size(a) for a in AXES)
    return (me.sy * sx + me.sx) * sz + me.sz


def at_slab(me, step):
    sy, sx, sz = (lax.axis_size(a) for a in SLAB)
    s = lax.rem(slab_index(me) + step + sy * sx * sz, sy * sx * sz)
    return me._replace(sy=s // (sx * sz), sx=(s // sz) % sx, sz=s % sz)


def greet(peers):
    barrier = pltpu.get_barrier_semaphore()
    for peer in peers:
        pl.semaphore_signal(barrier, inc=1, device_id=tuple(peer), device_id_type=MESH)
    pl.semaphore_wait(barrier, len(peers))


def push(src, dst, send, recv, peer):
    return pltpu.make_async_remote_copy(
        src_ref=src, dst_ref=dst, send_sem=send, recv_sem=recv,
        device_id=tuple(peer), device_id_type=MESH,
    )


def shapes(ch, planes, rows, half, wide, nz, ng):
    lanes, m = 4 * rows, half // 8 // nz
    ext = planes + 2
    f32 = jnp.float32
    one = dict(
        grid=(ch, ext, rows, half), wing=(ch, ext, rows, wide),
        rows=(ch, ext, 8, half), rwing=(ch, ext, 8, wide),
        plane=(2, ch, ext, rows, half), sigma=(2, planes, rows, half),
        slope=(2, planes, rows, half), colour=(2, 3, planes, rows, half),
        through=(2, planes, rows, half), glow=(2, planes, rows, half),
        taps=(2, 9, rows, half), pair=(2, 7, rows, half),
        codes=(2, rows, half), heading=(2, rows, half), pull=(2, 3, rows, half),
        ahead=(2, planes, rows, half), stack=(lanes, half),
        diff=(2, ch, planes + 4, rows, half), out=(ch, ext, rows, half),
        line=(ext, ch, half), pack=(rows + 8, max(wide, ch * ext)),
        fp=(ch, rows, half), fn=(ch, rows, half),
        rline=(3, ext, ch, half), rpack=(3, 2, rows + 8, max(wide, ch * ext)),
        tile=(wide, lanes),
        dl=(nz, m, 8, lanes), im=(nz, 2, m, 8, lanes), hd=(nz, m, 8, lanes),
        rdl=(nz, m, 8, lanes), rim=(nz, 2, m, 8, lanes), gm=(ng, m, 8, lanes),
        ret=(nz, m, 8, lanes), rb=(nz, m, 8, lanes),
        part=(2, m, 8, lanes), rpart=(ng, 8, lanes),
    )
    ints = dict(codes=0, heading=0)
    return {k: pltpu.VMEM(v, jnp.int32 if k in ints else f32) for k, v in one.items()}


def weights(b, g):
    level = LEVELS
    q = b.codes[g]
    frac = lambda raw: (raw.astype(jnp.float32) + 0.5) / level - 0.5
    fz, fy, fx = frac(q & 7), frac((q >> 3) & 7), frac(q >> 6)
    three = lambda f: (jnp.maximum(-f, 0.0), 1.0 - jnp.abs(f), jnp.maximum(f, 0.0))
    wy, wx = three(fy), three(fx)
    for i in range(3):
        for j in range(3):
            b.taps[g, 3 * i + j] = wy[i] * wx[j]
    ay, ax = jnp.abs(fy), jnp.abs(fx)
    for i, v in enumerate((fz, fy, fx, wy[1] * wx[1], wy[1] * ax, ay * wx[1], ay * ax)):
        b.pair[g, i] = v


def iota(shape, dim):
    return lax.broadcasted_iota(jnp.int32, shape, dim)


def sample_plane(b, me, p, keep):
    ch, _, rows, half = b.grid.shape
    tw = half // 2
    d, t = me.dir, me.tile
    row, lane = iota((rows, tw), 0), iota((rows, tw), 1)
    right = (d == 0).astype(jnp.float32)
    left = 1.0 - right
    under = (t == 0).astype(jnp.float32)
    over = 1.0 - under
    for c in range(ch):
        pick = lambda r: jnp.where(d == 0, r[:, 0:1], r[:, tw - 1:tw])
        edge = jnp.broadcast_to(pick(b.wing[c, p]), (rows, tw))
        fr = lambda r: jnp.where(t == 0, r[0:1], r[7:8])
        ecorner = jnp.broadcast_to(pick(fr(b.rwing[c, p])), (1, tw))
        m = [b.grid[c, p, :, x * tw:(x + 1) * tw] for x in range(2)] + [edge]
        far = [fr(b.rows[c, p, :, x * tw:(x + 1) * tw]) for x in range(2)] + [ecorner]
        up = [jnp.where(row == 0, f * over, pltpu.roll(a, 1, 0)) for a, f in zip(m, far)]
        dn = [jnp.where(row == rows - 1, f * under, pltpu.roll(a, rows - 1, 0))
              for a, f in zip(m, far)]
        spread = []
        for a in (up, m, dn):
            r = [pltpu.roll(a[x], 1, 1) for x in range(2)]
            l = [pltpu.roll(a[x], tw - 1, 1) for x in range(2)]
            lo = [jnp.where(lane == 0, a[2] * left, r[0]), jnp.where(lane == 0, r[0], r[1])]
            hi = [jnp.where(lane == tw - 1, l[1], l[0]),
                  jnp.where(lane == tw - 1, a[2] * right, l[1])]
            spread.append((lo, a[:2], hi))
        for x in range(2):
            at = slice(x * tw, (x + 1) * tw)
            for g in range(2):
                fy, fx = b.pair[g, 1, :, at], b.pair[g, 2, :, at]
                w00, w01 = b.pair[g, 3, :, at], b.pair[g, 4, :, at]
                w10, w11 = b.pair[g, 5, :, at], b.pair[g, 6, :, at]
                side = lambda s: jnp.where(fx > 0, s[2][x], s[0][x])
                down = fy > 0
                v = (w00 * m[x] + w01 * side(spread[1])
                     + w10 * jnp.where(down, dn[x], up[x])
                     + w11 * jnp.where(down, side(spread[2]), side(spread[0])))
                b.plane[g, c, p, :, at] = v if keep is None else v * keep


def shade_planes(b, scale):
    _, ch, ext, rows, half = b.plane.shape
    planes = ext - 2

    def step(k, acc):
        new = []
        for g in range(2):
            fz = b.pair[g, 0]
            az = jnp.abs(fz)
            v = []
            for c in range(ch):
                mid = b.plane[g, c, k + 1]
                far = jnp.where(fz > 0, b.plane[g, c, k + 2], b.plane[g, c, k])
                v.append((1.0 - az) * mid + az * far)
            sg = (jnp.maximum(v[0], 0.0) + jnp.log(1.0 + jnp.exp(-jnp.abs(v[0])))) * scale
            b.sigma[g, k] = sg
            b.slope[g, k] = (0.5 + 0.5 * jnp.tanh(0.5 * v[0])) * scale
            for c in range(3):
                b.colour[g, c, k] = 0.5 + 0.5 * jnp.tanh(0.5 * v[c + 1])
            b.ahead[g, k] = acc[g]
            new.append(acc[g] + sg)
        return tuple(new)

    zero = jnp.zeros((rows, half), jnp.float32)
    return lax.fori_loop(0, planes, step, (zero, zero))


def local_light(b, totals):
    _, planes, rows, half = b.sigma.shape
    images = []
    for g in range(2):
        forward = b.heading[g] == 0

        def step(k, acc):
            sg, ah = b.sigma[g, k], b.ahead[g, k]
            front = jnp.where(forward, ah, totals[g] - ah - sg)
            th = jnp.exp(-front)
            gl = th * (1.0 - jnp.exp(-sg))
            b.through[g, k] = th
            b.glow[g, k] = gl
            return tuple(acc[c] + gl * b.colour[g, c, k] for c in range(3))

        zero = jnp.zeros((rows, half), jnp.float32)
        images.append(lax.fori_loop(0, planes, step, (zero,) * 3))
    return images


def tiles_out(b, put, nz):
    lanes, half = b.stack.shape
    tw = half // 2
    for x in range(2):
        turned = b.stack[:, x * tw:(x + 1) * tw].T
        for i in range(tw // 8):
            j = x * (tw // 8) + i
            put(j % nz, j // nz, turned[8 * i:8 * i + 8])


def backward(b, kept):
    _, planes, rows, half = b.sigma.shape
    zero = jnp.zeros((rows, half), jnp.float32)
    for g in range(2):
        forward = b.heading[g] == 0
        reach = b.stack[2 * g * rows:(2 * g + 1) * rows]
        rest = b.stack[(2 * g + 1) * rows:(2 * g + 2) * rows]
        whole = reach * kept[g]
        for c in range(4):
            for k in (0, 1, planes + 2, planes + 3):
                b.diff[g, c, k] = zero

        def step(k, before):
            pull = [b.pull[g, c] for c in range(3)]
            col = [b.colour[g, c, k] for c in range(3)]
            shade = pull[0] * col[0] + pull[1] * col[1] + pull[2] * col[2]
            th, gl = b.through[g, k], b.glow[g, k]
            lit = reach * gl
            share = lit * shade
            behind = rest + jnp.where(forward, whole - before - share, before)
            b.diff[g, 0, k + 2] = (reach * (th - gl) * shade - behind) * b.slope[g, k]
            for c in range(3):
                b.diff[g, c + 1, k + 2] = pull[c] * lit * (col[c] * (1.0 - col[c]))
            return before + share

        lax.fori_loop(0, planes, step, zero)


def spill_plane(b, me, p):
    ch, ext, rows, half = b.out.shape
    tw = half // 2
    d, t = me.dir, me.tile
    row, lane = iota((rows, tw), 0), iota((rows, tw), 1)
    for c in range(ch):
        pos = c * ext + p
        cols = []
        for g in range(2):
            fz = b.pair[g, 0]
            cols.append((1.0 - jnp.abs(fz)) * b.diff[g, c, p + 1]
                        + jnp.maximum(fz, 0.0) * b.diff[g, c, p]
                        + jnp.maximum(-fz, 0.0) * b.diff[g, c, p + 2])
        bands = []
        for i in range(3):
            u = []
            for j in range(3):
                full = (b.taps[0, 3 * i + j] * cols[0] + b.taps[1, 3 * i + j] * cols[1])
                u.append([full[:, :tw], full[:, tw:]])
            l = [pltpu.roll(a, tw - 1, 1) for a in u[0]]
            r = [pltpu.roll(a, 1, 1) for a in u[2]]
            x0 = u[1][0] + jnp.where(lane == tw - 1, l[1], l[0]) + jnp.where(lane == 0, 0.0, r[0])
            x1 = u[1][1] + jnp.where(lane == tw - 1, 0.0, l[1]) + jnp.where(lane == 0, r[0], r[1])
            bands.append([x0, x1, jnp.where(d == 0, r[1], u[0][0])])
        done, far = [], []
        for x in range(3):
            up = pltpu.roll(bands[0][x], rows - 1, 0)
            dn = pltpu.roll(bands[2][x], 1, 0)
            done.append(bands[1][x] + jnp.where(row == rows - 1, 0.0, up)
                        + jnp.where(row == 0, 0.0, dn))
            far.append(jnp.where(t == 0, dn[0:1], up[rows - 1:rows]))
        b.out[c, p, :, :tw] = done[0]
        b.out[c, p, :, tw:] = done[1]
        b.line[p, c:c + 1, :tw] = far[0]
        b.line[p, c:c + 1, tw:] = far[1]
        slot = iota((rows, b.pack.shape[1]), 1)
        wide = b.pack.shape[1]
        b.pack[:rows] = jnp.where(
            slot == pos, jnp.broadcast_to(done[2][:, 0:1], (rows, wide)), b.pack[:rows])
        b.pack[rows:rows + 1] = jnp.where(
            slot[0:1] == pos, jnp.broadcast_to(far[2][:, 0:1], (1, wide)), b.pack[rows:rows + 1])


def gather_spill(b, me, has_prev, has_next, dest):
    ch, ext, rows, half = b.out.shape
    planes = ext - 2
    tw = half // 2
    wide = b.pack.shape[1]
    d, t = me.dir, me.tile
    touch = (1 - t) * (rows - 1)
    seam = (1 - d) * (half - 1)
    slot = iota((rows, wide), 1)
    row = iota((rows, tw), 0)
    lane = iota((rows, tw), 1)

    def merged(i, lo, hi):
        a = b.rpack[1, i, lo:hi]
        at = slot[:hi - lo] % ext
        a = a + jnp.where(at == 1, pltpu.roll(b.rpack[0, i, lo:hi], wide - planes, 1), 0.0) * has_prev
        return a + jnp.where(at == planes, pltpu.roll(b.rpack[2, i, lo:hi], planes, 1), 0.0) * has_next

    col = merged(0, 0, rows)
    corner = merged(1, rows, rows + 8)[0:1]
    col = col + jnp.where(iota((rows, wide), 0) == touch, jnp.broadcast_to(corner, (rows, wide)), 0.0)
    for c in range(ch):
        for k in range(planes):
            pos = c * ext + k + 1
            extra = b.rline[1, k + 1, c:c + 1]
            v = b.out[c, k + 1]
            if k == 0:
                extra = extra + b.rline[0, ext - 1, c:c + 1] * has_prev
                v = v + b.fp[c] * has_prev
            if k == planes - 1:
                extra = extra + b.rline[2, 0, c:c + 1] * has_next
                v = v + b.fn[c] * has_next
            bar = jnp.broadcast_to(col[:, pos:pos + 1], (rows, tw))
            for x in range(2):
                at = slice(x * tw, (x + 1) * tw)
                y = v[:, at] + jnp.where(row == touch, jnp.broadcast_to(extra[:, at], (rows, tw)), 0.0)
                y = y + jnp.where(lane + x * tw == seam, bar, 0.0)
                dest[c, k, :, at] = y


def render_kernel(scale, depth, names, vox, codes, head, cot, grad, img, *scratch):
    b = SimpleNamespace(**dict(zip(names, scratch)))
    sems = scratch[len(names):]
    (lsem, hs, hr, s1, r1, s2, r2, s3, r3, s4, r4, s5, r5, ss, sr) = sems
    me = places()
    nsy, nsx, nz = (lax.axis_size(a) for a in SLAB)
    ng = nsy * nsx
    blocks = ng // 2
    d, t, z = me.dir, me.tile, me.sz
    gi = me.sy * nsx + me.sx
    s = slab_index(me)
    prev, nxt = at_slab(me, -1), at_slab(me, 1)
    flip = lambda p: p._replace(tile=1 - p.tile)
    over = lambda p: p._replace(dir=1 - p.dir)
    near = [prev, me, nxt]
    mate = me._replace(dir=1 - d, sx=nsx - 1 - me.sx)
    ch, ext, rows, half = b.grid.shape
    planes = ext - 2
    wide = b.wing.shape[-1]
    has_prev = (s > 0).astype(jnp.float32)
    has_next = (s < nsy * nsx * nz - 1).astype(jnp.float32)

    mine = pl.ds(pl.multiple_of(d * half, half), half)
    theirs = pl.ds(pl.multiple_of((1 - d) * half, half), half)
    beside = pl.ds(pl.multiple_of(half - d * wide, wide), wide)
    loads = [
        (vox.at[:, :, :, mine], b.grid.at[:, 1:planes + 1]),
        (vox.at[:, :, :, beside], b.wing.at[:, 1:planes + 1]),
        (codes.at[0, :, mine], b.codes.at[0]),
        (head.at[0, :, mine], b.heading.at[0]),
        (cot.at[0, :, :, mine], b.pull.at[0]),
    ]
    loads = [pltpu.make_async_copy(a, c, lsem.at[i]) for i, (a, c) in enumerate(loads)]
    for c in loads:
        c.start()

    zpeer = [me._replace(sz=lax.rem(z + i, nz)) for i in range(1, nz)]
    gpeer, across = [], []
    for i in range(ng):
        g = lax.rem(gi + i, ng)
        p = me._replace(sy=g // nsx, sx=g % nsx)
        across.append(over(p))
        if i:
            gpeer.append(p)
    greet([prev, nxt] + [flip(p) for p in near] + [over(p) for p in near]
          + [over(flip(p)) for p in near] + zpeer + gpeer + across)

    rays = [
        (codes.at[0, :, theirs], b.codes.at[1], mate),
        (head.at[0, :, theirs], b.heading.at[1], mate),
        (cot.at[0, :, :, theirs], b.pull.at[1], mate),
    ]
    rays = [push(x, y, hs.at[i], hr.at[i], p) for i, (x, y, p) in enumerate(rays)]
    for c in rays:
        c.start()
    for c in loads[:2]:
        c.wait()
    edge = pl.ds(pl.multiple_of((1 - t) * (rows - 8), 8), 8)
    inner = pl.ds(1, planes)
    beyond = [
        (b.grid.at[:, inner, edge], b.rows.at[:, inner], flip(me)),
        (b.wing.at[:, inner, edge], b.rwing.at[:, inner], flip(me)),
        (b.grid.at[:, planes], b.grid.at[:, 0], nxt),
        (b.grid.at[:, 1], b.grid.at[:, ext - 1], prev),
        (b.wing.at[:, planes], b.wing.at[:, 0], nxt),
        (b.wing.at[:, 1], b.wing.at[:, ext - 1], prev),
        (b.grid.at[:, planes, edge], b.rows.at[:, 0], flip(nxt)),
        (b.grid.at[:, 1, edge], b.rows.at[:, ext - 1], flip(prev)),
        (b.wing.at[:, planes, edge], b.rwing.at[:, 0], flip(nxt)),
        (b.wing.at[:, 1, edge], b.rwing.at[:, ext - 1], flip(prev)),
    ]
    beyond = [push(x, y, hs.at[3 + i], hr.at[3 + i], p) for i, (x, y, p) in enumerate(beyond)]
    for c in beyond:
        c.start()
    for c in loads[2:]:
        c.wait()
    weights(b, 0)
    rays[0].wait()
    weights(b, 1)
    for c in beyond[:2]:
        c.wait()

    def inside(p, carry):
        sample_plane(b, me, p, None)
        return carry

    lax.fori_loop(1, planes + 1, inside, 0)
    for c in beyond[2:]:
        c.wait()

    def ends(i, carry):
        sample_plane(b, me, i * (ext - 1), jnp.where(i == 0, has_prev, has_next))
        return carry

    lax.fori_loop(0, 2, ends, 0)
    totals = shade_planes(b, scale)
    for c in rays[1:]:
        c.wait()
    for g in range(2):
        for c in range(3):
            b.pull[g, c] = b.pull[g, c] * depth
    images = local_light(b, totals)
    kept = []
    for g in range(2):
        kept.append(sum(b.pull[g, c] * images[g][c] for c in range(3)))
        b.stack[2 * g * rows:(2 * g + 1) * rows] = totals[g]
        b.stack[(2 * g + 1) * rows:(2 * g + 2) * rows] = kept[g]

    def put_dl(j, m, v):
        b.dl[j, m] = v

    tiles_out(b, put_dl, nz)
    first = [push(b.dl.at[p.sz], b.rdl.at[z], s1.at[i], r1.at[i], p)
             for i, p in enumerate(zpeer)]
    for c in first:
        c.start()
    for g in range(2):
        for c in range(3):
            b.stack[c * rows:(c + 1) * rows] = images[g][c]

        def put_im(j, m, v):
            b.im[j, g, m] = v

        tiles_out(b, put_im, nz)
    late = [push(b.im.at[p.sz], b.rim.at[z], s2.at[i], r2.at[i], p)
            for i, p in enumerate(zpeer)]
    for c in late:
        c.start()
    for g in range(2):
        for i in range(2):
            b.stack[(2 * g + i) * rows:(2 * g + i + 1) * rows] = b.heading[g].astype(jnp.float32)

    def put_hd(j, m, v):
        b.hd[j, m] = v

    tiles_out(b, put_hd, nz)
    b.rdl[z] = b.dl[z]
    b.rim[z] = b.im[z]
    lanes = b.dl.shape[-1]
    ahead = b.hd[z] == 0
    spot = iota(ahead.shape, 2)
    is_d = (spot // rows) % 2 == 0
    for c in first:
        c.wait()
    roll = lambda a, n: pltpu.roll(a, n % lanes, 2)

    def directed(parts):
        lows, low = [], jnp.zeros_like(parts[0])
        for p in parts:
            lows.append(low)
            low = low + p
        highs, high = [], jnp.zeros_like(parts[0])
        for p in reversed(parts):
            highs.append(high)
            high = high + p
        highs = highs[::-1]
        before = [jnp.where(ahead, x, y) for x, y in zip(lows, highs)]
        after = [jnp.where(ahead, y, x) for x, y in zip(lows, highs)]
        return before, after, low

    tiles = [b.rdl[i] for i in range(nz)]
    before, _, dsum = directed(tiles)
    reach = [jnp.exp(-x) for x in before]
    pulled = [roll(r, rows) * x for r, x in zip(reach, tiles)]
    _, behind, lsum = directed(pulled)
    b.gm[gi] = jnp.where(is_d, dsum, lsum)
    second = [push(b.gm.at[gi], b.gm.at[gi], s3.at[i], r3.at[i], p)
              for i, p in enumerate(gpeer)]
    for c in second:
        c.start()
    for c in second:
        c.wait()
    groups = [b.gm[i] for i in range(ng)]
    gbefore, _, _ = directed(groups)
    greach = [jnp.exp(-x) for x in gbefore]
    gpull = [roll(r, rows) * x for r, x in zip(greach, groups)]
    _, gafter, _ = directed(gpull)
    to_me = jnp.zeros_like(dsum)
    rest = jnp.zeros_like(dsum)
    for i in range(ng):
        to_me = jnp.where(gi == i, greach[i], to_me)
        rest = jnp.where(gi == i, gafter[i], rest)
    to_me_l = roll(to_me, rows)
    full = []
    for i in range(nz):
        r = to_me * reach[i]
        full.append(r)
        b.ret[i] = jnp.where(is_d, r, rest + to_me_l * behind[i])
    back = [push(b.ret.at[p.sz], b.rb.at[z], s4.at[i], r4.at[i], p)
            for i, p in enumerate(zpeer)]
    for c in back:
        c.start()
    b.rb[z] = b.ret[z]
    for c in late:
        c.wait()
    quarter = spot // rows
    for g in range(2):
        total = jnp.zeros_like(dsum)
        for i in range(nz):
            src = full[i]
            wash = roll(src, -2 * g * rows)
            wash = jnp.where(quarter == 1, roll(src, (1 - 2 * g) * rows), wash)
            wash = jnp.where(quarter == 2, roll(src, (2 - 2 * g) * rows), wash)
            total = total + wash * b.rim[i, g]
        b.part[g] = total
    half_of_me = gi // blocks
    out = []
    for g in range(2):
        for m in range(blocks):
            q = blocks * d + m
            peer = me._replace(dir=d if g == 0 else 1 - d, sy=q // nsx, sx=q % nsx)
            out.append(push(b.part.at[g, m], b.rpart.at[gi],
                            s5.at[g * blocks + m], r5.at[gi], peer))
    for g in range(2):
        for m in range(blocks):
            copy = out[g * blocks + m]
            if g == 0:
                itself = gi == blocks * d + m

                @pl.when(itself)
                def _():
                    b.rpart[gi] = b.part[0, m]

                @pl.when(jnp.logical_not(itself))
                def _():
                    copy.start()
            else:
                copy.start()
    for c in back:
        c.wait()

    tw = half // 2
    for x in range(2):
        for i in range(tw // 8):
            j = x * (tw // 8) + i
            b.tile[8 * i:8 * i + 8] = b.rb[j % nz, j // nz]
        b.stack[:, x * tw:(x + 1) * tw] = b.tile[...].T
    backward(b, kept)

    def spread(p, carry):
        spill_plane(b, me, p)
        return carry

    lax.fori_loop(0, ext, spread, 0)
    spill = [(b.out.at[:, ext - 1], b.fp, nxt), (b.out.at[:, 0], b.fn, prev)]
    for i, p in enumerate(near):
        spill.append((b.line, b.rline.at[2 - i], flip(p)))
    for i, p in enumerate(near):
        spill.append((b.pack, b.rpack.at[2 - i, 0], over(p)))
        spill.append((b.pack, b.rpack.at[2 - i, 1], over(flip(p))))
    spill = [push(x, y, ss.at[i], sr.at[i], p) for i, (x, y, p) in enumerate(spill)]
    for c in spill:
        c.start()

    for g in range(2):
        for m in range(blocks):
            copy = out[g * blocks + m]
            if g == 0:
                @pl.when(gi != blocks * d + m)
                def _():
                    copy.wait_send()
            else:
                copy.wait_send()
    for i in range(ng):
        arrive = push(b.part.at[0, 0], b.rpart.at[i], s5.at[0], r5.at[i], over(me))

        @pl.when(jnp.logical_or(half_of_me != d, gi != i))
        def _():
            arrive.wait_recv()
    total = b.rpart[0]
    for i in range(1, ng):
        total = total + b.rpart[i]
    img[...] = total
    for c in spill:
        c.wait()
    gather_spill(b, me, has_prev, has_next, grad)


def per_device(voxels, offsets, heading, cotangent):
    ch, planes, rows, total = voxels.shape
    nsy, nsx, nz = (lax.axis_size(a) for a in SLAB)
    ng = nsy * nsx
    depth = planes * nz * ng
    half = total // 2
    wide = half // 2
    room = shapes(ch, planes, rows, half, wide, nz, ng)
    dma = lambda n: pltpu.SemaphoreType.DMA((n,))
    grad, img = pl.pallas_call(
        functools.partial(render_kernel, 2.0 / depth, float(depth), tuple(room)),
        out_shape=(jax.ShapeDtypeStruct((ch, planes, rows, half), jnp.float32),
                   jax.ShapeDtypeStruct((8, 4 * rows), jnp.float32)),
        in_specs=[ANY] * 4,
        out_specs=(VM, VM),
        scratch_shapes=list(room.values()) + [
            dma(5), dma(13), dma(13),
            dma(nz - 1), dma(nz - 1), dma(nz - 1), dma(nz - 1),
            dma(ng - 1), dma(ng - 1), dma(nz - 1), dma(nz - 1),
            dma(ng), dma(ng), dma(11), dma(11),
        ],
        compiler_params=pltpu.CompilerParams(
            collective_id=0, has_side_effects=True, vmem_limit_bytes=60 * 1024 * 1024
        ),
    )(voxels, offsets, heading, cotangent)
    image = img.T.reshape(4, rows, 8)[None, :3]
    return (image, grad)


def solution(mesh):
    n = mesh.devices.size
    shape = (2, 4, 2, 8, 2) if n == 256 else (2, 2, 1, 2, 2)
    finer = Mesh(mesh.devices.reshape(shape), AXES)
    return jax.shard_map(
        per_device,
        mesh=finer,
        in_specs=(
            P(None, SLAB, "tile", None),
            P("dir", "tile", None),
            P("dir", "tile", None),
            P("dir", None, "tile", None),
        ),
        out_specs=(P("dir", None, "tile", SLAB), P(None, SLAB, "tile", "dir")),
        check_vma=False,
    )
```

```python
import functools
from types import SimpleNamespace
from typing import NamedTuple

import jax
import jax.numpy as jnp
from jax import lax
from jax.experimental import pallas as pl
from jax.experimental.pallas import tpu as pltpu
from jax.sharding import Mesh
from jax.sharding import PartitionSpec as P

LEVELS = 8
SIDE = 128
AXES = ("dir", "sy", "sx", "sz", "tile")
SLAB = AXES[1:4]
MESH = pl.DeviceIdType.MESH
ANY = pl.BlockSpec(memory_space=pl.ANY)
VM = pl.BlockSpec(memory_space=pltpu.VMEM)


class Place(NamedTuple):
    dir: int
    sy: int
    sx: int
    sz: int
    tile: int


def places():
    return Place(*[lax.axis_index(a) for a in AXES])


def slab_index(me):
    _, _, sx, sz, _ = (lax.axis_size(a) for a in AXES)
    return (me.sy * sx + me.sx) * sz + me.sz


def at_slab(me, step):
    sy, sx, sz = (lax.axis_size(a) for a in SLAB)
    s = lax.rem(slab_index(me) + step + sy * sx * sz, sy * sx * sz)
    return me._replace(sy=s // (sx * sz), sx=(s // sz) % sx, sz=s % sz)


def greet(peers):
    barrier = pltpu.get_barrier_semaphore()
    for peer in peers:
        pl.semaphore_signal(barrier, inc=1, device_id=tuple(peer), device_id_type=MESH)
    return lambda: pl.semaphore_wait(barrier, len(peers))


def push(src, dst, send, recv, peer):
    return pltpu.make_async_remote_copy(
        src_ref=src, dst_ref=dst, send_sem=send, recv_sem=recv,
        device_id=tuple(peer), device_id_type=MESH,
    )


def shapes(ch, planes, rows, half, wide, nz, ng):
    lanes, m = 4 * rows, half // 8 // nz
    ext = planes + 2
    f32 = jnp.float32
    one = dict(
        grid=(ch, ext, rows, half), wing=(ch, ext, rows, wide),
        rows=(ch, planes, 8, half), rwing=(ch, planes, 8, wide),
        cut=(2, rows, wide), rcut=(2, rows, wide), brim=(2, ch, half + wide),
        rbrim=(2, ch, half + wide),
        plane=(2, ch, ext, rows, half), sigma=(2, planes, rows, half),
        slope=(2, planes, rows, half), colour=(2, 3, planes, rows, half),
        through=(2, planes, rows, half), glow=(2, planes, rows, half),
        taps=(2, 9, rows, half), pair=(2, 7, rows, half),
        codes=(2, rows, half), heading=(2, rows, half), pull=(2, 3, rows, half),
        ahead=(2, planes, rows, half), stack=(lanes, half),
        diff=(2, ch, planes + 4, rows, half), out=(ch, ext, rows, half),
        line=(ext, ch, half), inpack=(SIDE, SIDE), zpack=(SIDE, SIDE),
        inturn=(SIDE, SIDE), zturn=(SIDE, SIDE),
        fp=(ch, rows, half), fn=(ch, rows, half),
        rline=(planes, ch, half), zline=(2, ch, half), rin=(ch * planes, SIDE),
        rfar=(8, SIDE), rzin=(2, 8, SIDE), rzfar=(2, 8, SIDE),
        tile=(wide, lanes),
        dl=(nz, m, 8, lanes), im=(nz, 2, m, 8, lanes), hd=(nz, m, 8, lanes),
        rdl=(nz, m, 8, lanes), rim=(nz, 2, m, 8, lanes), gm=(ng, m, 8, lanes),
        ret=(nz, m, 8, lanes), rb=(nz, m, 8, lanes),
        part=(2, m, 8, lanes), rpart=(ng, 8, lanes),
    )
    ints = dict(codes=0, heading=0)
    return {k: pltpu.VMEM(v, jnp.int32 if k in ints else f32) for k, v in one.items()}


def weights(b, g):
    level = LEVELS
    q = b.codes[g]
    frac = lambda raw: (raw.astype(jnp.float32) + 0.5) / level - 0.5
    fz, fy, fx = frac(q & 7), frac((q >> 3) & 7), frac(q >> 6)
    three = lambda f: (jnp.maximum(-f, 0.0), 1.0 - jnp.abs(f), jnp.maximum(f, 0.0))
    wy, wx = three(fy), three(fx)
    for i in range(3):
        for j in range(3):
            b.taps[g, 3 * i + j] = wy[i] * wx[j]
    ay, ax = jnp.abs(fy), jnp.abs(fx)
    for i, v in enumerate((fz, fy, fx, wy[1] * wx[1], wy[1] * ax, ay * wx[1], ay * ax)):
        b.pair[g, i] = v


def iota(shape, dim):
    return lax.broadcasted_iota(jnp.int32, shape, dim)


def lane_of(d, r):
    return jnp.where(d == 0, r[..., 0:1], r[..., r.shape[-1] - 1:])


def inner_edges(b, me, p):
    rows, wide = b.wing.shape[2:]
    d, t = me.dir, me.tile
    fr = lambda r: jnp.where(t == 0, r[0:1], r[7:8])

    def edges(c):
        edge = jnp.broadcast_to(lane_of(d, b.wing[c, p]), (rows, wide))
        far = fr(b.rows[c, p - 1])
        return edge, far, jnp.broadcast_to(lane_of(d, fr(b.rwing[c, p - 1])), (1, wide))

    return edges


def outer_edges(b, me, i):
    rows, wide = b.wing.shape[2:]
    half = b.grid.shape[3]

    def edges(c):
        edge = jnp.broadcast_to(b.rcut[i][:, c:c + 1], (rows, wide))
        line = b.rbrim[i, c:c + 1, :]
        return edge, line[:, :half], jnp.broadcast_to(lane_of(me.dir, line[:, half:]), (1, wide))

    return edges


def cut_faces(b, me):
    ch, ext, rows, half = b.grid.shape
    wide = b.wing.shape[3]
    slot = iota((rows, wide), 1)
    for i, p in enumerate((ext - 2, 1)):
        acc = jnp.zeros((rows, wide), jnp.float32)
        for c in range(ch):
            acc = jnp.where(slot == c, jnp.broadcast_to(lane_of(me.dir, b.wing[c, p]), (rows, wide)), acc)
            pick = lambda r: jnp.where(me.tile == 0, r[rows - 1:rows], r[0:1])
            b.brim[i, c:c + 1, :half] = pick(b.grid[c, p])
            b.brim[i, c:c + 1, half:] = pick(b.wing[c, p])
        b.cut[i] = acc


def sample_plane(b, me, p, gs, edges, keep):
    ch, _, rows, half = b.grid.shape
    tw = half // 2
    d, t = me.dir, me.tile
    row, lane = iota((rows, tw), 0), iota((rows, tw), 1)
    right = (d == 0).astype(jnp.float32)
    left = 1.0 - right
    under = (t == 0).astype(jnp.float32)
    over = 1.0 - under
    for c in range(ch):
        edge, line, corner = edges(c)
        m = [b.grid[c, p, :, x * tw:(x + 1) * tw] for x in range(2)] + [edge]
        far = [line[:, :tw], line[:, tw:], corner]
        up = [jnp.where(row == 0, f * over, pltpu.roll(a, 1, 0)) for a, f in zip(m, far)]
        dn = [jnp.where(row == rows - 1, f * under, pltpu.roll(a, rows - 1, 0))
              for a, f in zip(m, far)]
        spread = []
        for a in (up, m, dn):
            r = [pltpu.roll(a[x], 1, 1) for x in range(2)]
            l = [pltpu.roll(a[x], tw - 1, 1) for x in range(2)]
            lo = [jnp.where(lane == 0, a[2] * left, r[0]), jnp.where(lane == 0, r[0], r[1])]
            hi = [jnp.where(lane == tw - 1, l[1], l[0]),
                  jnp.where(lane == tw - 1, a[2] * right, l[1])]
            spread.append((lo, a[:2], hi))
        for x in range(2):
            at = slice(x * tw, (x + 1) * tw)
            for g in gs:
                fy, fx = b.pair[g, 1, :, at], b.pair[g, 2, :, at]
                w00, w01 = b.pair[g, 3, :, at], b.pair[g, 4, :, at]
                w10, w11 = b.pair[g, 5, :, at], b.pair[g, 6, :, at]
                side = lambda s: jnp.where(fx > 0, s[2][x], s[0][x])
                down = fy > 0
                v = (w00 * m[x] + w01 * side(spread[1])
                     + w10 * jnp.where(down, dn[x], up[x])
                     + w11 * jnp.where(down, side(spread[2]), side(spread[0])))
                b.plane[g, c, p, :, at] = v if keep is None else v * keep


def shade_planes(b, scale):
    _, ch, ext, rows, half = b.plane.shape
    planes = ext - 2

    def step(k, acc):
        new = []
        for g in range(2):
            fz = b.pair[g, 0]
            az = jnp.abs(fz)
            v = []
            for c in range(ch):
                mid = b.plane[g, c, k + 1]
                far = jnp.where(fz > 0, b.plane[g, c, k + 2], b.plane[g, c, k])
                v.append((1.0 - az) * mid + az * far)
            sg = (jnp.maximum(v[0], 0.0) + jnp.log(1.0 + jnp.exp(-jnp.abs(v[0])))) * scale
            b.sigma[g, k] = sg
            b.slope[g, k] = (0.5 + 0.5 * jnp.tanh(0.5 * v[0])) * scale
            for c in range(3):
                b.colour[g, c, k] = 0.5 + 0.5 * jnp.tanh(0.5 * v[c + 1])
            b.ahead[g, k] = acc[g]
            new.append(acc[g] + sg)
        return tuple(new)

    zero = jnp.zeros((rows, half), jnp.float32)
    return lax.fori_loop(0, planes, step, (zero, zero))


def local_light(b, totals):
    _, planes, rows, half = b.sigma.shape
    images = []
    for g in range(2):
        forward = b.heading[g] == 0

        def step(k, acc):
            sg, ah = b.sigma[g, k], b.ahead[g, k]
            front = jnp.where(forward, ah, totals[g] - ah - sg)
            th = jnp.exp(-front)
            gl = th * (1.0 - jnp.exp(-sg))
            b.through[g, k] = th
            b.glow[g, k] = gl
            return tuple(acc[c] + gl * b.colour[g, c, k] for c in range(3))

        zero = jnp.zeros((rows, half), jnp.float32)
        images.append(lax.fori_loop(0, planes, step, (zero,) * 3))
    return images


def tiles_out(b, put, nz):
    lanes, half = b.stack.shape
    tw = half // 2
    for x in range(2):
        turned = b.stack[:, x * tw:(x + 1) * tw].T
        for i in range(tw // 8):
            j = x * (tw // 8) + i
            put(j % nz, j // nz, turned[8 * i:8 * i + 8])


def backward(b, kept):
    _, planes, rows, half = b.sigma.shape
    zero = jnp.zeros((rows, half), jnp.float32)
    for g in range(2):
        forward = b.heading[g] == 0
        reach = b.stack[2 * g * rows:(2 * g + 1) * rows]
        rest = b.stack[(2 * g + 1) * rows:(2 * g + 2) * rows]
        whole = reach * kept[g]
        for c in range(4):
            for k in (0, 1, planes + 2, planes + 3):
                b.diff[g, c, k] = zero

        def step(k, before):
            pull = [b.pull[g, c] for c in range(3)]
            col = [b.colour[g, c, k] for c in range(3)]
            shade = pull[0] * col[0] + pull[1] * col[1] + pull[2] * col[2]
            th, gl = b.through[g, k], b.glow[g, k]
            lit = reach * gl
            share = lit * shade
            behind = rest + jnp.where(forward, whole - before - share, before)
            b.diff[g, 0, k + 2] = (reach * (th - gl) * shade - behind) * b.slope[g, k]
            for c in range(3):
                b.diff[g, c + 1, k + 2] = pull[c] * lit * (col[c] * (1.0 - col[c]))
            return before + share

        lax.fori_loop(0, planes, step, zero)


def spill_plane(b, me, p, pack, place):
    ch, ext, rows, half = b.out.shape
    tw = half // 2
    d, t = me.dir, me.tile
    row, lane = iota((rows, tw), 0), iota((rows, tw), 1)
    for c in range(ch):
        cols = []
        for g in range(2):
            fz = b.pair[g, 0]
            cols.append((1.0 - jnp.abs(fz)) * b.diff[g, c, p + 1]
                        + jnp.maximum(fz, 0.0) * b.diff[g, c, p]
                        + jnp.maximum(-fz, 0.0) * b.diff[g, c, p + 2])
        bands = []
        for i in range(3):
            u = []
            for j in range(3):
                full = (b.taps[0, 3 * i + j] * cols[0] + b.taps[1, 3 * i + j] * cols[1])
                u.append([full[:, :tw], full[:, tw:]])
            l = [pltpu.roll(a, tw - 1, 1) for a in u[0]]
            r = [pltpu.roll(a, 1, 1) for a in u[2]]
            x0 = u[1][0] + jnp.where(lane == tw - 1, l[1], l[0]) + jnp.where(lane == 0, 0.0, r[0])
            x1 = u[1][1] + jnp.where(lane == tw - 1, 0.0, l[1]) + jnp.where(lane == 0, r[0], r[1])
            bands.append([x0, x1, jnp.where(d == 0, r[1], u[0][0])])
        done, far = [], []
        for x in range(3):
            up = pltpu.roll(bands[0][x], rows - 1, 0)
            dn = pltpu.roll(bands[2][x], 1, 0)
            done.append(bands[1][x] + jnp.where(row == rows - 1, 0.0, up)
                        + jnp.where(row == 0, 0.0, dn))
            far.append(jnp.where(t == 0, dn[0:1], up[rows - 1:rows]))
        b.out[c, p, :, :tw] = done[0]
        b.out[c, p, :, tw:] = done[1]
        b.line[p, c:c + 1, :tw] = far[0]
        b.line[p, c:c + 1, tw:] = far[1]
        slot = iota((rows, SIDE), 1)
        pos = place(c)
        pack[:rows] = jnp.where(
            slot == pos, jnp.broadcast_to(done[2][:, 0:1], (rows, SIDE)), pack[:rows])
        pack[rows:rows + 1] = jnp.where(
            slot[0:1] == pos, jnp.broadcast_to(far[2][:, 0:1], (1, SIDE)), pack[rows:rows + 1])


def gather_spill(b, me, has_prev, has_next, dest):
    ch, ext, rows, half = b.out.shape
    planes = ext - 2
    tw = half // 2
    d, t = me.dir, me.tile
    touch = (1 - t) * (rows - 1)
    seam = (1 - d) * (half - 1)
    row = iota((rows, tw), 0)
    lane = iota((rows, tw), 1)
    spot = iota((1, SIDE), 1)
    b.inturn[:ch * planes] = b.rin[...]
    for c in range(ch):
        for k, i, r, has in ((0, 0, ch + c, has_prev), (planes - 1, 1, c, has_next)):
            far = jnp.broadcast_to(b.rzfar[i, r:r + 1, rows:rows + 1], (1, SIDE))
            add = jnp.where(spot < rows, b.rzin[i, r:r + 1], 0.0) + jnp.where(spot == touch, far, 0.0)
            j = c * planes + k
            b.inturn[j:j + 1] = b.inturn[j:j + 1] + add * has
    col = b.inturn[...].T[:rows]
    col = col + jnp.where(iota((rows, SIDE), 0) == touch, jnp.broadcast_to(b.rfar[0:1], (rows, SIDE)), 0.0)
    for c in range(ch):
        for k in range(planes):
            pos = c * planes + k
            extra = b.rline[k, c:c + 1]
            v = b.out[c, k + 1]
            if k == 0:
                extra = extra + b.zline[0, c:c + 1] * has_prev
                v = v + b.fp[c] * has_prev
            if k == planes - 1:
                extra = extra + b.zline[1, c:c + 1] * has_next
                v = v + b.fn[c] * has_next
            bar = jnp.broadcast_to(col[:, pos:pos + 1], (rows, tw))
            for x in range(2):
                at = slice(x * tw, (x + 1) * tw)
                y = v[:, at] + jnp.where(row == touch, jnp.broadcast_to(extra[:, at], (rows, tw)), 0.0)
                y = y + jnp.where(lane + x * tw == seam, bar, 0.0)
                dest[c, k, :, at] = y


def render_kernel(scale, depth, names, vox, codes, head, cot, grad, img, *scratch):
    b = SimpleNamespace(**dict(zip(names, scratch)))
    sems = scratch[len(names):]
    (lsem, hs, hr, s1, r1, s2, r2, s3, r3, s4, r4, s5, r5, ss, sr) = sems
    me = places()
    nsy, nsx, nz = (lax.axis_size(a) for a in SLAB)
    ng = nsy * nsx
    blocks = ng // 2
    d, t, z = me.dir, me.tile, me.sz
    gi = me.sy * nsx + me.sx
    s = slab_index(me)
    prev, nxt = at_slab(me, -1), at_slab(me, 1)
    flip = lambda p: p._replace(tile=1 - p.tile)
    over = lambda p: p._replace(dir=1 - p.dir)
    near = [prev, me, nxt]
    mate = me._replace(dir=1 - d, sx=nsx - 1 - me.sx)
    ch, ext, rows, half = b.grid.shape
    planes = ext - 2
    wide = b.wing.shape[-1]
    has_prev = (s > 0).astype(jnp.float32)
    has_next = (s < nsy * nsx * nz - 1).astype(jnp.float32)

    mine = pl.ds(pl.multiple_of(d * half, half), half)
    theirs = pl.ds(pl.multiple_of((1 - d) * half, half), half)
    beside = pl.ds(pl.multiple_of(half - d * wide, wide), wide)
    loads = [
        (vox.at[:, :, :, mine], b.grid.at[:, 1:planes + 1]),
        (vox.at[:, :, :, beside], b.wing.at[:, 1:planes + 1]),
        (codes.at[0, :, mine], b.codes.at[0]),
        (head.at[0, :, mine], b.heading.at[0]),
        (cot.at[0, :, :, mine], b.pull.at[0]),
    ]
    loads = [pltpu.make_async_copy(a, c, lsem.at[i]) for i, (a, c) in enumerate(loads)]
    for c in loads:
        c.start()

    zpeer = [me._replace(sz=lax.rem(z + i, nz)) for i in range(1, nz)]
    gpeer, across = [], []
    for i in range(ng):
        g = lax.rem(gi + i, ng)
        p = me._replace(sy=g // nsx, sx=g % nsx)
        across.append(over(p))
        if i:
            gpeer.append(p)
    ready = greet([prev, nxt] + [flip(p) for p in near] + [over(p) for p in near]
          + [over(flip(p)) for p in near] + zpeer + gpeer + across)

    for c in loads[:2]:
        c.wait()
    cut_faces(b, me)
    for c in loads[2:]:
        c.wait()
    weights(b, 0)
    ready()
    rays = [
        (codes.at[0, :, theirs], b.codes.at[1], mate),
        (head.at[0, :, theirs], b.heading.at[1], mate),
        (cot.at[0, :, :, theirs], b.pull.at[1], mate),
    ]
    rays = [push(x, y, hs.at[i], hr.at[i], p) for i, (x, y, p) in enumerate(rays)]
    for c in rays:
        c.start()
    edge = pl.ds(pl.multiple_of((1 - t) * (rows - 8), 8), 8)
    inner = pl.ds(1, planes)
    beyond = [
        (b.grid.at[:, inner, edge], b.rows, flip(me)),
        (b.wing.at[:, inner, edge], b.rwing, flip(me)),
        (b.cut.at[0], b.rcut.at[0], nxt),
        (b.cut.at[1], b.rcut.at[1], prev),
        (b.brim.at[0], b.rbrim.at[0], flip(nxt)),
        (b.brim.at[1], b.rbrim.at[1], flip(prev)),
        (b.grid.at[:, planes], b.grid.at[:, 0], nxt),
        (b.grid.at[:, 1], b.grid.at[:, ext - 1], prev),
    ]
    beyond = [push(x, y, hs.at[3 + i], hr.at[3 + i], p) for i, (x, y, p) in enumerate(beyond)]
    for c in beyond:
        c.start()
    for c in beyond[:2]:
        c.wait()

    def inside(gs):
        def step(p, carry):
            sample_plane(b, me, p, gs, inner_edges(b, me, p), None)
            return carry

        lax.fori_loop(1, planes + 1, step, 0)

    inside((0,))
    rays[0].wait()
    weights(b, 1)
    inside((1,))
    for c in beyond[2:]:
        c.wait()

    def ends(i, carry):
        sample_plane(b, me, i * (ext - 1), (0, 1), outer_edges(b, me, i),
                     jnp.where(i == 0, has_prev, has_next))
        return carry

    lax.fori_loop(0, 2, ends, 0)
    totals = shade_planes(b, scale)
    for c in rays[1:]:
        c.wait()
    for g in range(2):
        for c in range(3):
            b.pull[g, c] = b.pull[g, c] * depth
    images = local_light(b, totals)
    kept = []
    for g in range(2):
        kept.append(sum(b.pull[g, c] * images[g][c] for c in range(3)))
        b.stack[2 * g * rows:(2 * g + 1) * rows] = totals[g]
        b.stack[(2 * g + 1) * rows:(2 * g + 2) * rows] = kept[g]

    def put_dl(j, m, v):
        b.dl[j, m] = v

    tiles_out(b, put_dl, nz)
    first = [push(b.dl.at[p.sz], b.rdl.at[z], s1.at[i], r1.at[i], p)
             for i, p in enumerate(zpeer)]
    for c in first:
        c.start()
    for g in range(2):
        for c in range(3):
            b.stack[c * rows:(c + 1) * rows] = images[g][c]

        def put_im(j, m, v):
            b.im[j, g, m] = v

        tiles_out(b, put_im, nz)
    late = [push(b.im.at[p.sz], b.rim.at[z], s2.at[i], r2.at[i], p)
            for i, p in enumerate(zpeer)]
    for c in late:
        c.start()
    for g in range(2):
        for i in range(2):
            b.stack[(2 * g + i) * rows:(2 * g + i + 1) * rows] = b.heading[g].astype(jnp.float32)

    def put_hd(j, m, v):
        b.hd[j, m] = v

    tiles_out(b, put_hd, nz)
    b.rdl[z] = b.dl[z]
    b.rim[z] = b.im[z]
    lanes = b.dl.shape[-1]
    ahead = b.hd[z] == 0
    spot = iota(ahead.shape, 2)
    is_d = (spot // rows) % 2 == 0
    for c in first:
        c.wait()
    roll = lambda a, n: pltpu.roll(a, n % lanes, 2)

    def directed(parts):
        lows, low = [], jnp.zeros_like(parts[0])
        for p in parts:
            lows.append(low)
            low = low + p
        highs, high = [], jnp.zeros_like(parts[0])
        for p in reversed(parts):
            highs.append(high)
            high = high + p
        highs = highs[::-1]
        before = [jnp.where(ahead, x, y) for x, y in zip(lows, highs)]
        after = [jnp.where(ahead, y, x) for x, y in zip(lows, highs)]
        return before, after, low

    tiles = [b.rdl[i] for i in range(nz)]
    before, _, dsum = directed(tiles)
    reach = [jnp.exp(-x) for x in before]
    pulled = [roll(r, rows) * x for r, x in zip(reach, tiles)]
    _, behind, lsum = directed(pulled)
    b.gm[gi] = jnp.where(is_d, dsum, lsum)
    second = [push(b.gm.at[gi], b.gm.at[gi], s3.at[i], r3.at[i], p)
              for i, p in enumerate(gpeer)]
    for c in second:
        c.start()
    for c in second:
        c.wait()
    groups = [b.gm[i] for i in range(ng)]
    gbefore, _, _ = directed(groups)
    greach = [jnp.exp(-x) for x in gbefore]
    gpull = [roll(r, rows) * x for r, x in zip(greach, groups)]
    _, gafter, _ = directed(gpull)
    to_me = jnp.zeros_like(dsum)
    rest = jnp.zeros_like(dsum)
    for i in range(ng):
        to_me = jnp.where(gi == i, greach[i], to_me)
        rest = jnp.where(gi == i, gafter[i], rest)
    to_me_l = roll(to_me, rows)
    full = []
    for i in range(nz):
        r = to_me * reach[i]
        full.append(r)
        b.ret[i] = jnp.where(is_d, r, rest + to_me_l * behind[i])
    back = [push(b.ret.at[p.sz], b.rb.at[z], s4.at[i], r4.at[i], p)
            for i, p in enumerate(zpeer)]
    for c in back:
        c.start()
    b.rb[z] = b.ret[z]
    for c in late:
        c.wait()
    quarter = spot // rows
    for g in range(2):
        total = jnp.zeros_like(dsum)
        for i in range(nz):
            src = full[i]
            wash = roll(src, -2 * g * rows)
            wash = jnp.where(quarter == 1, roll(src, (1 - 2 * g) * rows), wash)
            wash = jnp.where(quarter == 2, roll(src, (2 - 2 * g) * rows), wash)
            total = total + wash * b.rim[i, g]
        b.part[g] = total
    half_of_me = gi // blocks
    out = []
    for g in range(2):
        for m in range(blocks):
            q = blocks * d + m
            peer = me._replace(dir=d if g == 0 else 1 - d, sy=q // nsx, sx=q % nsx)
            out.append(push(b.part.at[g, m], b.rpart.at[gi],
                            s5.at[g * blocks + m], r5.at[gi], peer))
    for g in range(2):
        for m in range(blocks):
            copy = out[g * blocks + m]
            if g == 0:
                itself = gi == blocks * d + m

                @pl.when(itself)
                def _():
                    b.rpart[gi] = b.part[0, m]

                @pl.when(jnp.logical_not(itself))
                def _():
                    copy.start()
            else:
                copy.start()
    for c in back:
        c.wait()

    tw = half // 2
    for x in range(2):
        for i in range(tw // 8):
            j = x * (tw // 8) + i
            b.tile[8 * i:8 * i + 8] = b.rb[j % nz, j // nz]
        b.stack[:, x * tw:(x + 1) * tw] = b.tile[...].T
    backward(b, kept)

    def spread_ends(i, carry):
        spill_plane(b, me, i * (ext - 1), b.zpack, lambda c: i * ch + c)
        return carry

    lax.fori_loop(0, 2, spread_ends, 0)
    b.zturn[...] = b.zpack[...].T
    spill = [
        (b.out.at[:, ext - 1], b.fp, nxt), (b.out.at[:, 0], b.fn, prev),
        (b.line.at[ext - 1], b.zline.at[0], flip(nxt)), (b.line.at[0], b.zline.at[1], flip(prev)),
    ]
    small = b.zturn.at[0:8]
    for i, p in enumerate((nxt, prev)):
        spill.append((small, b.rzin.at[i], over(p)))
        spill.append((small, b.rzfar.at[i], over(flip(p))))
    spill = [push(x, y, ss.at[i], sr.at[i], p) for i, (x, y, p) in enumerate(spill)]
    for c in spill:
        c.start()

    def spread(p, carry):
        spill_plane(b, me, p, b.inpack, lambda c: c * planes + p - 1)
        return carry

    lax.fori_loop(1, planes + 1, spread, 0)
    b.inturn[...] = b.inpack[...].T
    last = [
        (b.inturn.at[0:ch * planes], b.rin, over(me)),
        (b.inpack.at[rows:rows + 8], b.rfar, over(flip(me))),
        (b.line.at[inner], b.rline, flip(me)),
    ]
    last = [push(x, y, ss.at[8 + i], sr.at[8 + i], p) for i, (x, y, p) in enumerate(last)]
    for c in last:
        c.start()
    spill = spill + last

    for g in range(2):
        for m in range(blocks):
            copy = out[g * blocks + m]
            if g == 0:
                @pl.when(gi != blocks * d + m)
                def _():
                    copy.wait_send()
            else:
                copy.wait_send()
    for i in range(ng):
        arrive = push(b.part.at[0, 0], b.rpart.at[i], s5.at[0], r5.at[i], over(me))

        @pl.when(jnp.logical_or(half_of_me != d, gi != i))
        def _():
            arrive.wait_recv()
    total = b.rpart[0]
    for i in range(1, ng):
        total = total + b.rpart[i]
    img[...] = total
    for c in spill:
        c.wait()
    gather_spill(b, me, has_prev, has_next, grad)


def finish_kernel(rows, src, img, dst, image):
    dst[...] = src[...]
    for c in range(3):
        image[c] = img[:, c * rows:(c + 1) * rows]


def per_device(voxels, offsets, heading, cotangent):
    ch, planes, rows, total = voxels.shape
    nsy, nsx, nz = (lax.axis_size(a) for a in SLAB)
    ng = nsy * nsx
    depth = planes * nz * ng
    half = total // 2
    wide = half // 2
    room = shapes(ch, planes, rows, half, wide, nz, ng)
    dma = lambda n: pltpu.SemaphoreType.DMA((n,))
    grad, img = pl.pallas_call(
        functools.partial(render_kernel, 2.0 / depth, float(depth), tuple(room)),
        out_shape=(jax.ShapeDtypeStruct((ch, planes, rows, half), jnp.float32),
                   jax.ShapeDtypeStruct((8, 4 * rows), jnp.float32)),
        in_specs=[ANY] * 4,
        out_specs=(VM, VM),
        scratch_shapes=list(room.values()) + [
            dma(5), dma(11), dma(11),
            dma(nz - 1), dma(nz - 1), dma(nz - 1), dma(nz - 1),
            dma(ng - 1), dma(ng - 1), dma(nz - 1), dma(nz - 1),
            dma(ng), dma(ng), dma(11), dma(11),
        ],
        compiler_params=pltpu.CompilerParams(
            collective_id=0, has_side_effects=True, vmem_limit_bytes=60 * 1024 * 1024
        ),
    )(voxels, offsets, heading, cotangent)
    shape = grad.shape
    block = pl.BlockSpec((1,) + shape[1:], lambda c: (c, 0, 0, 0))
    grad, image = pl.pallas_call(
        functools.partial(finish_kernel, rows),
        grid=(ch,),
        out_shape=(jax.ShapeDtypeStruct(shape, jnp.float32),
                   jax.ShapeDtypeStruct((3, 8, rows), jnp.float32)),
        in_specs=[block, pl.BlockSpec(img.shape, lambda c: (0, 0))],
        out_specs=(block, pl.BlockSpec((3, 8, rows), lambda c: (0, 0, 0))),
    )(grad, img)
    image = jnp.swapaxes(image, 1, 2)[None]
    return (image, grad)


def solution(mesh):
    n = mesh.devices.size
    shape = (2, 4, 2, 8, 2) if n == 256 else (2, 2, 1, 2, 2)
    finer = Mesh(mesh.devices.reshape(shape), AXES)
    return jax.shard_map(
        per_device,
        mesh=finer,
        in_specs=(
            P(None, SLAB, "tile", None),
            P("dir", "tile", None),
            P("dir", "tile", None),
            P("dir", None, "tile", None),
        ),
        out_specs=(P("dir", None, "tile", SLAB), P(None, SLAB, "tile", "dir")),
        check_vma=False,
    )
```

```python
import functools
from types import SimpleNamespace
from typing import NamedTuple

import jax
import jax.numpy as jnp
from jax import lax
from jax.experimental import pallas as pl
from jax.experimental.pallas import tpu as pltpu
from jax.sharding import Mesh
from jax.sharding import PartitionSpec as P

LEVELS = 8
SIDE = 128
AXES = ("dir", "sy", "sx", "sz", "tile")
SLAB = AXES[1:4]
MESH = pl.DeviceIdType.MESH
HBM = pl.BlockSpec(memory_space=pltpu.HBM)
VM = pl.BlockSpec(memory_space=pltpu.VMEM)


class Place(NamedTuple):
    dir: int
    sy: int
    sx: int
    sz: int
    tile: int


def places():
    return Place(*[lax.axis_index(a) for a in AXES])


def slab_index(me):
    _, _, sx, sz, _ = (lax.axis_size(a) for a in AXES)
    return (me.sy * sx + me.sx) * sz + me.sz


def at_slab(me, step):
    sy, sx, sz = (lax.axis_size(a) for a in SLAB)
    s = lax.rem(slab_index(me) + step + sy * sx * sz, sy * sx * sz)
    return me._replace(sy=s // (sx * sz), sx=(s // sz) % sx, sz=s % sz)


def greet(peers):
    barrier = pltpu.get_barrier_semaphore()
    for peer in peers:
        pl.semaphore_signal(barrier, inc=1, device_id=tuple(peer), device_id_type=MESH)
    return lambda: pl.semaphore_wait(barrier, len(peers))


def push(src, dst, send, recv, peer):
    return pltpu.make_async_remote_copy(
        src_ref=src, dst_ref=dst, send_sem=send, recv_sem=recv,
        device_id=tuple(peer), device_id_type=MESH,
    )


def shapes(ch, planes, rows, half, wide, nz, ng):
    lanes, m = 4 * rows, half // 8 // nz
    ext = planes + 2
    f32 = jnp.float32
    one = dict(
        grid=(ch, ext, rows, half), wing=(ch, ext, rows, wide),
        rows=(ch, planes, 8, half), rwing=(ch, planes, 8, wide),
        cut=(2, rows, wide), rcut=(2, rows, wide), brim=(2, ch, half + wide),
        rbrim=(2, ch, half + wide),
        plane=(2, ch, ext, rows, half), sigma=(2, planes, rows, half),
        slope=(2, planes, rows, half), colour=(2, 3, planes, rows, half),
        through=(2, planes, rows, half), glow=(2, planes, rows, half),
        taps=(2, 9, rows, half), pair=(2, 7, rows, half),
        codes=(2, rows, half), heading=(2, rows, half), pull=(2, 3, rows, half),
        ahead=(2, planes, rows, half), stack=(lanes, half),
        diff=(2, ch, planes + 4, rows, half), out=(ch, ext, rows, half),
        line=(ext, ch, half), inpack=(SIDE, SIDE), zpack=(SIDE, SIDE),
        inturn=(SIDE, SIDE), zturn=(SIDE, SIDE),
        fp=(ch, rows, half), fn=(ch, rows, half),
        rline=(planes, ch, half), zline=(2, ch, half), rin=(ch * planes, SIDE),
        rfar=(8, SIDE), rzin=(2, 8, SIDE), rzfar=(2, 8, SIDE),
        tile=(wide, lanes),
        dl=(nz, m, 8, lanes), im=(nz, 2, m, 8, lanes), hd=(nz, m, 8, lanes),
        rdl=(nz, m, 8, lanes), rim=(nz, 2, m, 8, lanes), gm=(ng, m, 8, lanes),
        ret=(nz, m, 8, lanes), rb=(nz, m, 8, lanes),
        part=(2, m, 8, lanes), rpart=(ng, 8, lanes),
    )
    ints = dict(codes=0, heading=0)
    return {k: pltpu.VMEM(v, jnp.int32 if k in ints else f32) for k, v in one.items()}


def weights(b, g):
    level = LEVELS
    q = b.codes[g]
    frac = lambda raw: (raw.astype(jnp.float32) + 0.5) / level - 0.5
    fz, fy, fx = frac(q & 7), frac((q >> 3) & 7), frac(q >> 6)
    three = lambda f: (jnp.maximum(-f, 0.0), 1.0 - jnp.abs(f), jnp.maximum(f, 0.0))
    wy, wx = three(fy), three(fx)
    for i in range(3):
        for j in range(3):
            b.taps[g, 3 * i + j] = wy[i] * wx[j]
    ay, ax = jnp.abs(fy), jnp.abs(fx)
    for i, v in enumerate((fz, fy, fx, wy[1] * wx[1], wy[1] * ax, ay * wx[1], ay * ax)):
        b.pair[g, i] = v


def iota(shape, dim):
    return lax.broadcasted_iota(jnp.int32, shape, dim)


def lane_of(d, r):
    return jnp.where(d == 0, r[..., 0:1], r[..., r.shape[-1] - 1:])


def inner_edges(b, me, p):
    rows, wide = b.wing.shape[2:]
    d, t = me.dir, me.tile
    fr = lambda r: jnp.where(t == 0, r[0:1], r[7:8])

    def edges(c):
        edge = jnp.broadcast_to(lane_of(d, b.wing[c, p]), (rows, wide))
        far = fr(b.rows[c, p - 1])
        return edge, far, jnp.broadcast_to(lane_of(d, fr(b.rwing[c, p - 1])), (1, wide))

    return edges


def outer_edges(b, me, i):
    rows, wide = b.wing.shape[2:]
    half = b.grid.shape[3]

    def edges(c):
        edge = jnp.broadcast_to(b.rcut[i][:, c:c + 1], (rows, wide))
        line = b.rbrim[i, c:c + 1, :]
        return edge, line[:, :half], jnp.broadcast_to(lane_of(me.dir, line[:, half:]), (1, wide))

    return edges


def cut_faces(b, me):
    ch, ext, rows, half = b.grid.shape
    wide = b.wing.shape[3]
    slot = iota((rows, wide), 1)
    for i, p in enumerate((ext - 2, 1)):
        acc = jnp.zeros((rows, wide), jnp.float32)
        for c in range(ch):
            acc = jnp.where(slot == c, jnp.broadcast_to(lane_of(me.dir, b.wing[c, p]), (rows, wide)), acc)
            pick = lambda r: jnp.where(me.tile == 0, r[rows - 1:rows], r[0:1])
            b.brim[i, c:c + 1, :half] = pick(b.grid[c, p])
            b.brim[i, c:c + 1, half:] = pick(b.wing[c, p])
        b.cut[i] = acc


def sample_plane(b, me, p, gs, edges, keep):
    ch, _, rows, half = b.grid.shape
    tw = half // 2
    d, t = me.dir, me.tile
    row, lane = iota((rows, tw), 0), iota((rows, tw), 1)
    right = (d == 0).astype(jnp.float32)
    left = 1.0 - right
    under = (t == 0).astype(jnp.float32)
    over = 1.0 - under
    for c in range(ch):
        edge, line, corner = edges(c)
        m = [b.grid[c, p, :, x * tw:(x + 1) * tw] for x in range(2)] + [edge]
        far = [line[:, :tw], line[:, tw:], corner]
        up = [jnp.where(row == 0, f * over, pltpu.roll(a, 1, 0)) for a, f in zip(m, far)]
        dn = [jnp.where(row == rows - 1, f * under, pltpu.roll(a, rows - 1, 0))
              for a, f in zip(m, far)]
        spread = []
        for a in (up, m, dn):
            r = [pltpu.roll(a[x], 1, 1) for x in range(2)]
            l = [pltpu.roll(a[x], tw - 1, 1) for x in range(2)]
            lo = [jnp.where(lane == 0, a[2] * left, r[0]), jnp.where(lane == 0, r[0], r[1])]
            hi = [jnp.where(lane == tw - 1, l[1], l[0]),
                  jnp.where(lane == tw - 1, a[2] * right, l[1])]
            spread.append((lo, a[:2], hi))
        for x in range(2):
            at = slice(x * tw, (x + 1) * tw)
            for g in gs:
                fy, fx = b.pair[g, 1, :, at], b.pair[g, 2, :, at]
                w00, w01 = b.pair[g, 3, :, at], b.pair[g, 4, :, at]
                w10, w11 = b.pair[g, 5, :, at], b.pair[g, 6, :, at]
                side = lambda s: jnp.where(fx > 0, s[2][x], s[0][x])
                down = fy > 0
                v = (w00 * m[x] + w01 * side(spread[1])
                     + w10 * jnp.where(down, dn[x], up[x])
                     + w11 * jnp.where(down, side(spread[2]), side(spread[0])))
                b.plane[g, c, p, :, at] = v if keep is None else v * keep


def shade_planes(b, scale):
    _, ch, ext, rows, half = b.plane.shape
    planes = ext - 2

    def step(k, acc):
        new = []
        for g in range(2):
            fz = b.pair[g, 0]
            az = jnp.abs(fz)
            v = []
            for c in range(ch):
                mid = b.plane[g, c, k + 1]
                far = jnp.where(fz > 0, b.plane[g, c, k + 2], b.plane[g, c, k])
                v.append((1.0 - az) * mid + az * far)
            sg = (jnp.maximum(v[0], 0.0) + jnp.log(1.0 + jnp.exp(-jnp.abs(v[0])))) * scale
            b.sigma[g, k] = sg
            b.slope[g, k] = (0.5 + 0.5 * jnp.tanh(0.5 * v[0])) * scale
            for c in range(3):
                b.colour[g, c, k] = 0.5 + 0.5 * jnp.tanh(0.5 * v[c + 1])
            b.ahead[g, k] = acc[g]
            new.append(acc[g] + sg)
        return tuple(new)

    zero = jnp.zeros((rows, half), jnp.float32)
    return lax.fori_loop(0, planes, step, (zero, zero))


def local_light(b, totals):
    _, planes, rows, half = b.sigma.shape
    images = []
    for g in range(2):
        forward = b.heading[g] == 0

        def step(k, acc):
            sg, ah = b.sigma[g, k], b.ahead[g, k]
            front = jnp.where(forward, ah, totals[g] - ah - sg)
            th = jnp.exp(-front)
            gl = th * (1.0 - jnp.exp(-sg))
            b.through[g, k] = th
            b.glow[g, k] = gl
            return tuple(acc[c] + gl * b.colour[g, c, k] for c in range(3))

        zero = jnp.zeros((rows, half), jnp.float32)
        images.append(lax.fori_loop(0, planes, step, (zero,) * 3))
    return images


def tiles_out(b, put, nz):
    lanes, half = b.stack.shape
    tw = half // 2
    for x in range(2):
        turned = b.stack[:, x * tw:(x + 1) * tw].T
        for i in range(tw // 8):
            j = x * (tw // 8) + i
            put(j % nz, j // nz, turned[8 * i:8 * i + 8])


def backward(b, kept):
    _, planes, rows, half = b.sigma.shape
    zero = jnp.zeros((rows, half), jnp.float32)
    for g in range(2):
        forward = b.heading[g] == 0
        reach = b.stack[2 * g * rows:(2 * g + 1) * rows]
        rest = b.stack[(2 * g + 1) * rows:(2 * g + 2) * rows]
        whole = reach * kept[g]
        for c in range(4):
            for k in (0, 1, planes + 2, planes + 3):
                b.diff[g, c, k] = zero

        def step(k, before):
            pull = [b.pull[g, c] for c in range(3)]
            col = [b.colour[g, c, k] for c in range(3)]
            shade = pull[0] * col[0] + pull[1] * col[1] + pull[2] * col[2]
            th, gl = b.through[g, k], b.glow[g, k]
            lit = reach * gl
            share = lit * shade
            behind = rest + jnp.where(forward, whole - before - share, before)
            b.diff[g, 0, k + 2] = (reach * (th - gl) * shade - behind) * b.slope[g, k]
            for c in range(3):
                b.diff[g, c + 1, k + 2] = pull[c] * lit * (col[c] * (1.0 - col[c]))
            return before + share

        lax.fori_loop(0, planes, step, zero)


def spill_plane(b, me, p, pack, place):
    ch, ext, rows, half = b.out.shape
    tw = half // 2
    d, t = me.dir, me.tile
    row, lane = iota((rows, tw), 0), iota((rows, tw), 1)
    for c in range(ch):
        cols = []
        for g in range(2):
            fz = b.pair[g, 0]
            cols.append((1.0 - jnp.abs(fz)) * b.diff[g, c, p + 1]
                        + jnp.maximum(fz, 0.0) * b.diff[g, c, p]
                        + jnp.maximum(-fz, 0.0) * b.diff[g, c, p + 2])
        bands = []
        for i in range(3):
            u = []
            for j in range(3):
                full = (b.taps[0, 3 * i + j] * cols[0] + b.taps[1, 3 * i + j] * cols[1])
                u.append([full[:, :tw], full[:, tw:]])
            l = [pltpu.roll(a, tw - 1, 1) for a in u[0]]
            r = [pltpu.roll(a, 1, 1) for a in u[2]]
            x0 = u[1][0] + jnp.where(lane == tw - 1, l[1], l[0]) + jnp.where(lane == 0, 0.0, r[0])
            x1 = u[1][1] + jnp.where(lane == tw - 1, 0.0, l[1]) + jnp.where(lane == 0, r[0], r[1])
            bands.append([x0, x1, jnp.where(d == 0, r[1], u[0][0])])
        done, far = [], []
        for x in range(3):
            up = pltpu.roll(bands[0][x], rows - 1, 0)
            dn = pltpu.roll(bands[2][x], 1, 0)
            done.append(bands[1][x] + jnp.where(row == rows - 1, 0.0, up)
                        + jnp.where(row == 0, 0.0, dn))
            far.append(jnp.where(t == 0, dn[0:1], up[rows - 1:rows]))
        b.out[c, p, :, :tw] = done[0]
        b.out[c, p, :, tw:] = done[1]
        b.line[p, c:c + 1, :tw] = far[0]
        b.line[p, c:c + 1, tw:] = far[1]
        slot = iota((rows, SIDE), 1)
        pos = place(c)
        pack[:rows] = jnp.where(
            slot == pos, jnp.broadcast_to(done[2][:, 0:1], (rows, SIDE)), pack[:rows])
        pack[rows:rows + 1] = jnp.where(
            slot[0:1] == pos, jnp.broadcast_to(far[2][:, 0:1], (1, SIDE)), pack[rows:rows + 1])


def gather_spill(b, me, has_prev, has_next, dest):
    ch, ext, rows, half = b.out.shape
    planes = ext - 2
    tw = half // 2
    d, t = me.dir, me.tile
    touch = (1 - t) * (rows - 1)
    seam = (1 - d) * (half - 1)
    row = iota((rows, tw), 0)
    lane = iota((rows, tw), 1)
    spot = iota((1, SIDE), 1)
    b.inturn[:ch * planes] = b.rin[...]
    for c in range(ch):
        for k, i, r, has in ((0, 0, ch + c, has_prev), (planes - 1, 1, c, has_next)):
            far = jnp.broadcast_to(b.rzfar[i, r:r + 1, rows:rows + 1], (1, SIDE))
            add = jnp.where(spot < rows, b.rzin[i, r:r + 1], 0.0) + jnp.where(spot == touch, far, 0.0)
            j = c * planes + k
            b.inturn[j:j + 1] = b.inturn[j:j + 1] + add * has
    col = b.inturn[...].T[:rows]
    col = col + jnp.where(iota((rows, SIDE), 0) == touch, jnp.broadcast_to(b.rfar[0:1], (rows, SIDE)), 0.0)
    for c in range(ch):
        for k in range(planes):
            pos = c * planes + k
            extra = b.rline[k, c:c + 1]
            v = b.out[c, k + 1]
            if k == 0:
                extra = extra + b.zline[0, c:c + 1] * has_prev
                v = v + b.fp[c] * has_prev
            if k == planes - 1:
                extra = extra + b.zline[1, c:c + 1] * has_next
                v = v + b.fn[c] * has_next
            bar = jnp.broadcast_to(col[:, pos:pos + 1], (rows, tw))
            for x in range(2):
                at = slice(x * tw, (x + 1) * tw)
                y = v[:, at] + jnp.where(row == touch, jnp.broadcast_to(extra[:, at], (rows, tw)), 0.0)
                y = y + jnp.where(lane + x * tw == seam, bar, 0.0)
                dest[c, k, :, at] = y


def render_kernel(scale, depth, names, vox, codes, head, cot, grad, img, *scratch):
    b = SimpleNamespace(**dict(zip(names, scratch)))
    sems = scratch[len(names):]
    (lsem, hs, hr, s1, r1, s2, r2, s3, r3, s4, r4, s5, r5, ss, sr) = sems
    me = places()
    nsy, nsx, nz = (lax.axis_size(a) for a in SLAB)
    ng = nsy * nsx
    blocks = ng // 2
    d, t, z = me.dir, me.tile, me.sz
    gi = me.sy * nsx + me.sx
    s = slab_index(me)
    prev, nxt = at_slab(me, -1), at_slab(me, 1)
    flip = lambda p: p._replace(tile=1 - p.tile)
    over = lambda p: p._replace(dir=1 - p.dir)
    near = [prev, me, nxt]
    mate = me._replace(dir=1 - d, sx=nsx - 1 - me.sx)
    ch, ext, rows, half = b.grid.shape
    planes = ext - 2
    wide = b.wing.shape[-1]
    has_prev = (s > 0).astype(jnp.float32)
    has_next = (s < nsy * nsx * nz - 1).astype(jnp.float32)

    mine = pl.ds(pl.multiple_of(d * half, half), half)
    theirs = pl.ds(pl.multiple_of((1 - d) * half, half), half)
    beside = pl.ds(pl.multiple_of(half - d * wide, wide), wide)
    loads = [
        (vox.at[:, :, :, mine], b.grid.at[:, 1:planes + 1]),
        (vox.at[:, :, :, beside], b.wing.at[:, 1:planes + 1]),
        (codes.at[0, :, mine], b.codes.at[0]),
        (head.at[0, :, mine], b.heading.at[0]),
        (cot.at[0, :, :, mine], b.pull.at[0]),
    ]
    loads = [pltpu.make_async_copy(a, c, lsem.at[i]) for i, (a, c) in enumerate(loads)]
    for c in loads:
        c.start()

    far_first = sorted(range(1, nz), key=lambda i: -min(i, nz - i))
    zpeer = [me._replace(sz=lax.rem(z + i, nz)) for i in far_first]
    gpeer, across = [], []
    for i in range(ng):
        g = lax.rem(gi + i, ng)
        p = me._replace(sy=g // nsx, sx=g % nsx)
        across.append(over(p))
        if i:
            gpeer.append(p)
    ready = greet([prev, nxt] + [flip(p) for p in near] + [over(p) for p in near]
          + [over(flip(p)) for p in near] + zpeer + gpeer + across)

    for c in loads[:2]:
        c.wait()
    cut_faces(b, me)
    for c in loads[2:]:
        c.wait()
    weights(b, 0)
    ready()
    rays = [
        (codes.at[0, :, theirs], b.codes.at[1], mate),
        (head.at[0, :, theirs], b.heading.at[1], mate),
        (cot.at[0, :, :, theirs], b.pull.at[1], mate),
    ]
    rays = [push(x, y, hs.at[i], hr.at[i], p) for i, (x, y, p) in enumerate(rays)]
    for c in rays:
        c.start()
    edge = pl.ds(pl.multiple_of((1 - t) * (rows - 8), 8), 8)
    inner = pl.ds(1, planes)
    beyond = [
        (b.grid.at[:, inner, edge], b.rows, flip(me)),
        (b.wing.at[:, inner, edge], b.rwing, flip(me)),
        (b.cut.at[0], b.rcut.at[0], nxt),
        (b.cut.at[1], b.rcut.at[1], prev),
        (b.brim.at[0], b.rbrim.at[0], flip(nxt)),
        (b.brim.at[1], b.rbrim.at[1], flip(prev)),
        (b.grid.at[:, planes], b.grid.at[:, 0], nxt),
        (b.grid.at[:, 1], b.grid.at[:, ext - 1], prev),
    ]
    beyond = [push(x, y, hs.at[3 + i], hr.at[3 + i], p) for i, (x, y, p) in enumerate(beyond)]
    for c in beyond:
        c.start()
    for c in beyond[:2]:
        c.wait()

    def inside(gs):
        def step(p, carry):
            sample_plane(b, me, p, gs, inner_edges(b, me, p), None)
            return carry

        lax.fori_loop(1, planes + 1, step, 0)

    inside((0,))
    rays[0].wait()
    weights(b, 1)
    inside((1,))
    for c in beyond[2:]:
        c.wait()

    def ends(i, carry):
        sample_plane(b, me, i * (ext - 1), (0, 1), outer_edges(b, me, i),
                     jnp.where(i == 0, has_prev, has_next))
        return carry

    lax.fori_loop(0, 2, ends, 0)
    totals = shade_planes(b, scale)
    for c in rays[1:]:
        c.wait()
    for g in range(2):
        for c in range(3):
            b.pull[g, c] = b.pull[g, c] * depth
    images = local_light(b, totals)
    kept = []
    for g in range(2):
        kept.append(sum(b.pull[g, c] * images[g][c] for c in range(3)))
        b.stack[2 * g * rows:(2 * g + 1) * rows] = totals[g]
        b.stack[(2 * g + 1) * rows:(2 * g + 2) * rows] = kept[g]

    def put_dl(j, m, v):
        b.dl[j, m] = v

    tiles_out(b, put_dl, nz)
    first = [push(b.dl.at[p.sz], b.rdl.at[z], s1.at[i], r1.at[i], p)
             for i, p in enumerate(zpeer)]
    for c in first:
        c.start()
    for g in range(2):
        for c in range(3):
            b.stack[c * rows:(c + 1) * rows] = images[g][c]

        def put_im(j, m, v):
            b.im[j, g, m] = v

        tiles_out(b, put_im, nz)
    late = [push(b.im.at[p.sz], b.rim.at[z], s2.at[i], r2.at[i], p)
            for i, p in enumerate(zpeer)]
    for c in late:
        c.start()
    for g in range(2):
        for i in range(2):
            b.stack[(2 * g + i) * rows:(2 * g + i + 1) * rows] = b.heading[g].astype(jnp.float32)

    def put_hd(j, m, v):
        b.hd[j, m] = v

    tiles_out(b, put_hd, nz)
    b.rdl[z] = b.dl[z]
    b.rim[z] = b.im[z]
    lanes = b.dl.shape[-1]
    ahead = b.hd[z] == 0
    spot = iota(ahead.shape, 2)
    is_d = (spot // rows) % 2 == 0
    for c in first:
        c.wait()
    roll = lambda a, n: pltpu.roll(a, n % lanes, 2)

    def directed(parts):
        lows, low = [], jnp.zeros_like(parts[0])
        for p in parts:
            lows.append(low)
            low = low + p
        highs, high = [], jnp.zeros_like(parts[0])
        for p in reversed(parts):
            highs.append(high)
            high = high + p
        highs = highs[::-1]
        before = [jnp.where(ahead, x, y) for x, y in zip(lows, highs)]
        after = [jnp.where(ahead, y, x) for x, y in zip(lows, highs)]
        return before, after, low

    tiles = [b.rdl[i] for i in range(nz)]
    before, _, dsum = directed(tiles)
    reach = [jnp.exp(-x) for x in before]
    pulled = [roll(r, rows) * x for r, x in zip(reach, tiles)]
    _, behind, lsum = directed(pulled)
    b.gm[gi] = jnp.where(is_d, dsum, lsum)
    second = [push(b.gm.at[gi], b.gm.at[gi], s3.at[i], r3.at[i], p)
              for i, p in enumerate(gpeer)]
    for c in second:
        c.start()
    for c in second:
        c.wait()
    groups = [b.gm[i] for i in range(ng)]
    gbefore, _, _ = directed(groups)
    greach = [jnp.exp(-x) for x in gbefore]
    gpull = [roll(r, rows) * x for r, x in zip(greach, groups)]
    _, gafter, _ = directed(gpull)
    to_me = jnp.zeros_like(dsum)
    rest = jnp.zeros_like(dsum)
    for i in range(ng):
        to_me = jnp.where(gi == i, greach[i], to_me)
        rest = jnp.where(gi == i, gafter[i], rest)
    to_me_l = roll(to_me, rows)
    full = []
    for i in range(nz):
        r = to_me * reach[i]
        full.append(r)
        b.ret[i] = jnp.where(is_d, r, rest + to_me_l * behind[i])
    back = [push(b.ret.at[p.sz], b.rb.at[z], s4.at[i], r4.at[i], p)
            for i, p in enumerate(zpeer)]
    for c in back:
        c.start()
    b.rb[z] = b.ret[z]
    for c in late:
        c.wait()
    quarter = spot // rows
    for g in range(2):
        total = jnp.zeros_like(dsum)
        for i in range(nz):
            src = full[i]
            wash = roll(src, -2 * g * rows)
            wash = jnp.where(quarter == 1, roll(src, (1 - 2 * g) * rows), wash)
            wash = jnp.where(quarter == 2, roll(src, (2 - 2 * g) * rows), wash)
            total = total + wash * b.rim[i, g]
        b.part[g] = total
    half_of_me = gi // blocks
    out = []
    for g in range(2):
        for m in range(blocks):
            q = blocks * d + m
            peer = me._replace(dir=d if g == 0 else 1 - d, sy=q // nsx, sx=q % nsx)
            out.append(push(b.part.at[g, m], b.rpart.at[gi],
                            s5.at[g * blocks + m], r5.at[gi], peer))
    for g in range(2):
        for m in range(blocks):
            copy = out[g * blocks + m]
            if g == 0:
                itself = gi == blocks * d + m

                @pl.when(itself)
                def _():
                    b.rpart[gi] = b.part[0, m]

                @pl.when(jnp.logical_not(itself))
                def _():
                    copy.start()
            else:
                copy.start()
    for c in back:
        c.wait()

    tw = half // 2
    for x in range(2):
        for i in range(tw // 8):
            j = x * (tw // 8) + i
            b.tile[8 * i:8 * i + 8] = b.rb[j % nz, j // nz]
        b.stack[:, x * tw:(x + 1) * tw] = b.tile[...].T
    backward(b, kept)

    def spread_ends(i, carry):
        spill_plane(b, me, i * (ext - 1), b.zpack, lambda c: i * ch + c)
        return carry

    lax.fori_loop(0, 2, spread_ends, 0)
    b.zturn[...] = b.zpack[...].T
    spill = [
        (b.out.at[:, ext - 1], b.fp, nxt), (b.out.at[:, 0], b.fn, prev),
        (b.line.at[ext - 1], b.zline.at[0], flip(nxt)), (b.line.at[0], b.zline.at[1], flip(prev)),
    ]
    small = b.zturn.at[0:8]
    for i, p in enumerate((nxt, prev)):
        spill.append((small, b.rzin.at[i], over(p)))
        spill.append((small, b.rzfar.at[i], over(flip(p))))
    spill = [push(x, y, ss.at[i], sr.at[i], p) for i, (x, y, p) in enumerate(spill)]
    for c in spill:
        c.start()

    def spread(p, carry):
        spill_plane(b, me, p, b.inpack, lambda c: c * planes + p - 1)
        return carry

    lax.fori_loop(1, planes + 1, spread, 0)
    b.inturn[...] = b.inpack[...].T
    last = [
        (b.inturn.at[0:ch * planes], b.rin, over(me)),
        (b.inpack.at[rows:rows + 8], b.rfar, over(flip(me))),
        (b.line.at[inner], b.rline, flip(me)),
    ]
    last = [push(x, y, ss.at[8 + i], sr.at[8 + i], p) for i, (x, y, p) in enumerate(last)]
    for c in last:
        c.start()
    spill = spill + last

    for g in range(2):
        for m in range(blocks):
            copy = out[g * blocks + m]
            if g == 0:
                @pl.when(gi != blocks * d + m)
                def _():
                    copy.wait_send()
            else:
                copy.wait_send()
    for i in range(ng):
        arrive = push(b.part.at[0, 0], b.rpart.at[i], s5.at[0], r5.at[i], over(me))

        @pl.when(jnp.logical_or(half_of_me != d, gi != i))
        def _():
            arrive.wait_recv()
    total = b.rpart[0]
    for i in range(1, ng):
        total = total + b.rpart[i]
    for c in range(3):
        img[c] = total[:, c * rows:(c + 1) * rows]
    for c in spill:
        c.wait()
    gather_spill(b, me, has_prev, has_next, grad)


def per_device(voxels, offsets, heading, cotangent):
    ch, planes, rows, total = voxels.shape
    nsy, nsx, nz = (lax.axis_size(a) for a in SLAB)
    ng = nsy * nsx
    depth = planes * nz * ng
    half = total // 2
    wide = half // 2
    room = shapes(ch, planes, rows, half, wide, nz, ng)
    dma = lambda n: pltpu.SemaphoreType.DMA((n,))
    grad, img = pl.pallas_call(
        functools.partial(render_kernel, 2.0 / depth, float(depth), tuple(room)),
        out_shape=(pltpu.VMEM((ch, planes, rows, half), jnp.float32),
                   pltpu.VMEM((3, 8, rows), jnp.float32)),
        in_specs=[HBM] * 4,
        out_specs=(VM, VM),
        scratch_shapes=list(room.values()) + [
            dma(5), dma(11), dma(11),
            dma(nz - 1), dma(nz - 1), dma(nz - 1), dma(nz - 1),
            dma(ng - 1), dma(ng - 1), dma(nz - 1), dma(nz - 1),
            dma(ng), dma(ng), dma(11), dma(11),
        ],
        compiler_params=pltpu.CompilerParams(
            collective_id=0, has_side_effects=True, vmem_limit_bytes=58 * 1024 * 1024
        ),
    )(voxels, offsets, heading, cotangent)
    image = jnp.swapaxes(img, 1, 2)[None]
    return (image, grad)


def solution(mesh):
    n = mesh.devices.size
    shape = (2, 4, 2, 8, 2) if n == 256 else (2, 2, 1, 2, 2)
    finer = Mesh(mesh.devices.reshape(shape), AXES)
    return jax.shard_map(
        per_device,
        mesh=finer,
        in_specs=(
            P(None, SLAB, "tile", None),
            P("dir", "tile", None),
            P("dir", "tile", None),
            P("dir", None, "tile", None),
        ),
        out_specs=(P("dir", None, "tile", SLAB), P(None, SLAB, "tile", "dir")),
        check_vma=False,
    )
```

```python
import functools
from types import SimpleNamespace
from typing import NamedTuple

import jax
import jax.numpy as jnp
from jax import lax
from jax.experimental import pallas as pl
from jax.experimental.pallas import tpu as pltpu
from jax.sharding import Mesh
from jax.sharding import PartitionSpec as P

LEVELS = 8
SIDE = 128
AXES = ("dir", "sy", "sx", "sz", "tile")
SLAB = AXES[1:4]
MESH = pl.DeviceIdType.MESH
HBM = pl.BlockSpec(memory_space=pltpu.HBM)
VM = pl.BlockSpec(memory_space=pltpu.VMEM)


class Place(NamedTuple):
    dir: int
    sy: int
    sx: int
    sz: int
    tile: int


def places():
    return Place(*[lax.axis_index(a) for a in AXES])


def slab_index(me):
    _, _, sx, sz, _ = (lax.axis_size(a) for a in AXES)
    return (me.sy * sx + me.sx) * sz + me.sz


def at_slab(me, step):
    sy, sx, sz = (lax.axis_size(a) for a in SLAB)
    s = lax.rem(slab_index(me) + step + sy * sx * sz, sy * sx * sz)
    return me._replace(sy=s // (sx * sz), sx=(s // sz) % sx, sz=s % sz)


def greet(peers):
    barrier = pltpu.get_barrier_semaphore()
    for peer in peers:
        pl.semaphore_signal(barrier, inc=1, device_id=tuple(peer), device_id_type=MESH)
    return lambda: pl.semaphore_wait(barrier, len(peers))


def push(src, dst, send, recv, peer):
    return pltpu.make_async_remote_copy(
        src_ref=src, dst_ref=dst, send_sem=send, recv_sem=recv,
        device_id=tuple(peer), device_id_type=MESH,
    )


def shapes(ch, planes, rows, half, wide, nz, ng):
    lanes, m = 4 * rows, half // 8 // nz
    pairs = m // 2
    ext = planes + 2
    f32 = jnp.float32
    one = dict(
        grid=(ch, ext, rows, half), wing=(ch, ext, rows, wide),
        cut=(2, rows, wide), rcut=(2, rows, wide), brim=(ext, ch, half + wide),
        rbrim=(ext, ch, half + wide),
        plane=(2, ch, ext, rows, half), tail=(2, ext, rows, half),
        sigma=(2, planes, rows, half), colour=(2, 3, planes, rows, half),
        through=(2, planes, rows, half), glow=(2, planes, rows, half),
        taps=(2, 9, rows, half), pair=(2, 7, rows, half), kept=(2, rows, half),
        codes=(2, rows, half), heading=(2, rows, half), pull=(2, 3, rows, half),
        ahead=(2, planes, rows, half), stack=(lanes, wide), tile=(wide, lanes),
        diff=(2, ch + 1, planes + 4, rows, half), out=(ch, ext, rows, half),
        lit=(2, 2, rows, half), seam=(2, 2, rows, SIDE),
        line=(ext, ch, half), pack=(SIDE, SIDE), turn=(SIDE, SIDE),
        fp=(ch, rows, half), fn=(ch, rows, half),
        rline=(planes, ch, half), zline=(2, ch, half), rin=(ch * planes, SIDE),
        rfar=(8, SIDE), rzin=(2, 8, SIDE), rzfar=(2, 8, SIDE),
        dl=(2, nz, pairs, 8, lanes), hd=(2, nz, pairs, 8, lanes), rdl=(2, nz, pairs, 8, lanes),
        im=(2, nz, m, 8, lanes), rim=(2, nz, m, 8, lanes), gm=(2, ng, pairs, 8, lanes),
        zreach=(2, nz, pairs, 8, lanes), zlater=(2, nz, pairs, 8, lanes),
        ret=(2, nz, pairs, 8, lanes), rb=(2, nz, pairs, 8, lanes),
        part=(2, m, 8, lanes), rpart=(ng, 8, lanes),
    )
    ints = dict(codes=0, heading=0)
    return {k: pltpu.VMEM(v, jnp.int32 if k in ints else f32) for k, v in one.items()}


def weights(b, g):
    level = LEVELS
    q = b.codes[g]
    frac = lambda raw: (raw.astype(jnp.float32) + 0.5) / level - 0.5
    fz, fy, fx = frac(q & 7), frac((q >> 3) & 7), frac(q >> 6)
    three = lambda f: (jnp.maximum(-f, 0.0), 1.0 - jnp.abs(f), jnp.maximum(f, 0.0))
    wy, wx = three(fy), three(fx)
    for i in range(3):
        for j in range(3):
            b.taps[g, 3 * i + j] = wy[i] * wx[j]
    ay, ax = jnp.abs(fy), jnp.abs(fx)
    for i, v in enumerate((fz, fy, fx, wy[1] * wx[1], wy[1] * ax, ay * wx[1], ay * ax)):
        b.pair[g, i] = v


def iota(shape, dim):
    return lax.broadcasted_iota(jnp.int32, shape, dim)


def lane_of(d, r):
    return jnp.where(d == 0, r[..., 0:1], r[..., r.shape[-1] - 1:])


def inner_edges(b, me, p):
    return lambda c: jnp.broadcast_to(lane_of(me.dir, b.wing[c, p]), b.wing.shape[2:])


def outer_edges(b, me, i):
    return lambda c: jnp.broadcast_to(b.rcut[i][:, c:c + 1], b.wing.shape[2:])


def cut_faces(b, me):
    ch, ext, rows, half = b.grid.shape
    wide = b.wing.shape[3]
    slot = iota((rows, wide), 1)
    for i, p in enumerate((ext - 2, 1)):
        acc = jnp.zeros((rows, wide), jnp.float32)
        for c in range(ch):
            acc = jnp.where(slot == c, inner_edges(b, me, p)(c), acc)
        b.cut[i] = acc

    def trim(p, carry):
        pick = lambda r: jnp.where(me.tile == 0, r[rows - 1:rows], r[0:1])
        for c in range(ch):
            b.brim[p, c:c + 1, :half] = pick(b.grid[c, p])
            b.brim[p, c:c + 1, half:] = pick(b.wing[c, p])
        return carry

    lax.fori_loop(1, ext - 1, trim, 0)


def sample_plane(b, me, p, gs, edges, keep):
    ch, _, rows, half = b.grid.shape
    tw = half // 2
    d, t = me.dir, me.tile
    row, lane = iota((rows, tw), 0), iota((rows, tw), 1)
    right = (d == 0).astype(jnp.float32)
    left = 1.0 - right
    under = (t == 0).astype(jnp.float32)
    over = 1.0 - under
    for c in range(ch):
        edge, line = edges(c), b.rbrim[p, c:c + 1, :]
        corner = jnp.broadcast_to(lane_of(d, line[:, half:]), (1, tw))
        m = [b.grid[c, p, :, x * tw:(x + 1) * tw] for x in range(2)] + [edge]
        far = [line[:, :tw], line[:, tw:half], corner]
        up = [jnp.where(row == 0, f * over, pltpu.roll(a, 1, 0)) for a, f in zip(m, far)]
        dn = [jnp.where(row == rows - 1, f * under, pltpu.roll(a, rows - 1, 0))
              for a, f in zip(m, far)]
        spread = []
        for a in (up, m, dn):
            r = [pltpu.roll(a[x], 1, 1) for x in range(2)]
            l = [pltpu.roll(a[x], tw - 1, 1) for x in range(2)]
            lo = [jnp.where(lane == 0, a[2] * left, r[0]), jnp.where(lane == 0, r[0], r[1])]
            hi = [jnp.where(lane == tw - 1, l[1], l[0]),
                  jnp.where(lane == tw - 1, a[2] * right, l[1])]
            spread.append((lo, a[:2], hi))
        for x in range(2):
            at = slice(x * tw, (x + 1) * tw)
            for g in gs:
                fy, fx = b.pair[g, 1, :, at], b.pair[g, 2, :, at]
                w00, w01 = b.pair[g, 3, :, at], b.pair[g, 4, :, at]
                w10, w11 = b.pair[g, 5, :, at], b.pair[g, 6, :, at]
                side = lambda s: jnp.where(fx > 0, s[2][x], s[0][x])
                down = fy > 0
                v = (w00 * m[x] + w01 * side(spread[1])
                     + w10 * jnp.where(down, dn[x], up[x])
                     + w11 * jnp.where(down, side(spread[2]), side(spread[0])))
                b.plane[g, c, p, :, at] = v if keep is None else v * keep


def shade_planes(b, scale, g):
    _, ch, ext, rows, half = b.plane.shape
    fz = b.pair[g, 0]
    az = jnp.abs(fz)

    def step(k, acc):
        v = []
        for c in range(ch):
            far = jnp.where(fz > 0, b.plane[g, c, k + 2], b.plane[g, c, k])
            v.append((1.0 - az) * b.plane[g, c, k + 1] + az * far)
        sg = (jnp.maximum(v[0], 0.0) + jnp.log(1.0 + jnp.exp(-jnp.abs(v[0])))) * scale
        b.sigma[g, k] = sg
        b.diff[g, ch, k + 2] = (0.5 + 0.5 * jnp.tanh(0.5 * v[0])) * scale
        for c in range(3):
            b.colour[g, c, k] = 0.5 + 0.5 * jnp.tanh(0.5 * v[c + 1])
        b.ahead[g, k] = acc
        return acc + sg

    return lax.fori_loop(0, ext - 2, step, jnp.zeros((rows, half), jnp.float32))


def local_light(b, total, g):
    _, planes, rows, half = b.sigma.shape
    forward = b.heading[g] == 0

    def step(k, acc):
        sg, ah = b.sigma[g, k], b.ahead[g, k]
        front = jnp.where(forward, ah, total - ah - sg)
        th = jnp.exp(-front)
        gl = th * (1.0 - jnp.exp(-sg))
        b.through[g, k] = th
        b.glow[g, k] = gl
        return tuple(acc[c] + gl * b.colour[g, c, k] for c in range(3))

    zero = jnp.zeros((rows, half), jnp.float32)
    return lax.fori_loop(0, planes, step, (zero,) * 3)


def tiles_out(b, nz, put):
    turned = b.stack[...].T
    for i in range(turned.shape[0] // 8):
        put(i % nz, i // nz, turned[8 * i:8 * i + 8])


def prepare(b, g):
    _, planes, rows, half = b.sigma.shape
    ch = b.grid.shape[0]
    zero = jnp.zeros((rows, half), jnp.float32)
    forward = b.heading[g] == 0
    whole = b.kept[g]
    for c in range(ch + 1):
        for k in (0, 1, planes + 2, planes + 3):
            b.diff[g, c, k] = zero

    def step(k, before):
        pull = [b.pull[g, c] for c in range(3)]
        col = [b.colour[g, c, k] for c in range(3)]
        shade = pull[0] * col[0] + pull[1] * col[1] + pull[2] * col[2]
        th, gl = b.through[g, k], b.glow[g, k]
        share = gl * shade
        later = jnp.where(forward, whole - before - share, before)
        b.diff[g, 0, k + 2] = ((th - gl) * shade - later) * b.diff[g, ch, k + 2]
        for c in range(3):
            b.diff[g, c + 1, k + 2] = pull[c] * gl * (col[c] * (1.0 - col[c]))
        return before + share

    lax.fori_loop(0, planes, step, zero)

    def mix(p, carry):
        fz = b.pair[g, 0]
        mid, up, down = 1.0 - jnp.abs(fz), jnp.maximum(fz, 0.0), jnp.maximum(-fz, 0.0)
        for c in range(ch + 1):
            v = mid * b.diff[g, c, p + 1] + up * b.diff[g, c, p] + down * b.diff[g, c, p + 2]
            if c < ch:
                b.plane[g, c, p] = v
            else:
                b.tail[g, p] = v
        return carry

    lax.fori_loop(0, planes + 2, mix, 0)


def seam_slot(c, p, ch, planes):
    if p == 0:
        return ch * planes + c
    return ch * planes + ch + c if p == planes + 1 else c * planes + p - 1


def seam_of(d, r):
    return jnp.where(d == 0, r[..., r.shape[-1] - 1:], r[..., 0:1])


def gather_seam(b, me, g):
    _, ch, ext, rows, half = b.plane.shape
    slot = iota((rows, SIDE), 1)
    wide = lambda v: jnp.broadcast_to(seam_of(me.dir, v), (rows, SIDE))
    a = jnp.zeros((rows, SIDE), jnp.float32)
    r = a
    for p in range(ext):
        for c in range(ch):
            a = jnp.where(slot == seam_slot(c, p, ch, ext - 2), wide(b.plane[g, c, p]), a)
        r = jnp.where(slot == seam_slot(0, p, ch, ext - 2), wide(b.tail[g, p]), r)
    b.seam[g, 0] = a
    b.seam[g, 1] = r


def spill_seam(b, me):
    _, ch, ext, rows, half = b.plane.shape
    d, t = me.dir, me.tile
    row = iota((rows, SIDE), 0)
    wide = lambda v: jnp.broadcast_to(seam_of(d, v), (rows, SIDE))
    cols = [wide(b.lit[g, 0]) * b.seam[g, 0] - wide(b.lit[g, 1]) * b.seam[g, 1] for g in range(2)]
    bands = []
    for i in range(3):
        w = [jnp.where(d == 0, b.taps[g, 3 * i + 2, :, half - 1:half], b.taps[g, 3 * i, :, 0:1])
             for g in range(2)]
        bands.append(sum(jnp.broadcast_to(w[g], (rows, SIDE)) * cols[g] for g in range(2)))
    up = pltpu.roll(bands[0], rows - 1, 0)
    dn = pltpu.roll(bands[2], 1, 0)
    b.pack[:rows] = (bands[1] + jnp.where(row == rows - 1, 0.0, up) + jnp.where(row == 0, 0.0, dn))
    b.pack[rows:rows + 1] = jnp.where(t == 0, dn[0:1], up[rows - 1:rows])
    b.turn[...] = b.pack[...].T


def spill_plane(b, me, p):
    ch, ext, rows, half = b.out.shape
    tw = half // 2
    t = me.tile
    row, lane = iota((rows, tw), 0), iota((rows, tw), 1)
    for c in range(ch):
        cols = []
        for g in range(2):
            v = b.lit[g, 0] * b.plane[g, c, p]
            cols.append(v if c else v - b.lit[g, 1] * b.tail[g, p])
        bands = []
        for i in range(3):
            u = []
            for j in range(3):
                full = b.taps[0, 3 * i + j] * cols[0] + b.taps[1, 3 * i + j] * cols[1]
                u.append([full[:, :tw], full[:, tw:]])
            l = [pltpu.roll(a, tw - 1, 1) for a in u[0]]
            r = [pltpu.roll(a, 1, 1) for a in u[2]]
            x0 = u[1][0] + jnp.where(lane == tw - 1, l[1], l[0]) + jnp.where(lane == 0, 0.0, r[0])
            x1 = u[1][1] + jnp.where(lane == tw - 1, 0.0, l[1]) + jnp.where(lane == 0, r[0], r[1])
            bands.append([x0, x1])
        for x in range(2):
            at = slice(x * tw, (x + 1) * tw)
            up = pltpu.roll(bands[0][x], rows - 1, 0)
            dn = pltpu.roll(bands[2][x], 1, 0)
            b.out[c, p, :, at] = (bands[1][x] + jnp.where(row == rows - 1, 0.0, up)
                                  + jnp.where(row == 0, 0.0, dn))
            b.line[p, c:c + 1, at] = jnp.where(t == 0, dn[0:1], up[rows - 1:rows])


def gather_spill(b, me, has_prev, has_next, dest):
    ch, ext, rows, half = b.out.shape
    planes = ext - 2
    tw = half // 2
    d, t = me.dir, me.tile
    touch = (1 - t) * (rows - 1)
    seam = (1 - d) * (half - 1)
    row = iota((rows, tw), 0)
    lane = iota((rows, tw), 1)
    spot = iota((1, SIDE), 1)
    b.turn[:ch * planes] = b.rin[...]
    for c in range(ch):
        for k, i, r, has in ((0, 0, ch + c, has_prev), (planes - 1, 1, c, has_next)):
            far = jnp.broadcast_to(b.rzfar[i, r:r + 1, rows:rows + 1], (1, SIDE))
            add = jnp.where(spot < rows, b.rzin[i, r:r + 1], 0.0) + jnp.where(spot == touch, far, 0.0)
            j = c * planes + k
            b.turn[j:j + 1] = b.turn[j:j + 1] + add * has
    col = b.turn[...].T[:rows]
    col = col + jnp.where(iota((rows, SIDE), 0) == touch, jnp.broadcast_to(b.rfar[0:1], (rows, SIDE)), 0.0)
    for c in range(ch):
        for k in range(planes):
            pos = c * planes + k
            extra = b.rline[k, c:c + 1]
            v = b.out[c, k + 1]
            if k == 0:
                extra = extra + b.zline[0, c:c + 1] * has_prev
                v = v + b.fp[c] * has_prev
            if k == planes - 1:
                extra = extra + b.zline[1, c:c + 1] * has_next
                v = v + b.fn[c] * has_next
            bar = jnp.broadcast_to(col[:, pos:pos + 1], (rows, tw))
            for x in range(2):
                at = slice(x * tw, (x + 1) * tw)
                y = v[:, at] + jnp.where(row == touch, jnp.broadcast_to(extra[:, at], (rows, tw)), 0.0)
                y = y + jnp.where(lane + x * tw == seam, bar, 0.0)
                dest[c, k, :, at] = y


def render_kernel(scale, depth, names, vox, codes, head, cot, grad, img, *scratch):
    b = SimpleNamespace(**dict(zip(names, scratch)))
    sems = scratch[len(names):]
    (lsem, hs, hr, s1, r1, s2, r2, s3, r3, s4, r4, s5, r5, ss, sr) = sems
    me = places()
    nsy, nsx, nz = (lax.axis_size(a) for a in SLAB)
    ng = nsy * nsx
    blocks = ng // 2
    d, t, z = me.dir, me.tile, me.sz
    gi = me.sy * nsx + me.sx
    s = slab_index(me)
    prev, nxt = at_slab(me, -1), at_slab(me, 1)
    flip = lambda p: p._replace(tile=1 - p.tile)
    over = lambda p: p._replace(dir=1 - p.dir)
    near = [prev, me, nxt]
    mate = me._replace(dir=1 - d, sx=nsx - 1 - me.sx)
    ch, ext, rows, half = b.grid.shape
    planes = ext - 2
    wide = b.wing.shape[-1]
    has_prev = (s > 0).astype(jnp.float32)
    has_next = (s < nsy * nsx * nz - 1).astype(jnp.float32)

    mine = pl.ds(pl.multiple_of(d * half, half), half)
    theirs = pl.ds(pl.multiple_of((1 - d) * half, half), half)
    beside = pl.ds(pl.multiple_of(half - d * wide, wide), wide)
    loads = [
        (vox.at[:, :, :, mine], b.grid.at[:, 1:planes + 1]),
        (vox.at[:, :, :, beside], b.wing.at[:, 1:planes + 1]),
        (codes.at[0, :, mine], b.codes.at[0]),
        (head.at[0, :, mine], b.heading.at[0]),
        (cot.at[0, :, :, mine], b.pull.at[0]),
    ]
    loads = [pltpu.make_async_copy(a, c, lsem.at[i]) for i, (a, c) in enumerate(loads)]
    for c in loads:
        c.start()

    far_first = sorted(range(1, nz), key=lambda i: -min(i, nz - i))
    zpeer = [me._replace(sz=lax.rem(z + i, nz)) for i in far_first]
    gpeer, across = [], []
    for i in range(ng):
        g = lax.rem(gi + i, ng)
        p = me._replace(sy=g // nsx, sx=g % nsx)
        across.append(over(p))
        if i:
            gpeer.append(p)
    ready = greet([prev, nxt] + [flip(p) for p in near] + [over(prev), over(nxt)]
          + [over(flip(p)) for p in near] + zpeer + gpeer + across)

    for c in loads[:2]:
        c.wait()
    cut_faces(b, me)
    for c in loads[2:]:
        c.wait()
    weights(b, 0)
    ready()
    rays = [
        (codes.at[0, :, theirs], b.codes.at[1], mate),
        (head.at[0, :, theirs], b.heading.at[1], mate),
        (cot.at[0, :, :, theirs], b.pull.at[1], mate),
    ]
    rays = [push(x, y, hs.at[i], hr.at[i], p) for i, (x, y, p) in enumerate(rays)]
    for c in rays:
        c.start()
    inner = pl.ds(1, planes)
    beyond = [
        (b.brim.at[inner], b.rbrim.at[inner], flip(me)),
        (b.cut.at[0], b.rcut.at[0], nxt),
        (b.cut.at[1], b.rcut.at[1], prev),
        (b.brim.at[planes], b.rbrim.at[0], flip(nxt)),
        (b.brim.at[1], b.rbrim.at[ext - 1], flip(prev)),
        (b.grid.at[:, planes], b.grid.at[:, 0], nxt),
        (b.grid.at[:, 1], b.grid.at[:, ext - 1], prev),
    ]
    beyond = [push(x, y, hs.at[3 + i], hr.at[3 + i], p) for i, (x, y, p) in enumerate(beyond)]
    for c in beyond:
        c.start()
    beyond[0].wait()
    tw = half // 2
    pairs = blocks // 2
    first, late = [], []

    def rows_in(parts):
        for n, v in enumerate(parts):
            b.stack[n * rows:(n + 1) * rows] = v

    def chain(g):
        def inside(p, carry):
            sample_plane(b, me, p, (g,), inner_edges(b, me, p), None)
            return carry

        lax.fori_loop(1, planes + 1, inside, 0)
        if g == 0:
            for c in beyond[1:]:
                c.wait()

        def ends(i, carry):
            sample_plane(b, me, i * (ext - 1), (g,), outer_edges(b, me, i),
                         jnp.where(i == 0, has_prev, has_next))
            return carry

        lax.fori_loop(0, 2, ends, 0)
        total = shade_planes(b, scale, g)
        if g == 1:
            for c in rays[1:]:
                c.wait()
        for c in range(3):
            b.pull[g, c] = b.pull[g, c] * depth
        images = local_light(b, total, g)
        kept = sum(b.pull[g, c] * images[c] for c in range(3))
        b.kept[g] = kept
        sides = [slice(0, tw), slice(tw, half)]
        rows_in([v[:, x] for x in sides for v in (total, kept)])

        def put_dl(j, m, v):
            b.dl[g, j, m] = v

        tiles_out(b, nz, put_dl)
        first.append([push(b.dl.at[g, p.sz], b.rdl.at[g, z], s1.at[g * (nz - 1) + i],
                           r1.at[g * (nz - 1) + i], p) for i, p in enumerate(zpeer)])
        for c in first[g]:
            c.start()
        head_f = b.heading[g].astype(jnp.float32)
        rows_in([head_f[:, x] for x in sides for _ in range(2)])

        def put_hd(j, m, v):
            b.hd[g, j, m] = v

        tiles_out(b, nz, put_hd)
        for n, x in enumerate(sides):
            rows_in([v[:, x] for v in images])

            def put_im(j, m, v):
                b.im[g, j, n * pairs + m] = v

            tiles_out(b, nz, put_im)
        late.append([push(b.im.at[g, p.sz], b.rim.at[g, z], s2.at[g * (nz - 1) + i],
                          r2.at[g * (nz - 1) + i], p) for i, p in enumerate(zpeer)])
        for c in late[g]:
            c.start()

    chain(0)
    rays[0].wait()
    weights(b, 1)
    chain(1)
    lanes = b.dl.shape[-1]
    spot = iota(b.dl.shape[2:], 2)
    is_d = (spot // rows) % 2 == 0
    roll = lambda a, n: pltpu.roll(a, n % lanes, 2)

    def directed(parts, ahead):
        lows, low = [], jnp.zeros_like(parts[0])
        for p in parts:
            lows.append(low)
            low = low + p
        highs, high = [], jnp.zeros_like(parts[0])
        for p in reversed(parts):
            highs.append(high)
            high = high + p
        highs = highs[::-1]
        before = [jnp.where(ahead, x, y) for x, y in zip(lows, highs)]
        after = [jnp.where(ahead, y, x) for x, y in zip(lows, highs)]
        return before, after, low

    def compose(g):
        b.rdl[g, z] = b.dl[g, z]
        for c in first[g]:
            c.wait()
        ahead = b.hd[g, z] == 0
        tiles = [b.rdl[g, i] for i in range(nz)]
        before, _, dsum = directed(tiles, ahead)
        reach = [jnp.exp(-x) for x in before]
        _, later, lsum = directed([roll(r, rows) * x for r, x in zip(reach, tiles)], ahead)
        b.gm[g, gi] = jnp.where(is_d, dsum, lsum)
        copies = [push(b.gm.at[g, gi], b.gm.at[g, gi], s3.at[g * (ng - 1) + i],
                       r3.at[g * (ng - 1) + i], p) for i, p in enumerate(gpeer)]
        for c in copies:
            c.start()
        for i in range(nz):
            b.zreach[g, i] = reach[i]
            b.zlater[g, i] = later[i]
        return copies

    def conclude(g, copies):
        for c in copies:
            c.wait()
        ahead = b.hd[g, z] == 0
        groups = [b.gm[g, i] for i in range(ng)]
        before, _, _ = directed(groups, ahead)
        reach = [jnp.exp(-x) for x in before]
        _, after, _ = directed([roll(r, rows) * x for r, x in zip(reach, groups)], ahead)
        to_me = jnp.zeros_like(reach[0])
        rest = jnp.zeros_like(reach[0])
        for i in range(ng):
            to_me = jnp.where(gi == i, reach[i], to_me)
            rest = jnp.where(gi == i, after[i], rest)
        to_me_l = roll(to_me, rows)
        for i in range(nz):
            b.ret[g, i] = jnp.where(is_d, to_me * b.zreach[g, i],
                                    rest + to_me_l * b.zlater[g, i])
        copies = [push(b.ret.at[g, p.sz], b.rb.at[g, z], s4.at[g * (nz - 1) + i],
                       r4.at[g * (nz - 1) + i], p) for i, p in enumerate(zpeer)]
        for c in copies:
            c.start()
        b.rb[g, z] = b.ret[g, z]
        return copies

    second0 = compose(0)
    prepare(b, 0)
    gather_seam(b, me, 0)
    b.rim[0, z] = b.im[0, z]
    second1 = compose(1)
    back0 = conclude(0, second0)
    prepare(b, 1)
    back1 = conclude(1, second1)
    b.rim[1, z] = b.im[1, z]
    gather_seam(b, me, 1)
    for g, back in enumerate((back0, back1)):
        for c in back:
            c.wait()
        for i in range(tw // 8):
            b.tile[8 * i:8 * i + 8] = b.rb[g, i % nz, i // nz]
        turned = b.tile[...].T
        for n in range(4):
            x, q = n // 2, n % 2
            b.lit[g, q, :, x * tw:(x + 1) * tw] = turned[n * rows:(n + 1) * rows]
    def spread_ends(i, carry):
        spill_plane(b, me, i * (ext - 1))
        return carry

    lax.fori_loop(0, 2, spread_ends, 0)
    faces = [
        (b.out.at[:, ext - 1], b.fp, nxt), (b.out.at[:, 0], b.fn, prev),
        (b.line.at[ext - 1], b.zline.at[0], flip(nxt)), (b.line.at[0], b.zline.at[1], flip(prev)),
    ]
    faces = [push(x, y, ss.at[6 + i], sr.at[6 + i], p) for i, (x, y, p) in enumerate(faces)]
    for c in faces:
        c.start()

    spill_seam(b, me)
    small = b.turn.at[ch * planes:ch * planes + 8]
    spill = [
        (b.turn.at[0:ch * planes], b.rin, over(me)),
        (b.pack.at[rows:rows + 8], b.rfar, over(flip(me))),
    ]
    for i, p in enumerate((nxt, prev)):
        spill.append((small, b.rzin.at[i], over(p)))
        spill.append((small, b.rzfar.at[i], over(flip(p))))
    spill = [push(x, y, ss.at[i], sr.at[i], p) for i, (x, y, p) in enumerate(spill)]
    for c in spill:
        c.start()

    for c in late[0] + late[1]:
        c.wait()
    quarter = spot // rows
    for g in range(2):
        for x in range(2):
            total = jnp.zeros(b.dl.shape[2:], jnp.float32)
            for i in range(nz):
                src = b.ret[g, i]
                wash = roll(src, -2 * x * rows)
                wash = jnp.where(quarter == 1, roll(src, (1 - 2 * x) * rows), wash)
                wash = jnp.where(quarter == 2, roll(src, (2 - 2 * x) * rows), wash)
                total = total + wash * b.rim[g, i, x * pairs:(x + 1) * pairs]
            b.part[g, x * pairs:(x + 1) * pairs] = total
    half_of_me = gi // blocks
    out = []
    for g in range(2):
        for m in range(blocks):
            q = blocks * d + m
            peer = me._replace(dir=d if g == 0 else 1 - d, sy=q // nsx, sx=q % nsx)
            out.append(push(b.part.at[g, m], b.rpart.at[gi],
                            s5.at[g * blocks + m], r5.at[gi], peer))
    for g in range(2):
        for m in range(blocks):
            copy = out[g * blocks + m]
            if g == 0:
                itself = gi == blocks * d + m

                @pl.when(itself)
                def _():
                    b.rpart[gi] = b.part[0, m]

                @pl.when(jnp.logical_not(itself))
                def _():
                    copy.start()
            else:
                copy.start()

    def spread(p, carry):
        spill_plane(b, me, p)
        return carry

    lax.fori_loop(1, planes + 1, spread, 0)
    lines = push(b.line.at[inner], b.rline, ss.at[10], sr.at[10], flip(me))
    lines.start()
    spill = spill + faces + [lines]

    for g in range(2):
        for m in range(blocks):
            copy = out[g * blocks + m]
            if g == 0:
                @pl.when(gi != blocks * d + m)
                def _():
                    copy.wait_send()
            else:
                copy.wait_send()
    for i in range(ng):
        arrive = push(b.part.at[0, 0], b.rpart.at[i], s5.at[0], r5.at[i], over(me))

        @pl.when(jnp.logical_or(half_of_me != d, gi != i))
        def _():
            arrive.wait_recv()
    total = b.rpart[0]
    for i in range(1, ng):
        total = total + b.rpart[i]
    for c in range(3):
        img[c] = total[:, c * rows:(c + 1) * rows]
    for c in spill:
        c.wait()
    gather_spill(b, me, has_prev, has_next, grad)


def per_device(voxels, offsets, heading, cotangent):
    ch, planes, rows, total = voxels.shape
    nsy, nsx, nz = (lax.axis_size(a) for a in SLAB)
    ng = nsy * nsx
    depth = planes * nz * ng
    half = total // 2
    wide = half // 2
    room = shapes(ch, planes, rows, half, wide, nz, ng)
    dma = lambda n: pltpu.SemaphoreType.DMA((n,))
    grad, img = pl.pallas_call(
        functools.partial(render_kernel, 2.0 / depth, float(depth), tuple(room)),
        out_shape=(pltpu.VMEM((ch, planes, rows, half), jnp.float32),
                   pltpu.VMEM((3, 8, rows), jnp.float32)),
        in_specs=[HBM] * 4,
        out_specs=(VM, VM),
        scratch_shapes=list(room.values()) + [
            dma(5), dma(10), dma(10),
            dma(2 * nz - 2), dma(2 * nz - 2), dma(2 * nz - 2), dma(2 * nz - 2),
            dma(2 * ng - 2), dma(2 * ng - 2), dma(2 * nz - 2), dma(2 * nz - 2),
            dma(ng), dma(ng), dma(11), dma(11),
        ],
        compiler_params=pltpu.CompilerParams(
            collective_id=0, has_side_effects=True, vmem_limit_bytes=58 * 1024 * 1024
        ),
    )(voxels, offsets, heading, cotangent)
    image = jnp.swapaxes(img, 1, 2)[None]
    return (image, grad)


def solution(mesh):
    n = mesh.devices.size
    shape = (2, 4, 2, 8, 2) if n == 256 else (2,) * 5
    finer = Mesh(mesh.devices.reshape(shape), AXES)
    return jax.shard_map(
        per_device,
        mesh=finer,
        in_specs=(
            P(None, SLAB, "tile", None),
            P("dir", "tile", None),
            P("dir", "tile", None),
            P("dir", None, "tile", None),
        ),
        out_specs=(P("dir", None, "tile", SLAB), P(None, SLAB, "tile", "dir")),
        check_vma=False,
    )
```

```python
import functools
from types import SimpleNamespace
from typing import NamedTuple

import jax
import jax.numpy as jnp
from jax import lax
from jax.experimental import pallas as pl
from jax.experimental.pallas import tpu as pltpu
from jax.sharding import Mesh
from jax.sharding import PartitionSpec as P

LEVELS = 8
SIDE = 128
AXES = ("dir", "sy", "sx", "sz", "tile")
SLAB = AXES[1:4]
MESH = pl.DeviceIdType.MESH
HBM = pl.BlockSpec(memory_space=pltpu.HBM)
VM = pl.BlockSpec(memory_space=pltpu.VMEM)


class Place(NamedTuple):
    dir: int
    sy: int
    sx: int
    sz: int
    tile: int


def places():
    return Place(*[lax.axis_index(a) for a in AXES])


def slab_index(me):
    _, _, sx, sz, _ = (lax.axis_size(a) for a in AXES)
    return (me.sy * sx + me.sx) * sz + me.sz


def at_slab(me, step):
    sy, sx, sz = (lax.axis_size(a) for a in SLAB)
    s = lax.rem(slab_index(me) + step + sy * sx * sz, sy * sx * sz)
    return me._replace(sy=s // (sx * sz), sx=(s // sz) % sx, sz=s % sz)


def greet(peers):
    barrier = pltpu.get_barrier_semaphore()
    for peer in peers:
        pl.semaphore_signal(barrier, inc=1, device_id=tuple(peer), device_id_type=MESH)
    return lambda: pl.semaphore_wait(barrier, len(peers))


def push(src, dst, send, recv, peer):
    return pltpu.make_async_remote_copy(
        src_ref=src, dst_ref=dst, send_sem=send, recv_sem=recv,
        device_id=tuple(peer), device_id_type=MESH,
    )


def shapes(ch, planes, rows, half, wide, nz, ng):
    lanes, m = 4 * rows, half // 8 // nz
    pairs = m // 2
    ext = planes + 2
    f32 = jnp.float32
    one = dict(
        grid=(ch, ext, rows, half), wing=(ch, ext, rows, wide),
        cut=(2, rows, wide), rcut=(2, rows, wide), brim=(ext, ch, half + wide),
        rbrim=(ext, ch, half + wide),
        shift=(8, ch, ext, rows, half),
        plane=(2, ch, ext, rows, half), tail=(2, ext, rows, half),
        sigma=(2, planes, rows, half), colour=(2, 3, planes, rows, half),
        through=(2, planes, rows, half), glow=(2, planes, rows, half),
        taps=(2, 9, rows, half), pair=(2, 7, rows, half), kept=(2, rows, half),
        codes=(2, rows, half), heading=(2, rows, half), pull=(2, 3, rows, half),
        ahead=(2, planes, rows, half), stack=(lanes, wide), tile=(wide, lanes),
        diff=(2, ch + 1, planes + 4, rows, half), out=(ch, ext, rows, half),
        lit=(2, 2, rows, half), seam=(2, 2, rows, SIDE),
        line=(ext, ch, half), pack=(SIDE, SIDE), turn=(SIDE, SIDE),
        fp=(ch, rows, half), fn=(ch, rows, half),
        rline=(planes, ch, half), zline=(2, ch, half), rin=(ch * planes, SIDE),
        rfar=(8, SIDE), rzin=(2, 8, SIDE), rzfar=(2, 8, SIDE),
        dl=(2, nz, pairs, 8, lanes), hd=(2, nz, pairs, 8, lanes), rdl=(2, nz, pairs, 8, lanes),
        im=(2, nz, m, 8, lanes), rim=(2, nz, m, 8, lanes), gm=(2, ng, pairs, 8, lanes),
        zreach=(2, nz, pairs, 8, lanes), zlater=(2, nz, pairs, 8, lanes),
        ret=(2, nz, pairs, 8, lanes), rb=(2, nz, pairs, 8, lanes),
        part=(2, m, 8, lanes), rpart=(ng, 8, lanes),
    )
    ints = dict(codes=0, heading=0)
    return {k: pltpu.VMEM(v, jnp.int32 if k in ints else f32) for k, v in one.items()}


def weights(b, g):
    level = LEVELS
    q = b.codes[g]
    frac = lambda raw: (raw.astype(jnp.float32) + 0.5) / level - 0.5
    fz, fy, fx = frac(q & 7), frac((q >> 3) & 7), frac(q >> 6)
    three = lambda f: (jnp.maximum(-f, 0.0), 1.0 - jnp.abs(f), jnp.maximum(f, 0.0))
    wy, wx = three(fy), three(fx)
    for i in range(3):
        for j in range(3):
            b.taps[g, 3 * i + j] = wy[i] * wx[j]
    ay, ax = jnp.abs(fy), jnp.abs(fx)
    for i, v in enumerate((fz, fy, fx, wy[1] * wx[1], wy[1] * ax, ay * wx[1], ay * ax)):
        b.pair[g, i] = v


def iota(shape, dim):
    return lax.broadcasted_iota(jnp.int32, shape, dim)


def lane_of(d, r):
    return jnp.where(d == 0, r[..., 0:1], r[..., r.shape[-1] - 1:])


def inner_edges(b, me, p):
    return lambda c: jnp.broadcast_to(lane_of(me.dir, b.wing[c, p]), b.wing.shape[2:])


def outer_edges(b, me, i):
    return lambda c: jnp.broadcast_to(b.rcut[i][:, c:c + 1], b.wing.shape[2:])


def cut_faces(b, me):
    ch, ext, rows, half = b.grid.shape
    wide = b.wing.shape[3]
    slot = iota((rows, wide), 1)
    for i, p in enumerate((ext - 2, 1)):
        acc = jnp.zeros((rows, wide), jnp.float32)
        for c in range(ch):
            acc = jnp.where(slot == c, inner_edges(b, me, p)(c), acc)
        b.cut[i] = acc

    def trim(p, carry):
        pick = lambda r: jnp.where(me.tile == 0, r[rows - 1:rows], r[0:1])
        for c in range(ch):
            b.brim[p, c:c + 1, :half] = pick(b.grid[c, p])
            b.brim[p, c:c + 1, half:] = pick(b.wing[c, p])
        return carry

    lax.fori_loop(1, ext - 1, trim, 0)


def sample_plane(b, me, p, gs, edges, keep):
    ch, _, rows, half = b.grid.shape
    tw = half // 2
    d, t = me.dir, me.tile
    row, lane = iota((rows, tw), 0), iota((rows, tw), 1)
    right = (d == 0).astype(jnp.float32)
    left = 1.0 - right
    under = (t == 0).astype(jnp.float32)
    over = 1.0 - under
    for c in range(ch):
        edge, line = edges(c), b.rbrim[p, c:c + 1, :]
        corner = jnp.broadcast_to(lane_of(d, line[:, half:]), (1, tw))
        m = [b.grid[c, p, :, x * tw:(x + 1) * tw] for x in range(2)] + [edge]
        far = [line[:, :tw], line[:, tw:half], corner]
        up = [jnp.where(row == 0, f * over, pltpu.roll(a, 1, 0)) for a, f in zip(m, far)]
        dn = [jnp.where(row == rows - 1, f * under, pltpu.roll(a, rows - 1, 0))
              for a, f in zip(m, far)]
        spread = []
        for a in (up, m, dn):
            r = [pltpu.roll(a[x], 1, 1) for x in range(2)]
            l = [pltpu.roll(a[x], tw - 1, 1) for x in range(2)]
            lo = [jnp.where(lane == 0, a[2] * left, r[0]), jnp.where(lane == 0, r[0], r[1])]
            hi = [jnp.where(lane == tw - 1, l[1], l[0]),
                  jnp.where(lane == tw - 1, a[2] * right, l[1])]
            spread.append((lo, a[:2], hi))
        for n, v in enumerate([up, dn] + [q[0] for q in spread] + [q[2] for q in spread]):
            b.shift[n, c, p, :, :tw] = v[0]
            b.shift[n, c, p, :, tw:] = v[1]
        for x in range(2):
            at = slice(x * tw, (x + 1) * tw)
            for g in gs:
                fy, fx = b.pair[g, 1, :, at], b.pair[g, 2, :, at]
                w00, w01 = b.pair[g, 3, :, at], b.pair[g, 4, :, at]
                w10, w11 = b.pair[g, 5, :, at], b.pair[g, 6, :, at]
                side = lambda s: jnp.where(fx > 0, s[2][x], s[0][x])
                down = fy > 0
                v = (w00 * m[x] + w01 * side(spread[1])
                     + w10 * jnp.where(down, dn[x], up[x])
                     + w11 * jnp.where(down, side(spread[2]), side(spread[0])))
                b.plane[g, c, p, :, at] = v if keep is None else v * keep


def sample_again(b, p, g, keep):
    right, down = b.pair[g, 2] > 0, b.pair[g, 1] > 0
    for c in range(b.grid.shape[0]):
        up, dn, *sides = [b.shift[n, c, p] for n in range(8)]
        side = [jnp.where(right, sides[n + 3], sides[n]) for n in range(3)]
        v = (b.pair[g, 3] * b.grid[c, p] + b.pair[g, 4] * side[1]
             + b.pair[g, 5] * jnp.where(down, dn, up)
             + b.pair[g, 6] * jnp.where(down, side[2], side[0]))
        b.plane[g, c, p] = v if keep is None else v * keep


def shade_planes(b, scale, g):
    _, ch, ext, rows, half = b.plane.shape
    fz = b.pair[g, 0]
    az = jnp.abs(fz)

    def step(k, acc):
        v = []
        for c in range(ch):
            far = jnp.where(fz > 0, b.plane[g, c, k + 2], b.plane[g, c, k])
            v.append((1.0 - az) * b.plane[g, c, k + 1] + az * far)
        sg = (jnp.maximum(v[0], 0.0) + jnp.log(1.0 + jnp.exp(-jnp.abs(v[0])))) * scale
        b.sigma[g, k] = sg
        b.diff[g, ch, k + 2] = (0.5 + 0.5 * jnp.tanh(0.5 * v[0])) * scale
        for c in range(3):
            b.colour[g, c, k] = 0.5 + 0.5 * jnp.tanh(0.5 * v[c + 1])
        b.ahead[g, k] = acc
        return acc + sg

    return lax.fori_loop(0, ext - 2, step, jnp.zeros((rows, half), jnp.float32))


def local_light(b, total, g):
    _, planes, rows, half = b.sigma.shape
    forward = b.heading[g] == 0

    def step(k, acc):
        sg, ah = b.sigma[g, k], b.ahead[g, k]
        front = jnp.where(forward, ah, total - ah - sg)
        th = jnp.exp(-front)
        gl = th * (1.0 - jnp.exp(-sg))
        b.through[g, k] = th
        b.glow[g, k] = gl
        return tuple(acc[c] + gl * b.colour[g, c, k] for c in range(3))

    zero = jnp.zeros((rows, half), jnp.float32)
    return lax.fori_loop(0, planes, step, (zero,) * 3)


def tiles_out(b, nz, put):
    turned = b.stack[...].T
    for i in range(turned.shape[0] // 8):
        put(i % nz, i // nz, turned[8 * i:8 * i + 8])


def prepare(b, g):
    _, planes, rows, half = b.sigma.shape
    ch = b.grid.shape[0]
    zero = jnp.zeros((rows, half), jnp.float32)
    forward = b.heading[g] == 0
    whole = b.kept[g]
    for c in range(ch + 1):
        for k in (0, 1, planes + 2, planes + 3):
            b.diff[g, c, k] = zero

    def step(k, before):
        pull = [b.pull[g, c] for c in range(3)]
        col = [b.colour[g, c, k] for c in range(3)]
        shade = pull[0] * col[0] + pull[1] * col[1] + pull[2] * col[2]
        th, gl = b.through[g, k], b.glow[g, k]
        share = gl * shade
        later = jnp.where(forward, whole - before - share, before)
        b.diff[g, 0, k + 2] = ((th - gl) * shade - later) * b.diff[g, ch, k + 2]
        for c in range(3):
            b.diff[g, c + 1, k + 2] = pull[c] * gl * (col[c] * (1.0 - col[c]))
        return before + share

    lax.fori_loop(0, planes, step, zero)

    def mix(p, carry):
        fz = b.pair[g, 0]
        mid, up, down = 1.0 - jnp.abs(fz), jnp.maximum(fz, 0.0), jnp.maximum(-fz, 0.0)
        for c in range(ch + 1):
            v = mid * b.diff[g, c, p + 1] + up * b.diff[g, c, p] + down * b.diff[g, c, p + 2]
            if c < ch:
                b.plane[g, c, p] = v
            else:
                b.tail[g, p] = v
        return carry

    lax.fori_loop(0, planes + 2, mix, 0)


def seam_slot(c, p, ch, planes):
    if p == 0:
        return ch * planes + c
    return ch * planes + ch + c if p == planes + 1 else c * planes + p - 1


def seam_of(d, r):
    return jnp.where(d == 0, r[..., r.shape[-1] - 1:], r[..., 0:1])


def gather_seam(b, me, g):
    _, ch, ext, rows, half = b.plane.shape
    slot = iota((rows, SIDE), 1)
    wide = lambda v: jnp.broadcast_to(seam_of(me.dir, v), (rows, SIDE))
    a = jnp.zeros((rows, SIDE), jnp.float32)
    r = a
    for p in range(ext):
        for c in range(ch):
            a = jnp.where(slot == seam_slot(c, p, ch, ext - 2), wide(b.plane[g, c, p]), a)
        r = jnp.where(slot == seam_slot(0, p, ch, ext - 2), wide(b.tail[g, p]), r)
    b.seam[g, 0] = a
    b.seam[g, 1] = r


def spill_seam(b, me):
    _, ch, ext, rows, half = b.plane.shape
    d, t = me.dir, me.tile
    row = iota((rows, SIDE), 0)
    wide = lambda v: jnp.broadcast_to(seam_of(d, v), (rows, SIDE))
    cols = [wide(b.lit[g, 0]) * b.seam[g, 0] - wide(b.lit[g, 1]) * b.seam[g, 1] for g in range(2)]
    bands = []
    for i in range(3):
        w = [jnp.where(d == 0, b.taps[g, 3 * i + 2, :, half - 1:half], b.taps[g, 3 * i, :, 0:1])
             for g in range(2)]
        bands.append(sum(jnp.broadcast_to(w[g], (rows, SIDE)) * cols[g] for g in range(2)))
    up = pltpu.roll(bands[0], rows - 1, 0)
    dn = pltpu.roll(bands[2], 1, 0)
    b.pack[:rows] = (bands[1] + jnp.where(row == rows - 1, 0.0, up) + jnp.where(row == 0, 0.0, dn))
    b.pack[rows:rows + 1] = jnp.where(t == 0, dn[0:1], up[rows - 1:rows])
    b.turn[...] = b.pack[...].T


def spill_plane(b, me, p):
    ch, ext, rows, half = b.out.shape
    tw = half // 2
    t = me.tile
    row, lane = iota((rows, tw), 0), iota((rows, tw), 1)
    for c in range(ch):
        cols = []
        for g in range(2):
            v = b.lit[g, 0] * b.plane[g, c, p]
            cols.append(v if c else v - b.lit[g, 1] * b.tail[g, p])
        bands = []
        for i in range(3):
            u = []
            for j in range(3):
                full = b.taps[0, 3 * i + j] * cols[0] + b.taps[1, 3 * i + j] * cols[1]
                u.append([full[:, :tw], full[:, tw:]])
            l = [pltpu.roll(a, tw - 1, 1) for a in u[0]]
            r = [pltpu.roll(a, 1, 1) for a in u[2]]
            x0 = u[1][0] + jnp.where(lane == tw - 1, l[1], l[0]) + jnp.where(lane == 0, 0.0, r[0])
            x1 = u[1][1] + jnp.where(lane == tw - 1, 0.0, l[1]) + jnp.where(lane == 0, r[0], r[1])
            bands.append([x0, x1])
        for x in range(2):
            at = slice(x * tw, (x + 1) * tw)
            up = pltpu.roll(bands[0][x], rows - 1, 0)
            dn = pltpu.roll(bands[2][x], 1, 0)
            b.out[c, p, :, at] = (bands[1][x] + jnp.where(row == rows - 1, 0.0, up)
                                  + jnp.where(row == 0, 0.0, dn))
            b.line[p, c:c + 1, at] = jnp.where(t == 0, dn[0:1], up[rows - 1:rows])


def gather_spill(b, me, has_prev, has_next, dest):
    ch, ext, rows, half = b.out.shape
    planes = ext - 2
    tw = half // 2
    d, t = me.dir, me.tile
    touch = (1 - t) * (rows - 1)
    seam = (1 - d) * (half - 1)
    row = iota((rows, tw), 0)
    lane = iota((rows, tw), 1)
    spot = iota((1, SIDE), 1)
    b.turn[:ch * planes] = b.rin[...]
    for c in range(ch):
        for k, i, r, has in ((0, 0, ch + c, has_prev), (planes - 1, 1, c, has_next)):
            far = jnp.broadcast_to(b.rzfar[i, r:r + 1, rows:rows + 1], (1, SIDE))
            add = jnp.where(spot < rows, b.rzin[i, r:r + 1], 0.0) + jnp.where(spot == touch, far, 0.0)
            j = c * planes + k
            b.turn[j:j + 1] = b.turn[j:j + 1] + add * has
    col = b.turn[...].T[:rows]
    col = col + jnp.where(iota((rows, SIDE), 0) == touch, jnp.broadcast_to(b.rfar[0:1], (rows, SIDE)), 0.0)
    for c in range(ch):
        for k in range(planes):
            pos = c * planes + k
            extra = b.rline[k, c:c + 1]
            v = b.out[c, k + 1]
            if k == 0:
                extra = extra + b.zline[0, c:c + 1] * has_prev
                v = v + b.fp[c] * has_prev
            if k == planes - 1:
                extra = extra + b.zline[1, c:c + 1] * has_next
                v = v + b.fn[c] * has_next
            bar = jnp.broadcast_to(col[:, pos:pos + 1], (rows, tw))
            for x in range(2):
                at = slice(x * tw, (x + 1) * tw)
                y = v[:, at] + jnp.where(row == touch, jnp.broadcast_to(extra[:, at], (rows, tw)), 0.0)
                y = y + jnp.where(lane + x * tw == seam, bar, 0.0)
                dest[c, k, :, at] = y


def render_kernel(scale, depth, names, vox, codes, head, cot, grad, img, *scratch):
    b = SimpleNamespace(**dict(zip(names, scratch)))
    sems = scratch[len(names):]
    (lsem, hs, hr, s1, r1, s2, r2, s3, r3, s4, r4, s5, r5, ss, sr) = sems
    me = places()
    nsy, nsx, nz = (lax.axis_size(a) for a in SLAB)
    ng = nsy * nsx
    blocks = ng // 2
    d, t, z = me.dir, me.tile, me.sz
    gi = me.sy * nsx + me.sx
    s = slab_index(me)
    prev, nxt = at_slab(me, -1), at_slab(me, 1)
    flip = lambda p: p._replace(tile=1 - p.tile)
    over = lambda p: p._replace(dir=1 - p.dir)
    near = [prev, me, nxt]
    mate = me._replace(dir=1 - d, sx=nsx - 1 - me.sx)
    ch, ext, rows, half = b.grid.shape
    planes = ext - 2
    wide = b.wing.shape[-1]
    has_prev = (s > 0).astype(jnp.float32)
    has_next = (s < nsy * nsx * nz - 1).astype(jnp.float32)

    mine = pl.ds(pl.multiple_of(d * half, half), half)
    theirs = pl.ds(pl.multiple_of((1 - d) * half, half), half)
    beside = pl.ds(pl.multiple_of(half - d * wide, wide), wide)
    loads = [
        (vox.at[:, :, :, mine], b.grid.at[:, 1:planes + 1]),
        (vox.at[:, :, :, beside], b.wing.at[:, 1:planes + 1]),
        (codes.at[0, :, mine], b.codes.at[0]),
        (head.at[0, :, mine], b.heading.at[0]),
        (cot.at[0, :, :, mine], b.pull.at[0]),
    ]
    loads = [pltpu.make_async_copy(a, c, lsem.at[i]) for i, (a, c) in enumerate(loads)]
    for c in loads:
        c.start()

    far_first = sorted(range(1, nz), key=lambda i: -min(i, nz - i))
    zpeer = [me._replace(sz=lax.rem(z + i, nz)) for i in far_first]
    gpeer, across = [], []
    for i in range(ng):
        g = lax.rem(gi + i, ng)
        p = me._replace(sy=g // nsx, sx=g % nsx)
        across.append(over(p))
        if i:
            gpeer.append(p)
    ready = greet([prev, nxt] + [flip(p) for p in near] + [over(prev), over(nxt)]
          + [over(flip(p)) for p in near] + zpeer + gpeer + across)

    for c in loads[:2]:
        c.wait()
    cut_faces(b, me)
    for c in loads[2:]:
        c.wait()
    weights(b, 0)
    ready()
    rays = [
        (codes.at[0, :, theirs], b.codes.at[1], mate),
        (head.at[0, :, theirs], b.heading.at[1], mate),
        (cot.at[0, :, :, theirs], b.pull.at[1], mate),
    ]
    rays = [push(x, y, hs.at[i], hr.at[i], p) for i, (x, y, p) in enumerate(rays)]
    for c in rays:
        c.start()
    inner = pl.ds(1, planes)
    beyond = [
        (b.brim.at[inner], b.rbrim.at[inner], flip(me)),
        (b.cut.at[0], b.rcut.at[0], nxt),
        (b.cut.at[1], b.rcut.at[1], prev),
        (b.brim.at[planes], b.rbrim.at[0], flip(nxt)),
        (b.brim.at[1], b.rbrim.at[ext - 1], flip(prev)),
        (b.grid.at[:, planes], b.grid.at[:, 0], nxt),
        (b.grid.at[:, 1], b.grid.at[:, ext - 1], prev),
    ]
    beyond = [push(x, y, hs.at[3 + i], hr.at[3 + i], p) for i, (x, y, p) in enumerate(beyond)]
    for c in beyond:
        c.start()
    beyond[0].wait()
    tw = half // 2
    pairs = blocks // 2
    first, late = [], []

    def rows_in(parts):
        for n, v in enumerate(parts):
            b.stack[n * rows:(n + 1) * rows] = v

    def chain(g):
        def inside(p, carry):
            if g == 0:
                sample_plane(b, me, p, (g,), inner_edges(b, me, p), None)
            else:
                sample_again(b, p, g, None)
            return carry

        lax.fori_loop(1, planes + 1, inside, 0)
        if g == 0:
            for c in beyond[1:]:
                c.wait()

        def ends(i, carry):
            keep = jnp.where(i == 0, has_prev, has_next)
            if g == 0:
                sample_plane(b, me, i * (ext - 1), (g,), outer_edges(b, me, i), keep)
            else:
                sample_again(b, i * (ext - 1), g, keep)
            return carry

        lax.fori_loop(0, 2, ends, 0)
        total = shade_planes(b, scale, g)
        if g == 1:
            for c in rays[1:]:
                c.wait()
        for c in range(3):
            b.pull[g, c] = b.pull[g, c] * depth
        images = local_light(b, total, g)
        kept = sum(b.pull[g, c] * images[c] for c in range(3))
        b.kept[g] = kept
        sides = [slice(0, tw), slice(tw, half)]
        rows_in([v[:, x] for x in sides for v in (total, kept)])

        def put_dl(j, m, v):
            b.dl[g, j, m] = v

        tiles_out(b, nz, put_dl)
        first.append([push(b.dl.at[g, p.sz], b.rdl.at[g, z], s1.at[g * (nz - 1) + i],
                           r1.at[g * (nz - 1) + i], p) for i, p in enumerate(zpeer)])
        for c in first[g]:
            c.start()
        head_f = b.heading[g].astype(jnp.float32)
        rows_in([head_f[:, x] for x in sides for _ in range(2)])

        def put_hd(j, m, v):
            b.hd[g, j, m] = v

        tiles_out(b, nz, put_hd)
        for n, x in enumerate(sides):
            rows_in([v[:, x] for v in images])

            def put_im(j, m, v):
                b.im[g, j, n * pairs + m] = v

            tiles_out(b, nz, put_im)
        late.append([push(b.im.at[g, p.sz], b.rim.at[g, z], s2.at[g * (nz - 1) + i],
                          r2.at[g * (nz - 1) + i], p) for i, p in enumerate(zpeer)])
        if g == 0:
            for c in late[g]:
                c.start()

    chain(0)
    rays[0].wait()
    weights(b, 1)
    chain(1)
    lanes = b.dl.shape[-1]
    spot = iota(b.dl.shape[2:], 2)
    is_d = (spot // rows) % 2 == 0
    roll = lambda a, n: pltpu.roll(a, n % lanes, 2)

    def directed(parts, ahead):
        lows, low = [], jnp.zeros_like(parts[0])
        for p in parts:
            lows.append(low)
            low = low + p
        highs, high = [], jnp.zeros_like(parts[0])
        for p in reversed(parts):
            highs.append(high)
            high = high + p
        highs = highs[::-1]
        before = [jnp.where(ahead, x, y) for x, y in zip(lows, highs)]
        after = [jnp.where(ahead, y, x) for x, y in zip(lows, highs)]
        return before, after, low

    def compose(g):
        b.rdl[g, z] = b.dl[g, z]
        for c in first[g]:
            c.wait()
        ahead = b.hd[g, z] == 0
        tiles = [b.rdl[g, i] for i in range(nz)]
        before, _, dsum = directed(tiles, ahead)
        reach = [jnp.exp(-x) for x in before]
        _, later, lsum = directed([roll(r, rows) * x for r, x in zip(reach, tiles)], ahead)
        b.gm[g, gi] = jnp.where(is_d, dsum, lsum)
        copies = [push(b.gm.at[g, gi], b.gm.at[g, gi], s3.at[g * (ng - 1) + i],
                       r3.at[g * (ng - 1) + i], p) for i, p in enumerate(gpeer)]
        for c in copies:
            c.start()
        for i in range(nz):
            b.zreach[g, i] = reach[i]
            b.zlater[g, i] = later[i]
        return copies

    def conclude(g, copies):
        for c in copies:
            c.wait()
        ahead = b.hd[g, z] == 0
        groups = [b.gm[g, i] for i in range(ng)]
        before, _, _ = directed(groups, ahead)
        reach = [jnp.exp(-x) for x in before]
        _, after, _ = directed([roll(r, rows) * x for r, x in zip(reach, groups)], ahead)
        to_me = jnp.zeros_like(reach[0])
        rest = jnp.zeros_like(reach[0])
        for i in range(ng):
            to_me = jnp.where(gi == i, reach[i], to_me)
            rest = jnp.where(gi == i, after[i], rest)
        to_me_l = roll(to_me, rows)
        for i in range(nz):
            b.ret[g, i] = jnp.where(is_d, to_me * b.zreach[g, i],
                                    rest + to_me_l * b.zlater[g, i])
        copies = [push(b.ret.at[g, p.sz], b.rb.at[g, z], s4.at[g * (nz - 1) + i],
                       r4.at[g * (nz - 1) + i], p) for i, p in enumerate(zpeer)]
        for c in copies:
            c.start()
        b.rb[g, z] = b.ret[g, z]
        return copies

    second0 = compose(0)
    prepare(b, 0)
    gather_seam(b, me, 0)
    b.rim[0, z] = b.im[0, z]
    second1 = compose(1)
    back0 = conclude(0, second0)
    prepare(b, 1)
    back1 = conclude(1, second1)
    for c in late[1]:
        c.start()
    b.rim[1, z] = b.im[1, z]
    gather_seam(b, me, 1)
    for g, back in enumerate((back0, back1)):
        for c in back:
            c.wait()
        for i in range(tw // 8):
            b.tile[8 * i:8 * i + 8] = b.rb[g, i % nz, i // nz]
        turned = b.tile[...].T
        for n in range(4):
            x, q = n // 2, n % 2
            b.lit[g, q, :, x * tw:(x + 1) * tw] = turned[n * rows:(n + 1) * rows]
    faces = []
    for i, (p, to, r, zl) in enumerate(((ext - 1, nxt, b.fp, 0), (0, prev, b.fn, 1))):
        spill_plane(b, me, p)
        faces += [push(b.out.at[:, p], r, ss.at[6 + 2 * i], sr.at[6 + 2 * i], to),
                  push(b.line.at[p], b.zline.at[zl], ss.at[7 + 2 * i], sr.at[7 + 2 * i], flip(to))]
        for c in faces[2 * i:]:
            c.start()
    spill_seam(b, me)
    small = b.turn.at[ch * planes:ch * planes + 8]
    spill = [
        (b.turn.at[0:ch * planes], b.rin, over(me)),
        (b.pack.at[rows:rows + 8], b.rfar, over(flip(me))),
    ]
    for i, p in enumerate((nxt, prev)):
        spill.append((small, b.rzin.at[i], over(p)))
        spill.append((small, b.rzfar.at[i], over(flip(p))))
    spill = [push(x, y, ss.at[i], sr.at[i], p) for i, (x, y, p) in enumerate(spill)]
    for c in spill:
        c.start()

    for c in late[0] + late[1]:
        c.wait()
    quarter = spot // rows
    for g in range(2):
        for x in range(2):
            total = jnp.zeros(b.dl.shape[2:], jnp.float32)
            for i in range(nz):
                src = b.ret[g, i]
                wash = roll(src, -2 * x * rows)
                wash = jnp.where(quarter == 1, roll(src, (1 - 2 * x) * rows), wash)
                wash = jnp.where(quarter == 2, roll(src, (2 - 2 * x) * rows), wash)
                total = total + wash * b.rim[g, i, x * pairs:(x + 1) * pairs]
            b.part[g, x * pairs:(x + 1) * pairs] = total
    half_of_me = gi // blocks
    out = []
    for g in range(2):
        for m in range(blocks):
            q = blocks * d + m
            peer = me._replace(dir=d if g == 0 else 1 - d, sy=q // nsx, sx=q % nsx)
            out.append(push(b.part.at[g, m], b.rpart.at[gi],
                            s5.at[g * blocks + m], r5.at[gi], peer))
    for g in range(2):
        for m in range(blocks):
            copy = out[g * blocks + m]
            if g == 0:
                itself = gi == blocks * d + m

                @pl.when(itself)
                def _():
                    b.rpart[gi] = b.part[0, m]

                @pl.when(jnp.logical_not(itself))
                def _():
                    copy.start()
            else:
                copy.start()

    def spread(p, carry):
        spill_plane(b, me, p)
        return carry

    lax.fori_loop(1, planes + 1, spread, 0)
    lines = push(b.line.at[inner], b.rline, ss.at[10], sr.at[10], flip(me))
    lines.start()
    spill = spill + faces + [lines]

    for g in range(2):
        for m in range(blocks):
            copy = out[g * blocks + m]
            if g == 0:
                @pl.when(gi != blocks * d + m)
                def _():
                    copy.wait_send()
            else:
                copy.wait_send()
    for i in range(ng):
        arrive = push(b.part.at[0, 0], b.rpart.at[i], s5.at[0], r5.at[i], over(me))

        @pl.when(jnp.logical_or(half_of_me != d, gi != i))
        def _():
            arrive.wait_recv()
    total = b.rpart[0]
    for i in range(1, ng):
        total = total + b.rpart[i]
    for c in range(3):
        img[c] = total[:, c * rows:(c + 1) * rows]
    for c in spill:
        c.wait()
    gather_spill(b, me, has_prev, has_next, grad)


def per_device(voxels, offsets, heading, cotangent):
    ch, planes, rows, total = voxels.shape
    nsy, nsx, nz = (lax.axis_size(a) for a in SLAB)
    ng = nsy * nsx
    depth = planes * nz * ng
    half = total // 2
    wide = half // 2
    room = shapes(ch, planes, rows, half, wide, nz, ng)
    dma = lambda n: pltpu.SemaphoreType.DMA((n,))
    grad, img = pl.pallas_call(
        functools.partial(render_kernel, 2.0 / depth, float(depth), tuple(room)),
        out_shape=(pltpu.VMEM((ch, planes, rows, half), jnp.float32),
                   pltpu.VMEM((3, 8, rows), jnp.float32)),
        in_specs=[HBM] * 4,
        out_specs=(VM, VM),
        scratch_shapes=list(room.values()) + [
            dma(5), dma(10), dma(10),
            dma(2 * nz - 2), dma(2 * nz - 2), dma(2 * nz - 2), dma(2 * nz - 2),
            dma(2 * ng - 2), dma(2 * ng - 2), dma(2 * nz - 2), dma(2 * nz - 2),
            dma(ng), dma(ng), dma(11), dma(11),
        ],
        compiler_params=pltpu.CompilerParams(
            collective_id=0, has_side_effects=True, vmem_limit_bytes=58 * 1024 * 1024
        ),
    )(voxels, offsets, heading, cotangent)
    image = jnp.swapaxes(img, 1, 2)[None]
    return (image, grad)


def solution(mesh):
    n = mesh.devices.size
    shape = (2, 4, 2, 8, 2) if n == 256 else (2,) * 5
    finer = Mesh(mesh.devices.reshape(shape), AXES)
    return jax.shard_map(
        per_device,
        mesh=finer,
        in_specs=(
            P(None, SLAB, "tile", None),
            P("dir", "tile", None),
            P("dir", "tile", None),
            P("dir", None, "tile", None),
        ),
        out_specs=(P("dir", None, "tile", SLAB), P(None, SLAB, "tile", "dir")),
        check_vma=False,
    )
```

```python
import functools
from types import SimpleNamespace
from typing import NamedTuple

import jax
import jax.numpy as jnp
from jax import lax
from jax.experimental import pallas as pl
from jax.experimental.pallas import tpu as pltpu
from jax.sharding import Mesh
from jax.sharding import PartitionSpec as P

LEVELS = 8
SIDE = 128
AXES = ("dir", "sy", "sx", "sz", "tile")
SLAB = AXES[1:4]
MESH = pl.DeviceIdType.MESH
HBM = pl.BlockSpec(memory_space=pltpu.HBM)
VM = pl.BlockSpec(memory_space=pltpu.VMEM)


class Place(NamedTuple):
    dir: int
    sy: int
    sx: int
    sz: int
    tile: int


def places():
    return Place(*[lax.axis_index(a) for a in AXES])


def slab_index(me):
    _, _, sx, sz, _ = (lax.axis_size(a) for a in AXES)
    return (me.sy * sx + me.sx) * sz + me.sz


def at_slab(me, step):
    sy, sx, sz = (lax.axis_size(a) for a in SLAB)
    s = lax.rem(slab_index(me) + step + sy * sx * sz, sy * sx * sz)
    return me._replace(sy=s // (sx * sz), sx=(s // sz) % sx, sz=s % sz)


def greet(peers):
    barrier = pltpu.get_barrier_semaphore()
    for peer in peers:
        pl.semaphore_signal(barrier, inc=1, device_id=tuple(peer), device_id_type=MESH)
    return lambda: pl.semaphore_wait(barrier, len(peers))


def push(src, dst, send, recv, peer):
    return pltpu.make_async_remote_copy(
        src_ref=src, dst_ref=dst, send_sem=send, recv_sem=recv,
        device_id=tuple(peer), device_id_type=MESH,
    )


def shapes(ch, planes, rows, half, wide, nz, ng):
    lanes, m = 4 * rows, half // 8 // nz
    pairs = m // 2
    ext = planes + 2
    f32 = jnp.float32
    one = dict(
        grid=(ch, ext, rows, half), wing=(ch, ext, rows, wide),
        cut=(2, rows, wide), rcut=(2, rows, wide), brim=(ext, ch, half + wide),
        rbrim=(ext, ch, half + wide),
        shift=(8, ch, ext, rows, half),
        plane=(2, ch, ext, rows, half), tail=(2, ext, rows, half),
        sigma=(2, planes, rows, half), colour=(2, 3, planes, rows, half),
        through=(2, planes, rows, half), glow=(2, planes, rows, half),
        taps=(2, 9, rows, half), pair=(2, 7, rows, half), kept=(2, rows, half),
        codes=(2, rows, half), heading=(2, rows, half), pull=(2, 3, rows, half),
        ahead=(2, planes, rows, half), stack=(lanes, wide), tile=(wide, lanes),
        diff=(2, ch + 1, planes + 4, rows, half), out=(ch, ext, rows, half),
        lit=(2, 2, rows, half), seam=(2, 2, rows, SIDE),
        line=(ext, ch, half), pack=(SIDE, SIDE), turn=(SIDE, SIDE),
        fp=(ch, rows, half), fn=(ch, rows, half),
        rline=(planes, ch, half), zline=(2, ch, half), rin=(ch * planes, SIDE),
        rfar=(8, SIDE), rzin=(2, 8, SIDE), rzfar=(2, 8, SIDE),
        dl=(2, nz, pairs, 8, lanes), hd=(2, nz, pairs, 8, lanes), rdl=(2, nz, pairs, 8, lanes),
        im=(2, nz, m, 8, lanes), rim=(2, nz, m, 8, lanes), gm=(2, ng, pairs, 8, lanes),
        zreach=(2, nz, pairs, 8, lanes), zlater=(2, nz, pairs, 8, lanes),
        ret=(2, nz, pairs, 8, lanes), rb=(2, nz, pairs, 8, lanes),
        part=(2, m, 8, lanes), rpart=(ng, 8, lanes),
    )
    ints = dict(codes=0, heading=0)
    return {k: pltpu.VMEM(v, jnp.int32 if k in ints else f32) for k, v in one.items()}


def weights(b, g):
    level = LEVELS
    q = b.codes[g]
    frac = lambda raw: (raw.astype(jnp.float32) + 0.5) / level - 0.5
    fz, fy, fx = frac(q & 7), frac((q >> 3) & 7), frac(q >> 6)
    three = lambda f: (jnp.maximum(-f, 0.0), 1.0 - jnp.abs(f), jnp.maximum(f, 0.0))
    wy, wx = three(fy), three(fx)
    for i in range(3):
        for j in range(3):
            b.taps[g, 3 * i + j] = wy[i] * wx[j]
    ay, ax = jnp.abs(fy), jnp.abs(fx)
    for i, v in enumerate((fz, fy, fx, wy[1] * wx[1], wy[1] * ax, ay * wx[1], ay * ax)):
        b.pair[g, i] = v


def iota(shape, dim):
    return lax.broadcasted_iota(jnp.int32, shape, dim)


def lane_of(d, r):
    return jnp.where(d == 0, r[..., 0:1], r[..., r.shape[-1] - 1:])


def inner_edges(b, me, p):
    return lambda c: jnp.broadcast_to(lane_of(me.dir, b.wing[c, p]), b.wing.shape[2:])


def outer_edges(b, me, i):
    return lambda c: jnp.broadcast_to(b.rcut[i][:, c:c + 1], b.wing.shape[2:])


def cut_faces(b, me):
    ch, ext, rows, half = b.grid.shape
    wide = b.wing.shape[3]
    slot = iota((rows, wide), 1)
    for i, p in enumerate((ext - 2, 1)):
        acc = jnp.zeros((rows, wide), jnp.float32)
        for c in range(ch):
            acc = jnp.where(slot == c, inner_edges(b, me, p)(c), acc)
        b.cut[i] = acc

    def trim(p, carry):
        pick = lambda r: jnp.where(me.tile == 0, r[rows - 1:rows], r[0:1])
        for c in range(ch):
            b.brim[p, c:c + 1, :half] = pick(b.grid[c, p])
            b.brim[p, c:c + 1, half:] = pick(b.wing[c, p])
        return carry

    lax.fori_loop(1, ext - 1, trim, 0)


def sample_plane(b, me, p, gs, edges, keep):
    ch, _, rows, half = b.grid.shape
    tw = half // 2
    d, t = me.dir, me.tile
    row, lane = iota((rows, tw), 0), iota((rows, tw), 1)
    right = (d == 0).astype(jnp.float32)
    left = 1.0 - right
    under = (t == 0).astype(jnp.float32)
    over = 1.0 - under
    for c in range(ch):
        edge, line = edges(c), b.rbrim[p, c:c + 1, :]
        corner = jnp.broadcast_to(lane_of(d, line[:, half:]), (1, tw))
        m = [b.grid[c, p, :, x * tw:(x + 1) * tw] for x in range(2)] + [edge]
        far = [line[:, :tw], line[:, tw:half], corner]
        up = [jnp.where(row == 0, f * over, pltpu.roll(a, 1, 0)) for a, f in zip(m, far)]
        dn = [jnp.where(row == rows - 1, f * under, pltpu.roll(a, rows - 1, 0))
              for a, f in zip(m, far)]
        spread = []
        for a in (up, m, dn):
            r = [pltpu.roll(a[x], 1, 1) for x in range(2)]
            l = [pltpu.roll(a[x], tw - 1, 1) for x in range(2)]
            lo = [jnp.where(lane == 0, a[2] * left, r[0]), jnp.where(lane == 0, r[0], r[1])]
            hi = [jnp.where(lane == tw - 1, l[1], l[0]),
                  jnp.where(lane == tw - 1, a[2] * right, l[1])]
            spread.append((lo, a[:2], hi))
        for n, v in enumerate([up, dn] + [q[0] for q in spread] + [q[2] for q in spread]):
            b.shift[n, c, p, :, :tw] = v[0]
            b.shift[n, c, p, :, tw:] = v[1]
        for x in range(2):
            at = slice(x * tw, (x + 1) * tw)
            for g in gs:
                fy, fx = b.pair[g, 1, :, at], b.pair[g, 2, :, at]
                w00, w01 = b.pair[g, 3, :, at], b.pair[g, 4, :, at]
                w10, w11 = b.pair[g, 5, :, at], b.pair[g, 6, :, at]
                side = lambda s: jnp.where(fx > 0, s[2][x], s[0][x])
                down = fy > 0
                v = (w00 * m[x] + w01 * side(spread[1])
                     + w10 * jnp.where(down, dn[x], up[x])
                     + w11 * jnp.where(down, side(spread[2]), side(spread[0])))
                b.plane[g, c, p, :, at] = v if keep is None else v * keep


def sample_again(b, p, g, keep):
    right, down = b.pair[g, 2] > 0, b.pair[g, 1] > 0
    for c in range(b.grid.shape[0]):
        up, dn, *sides = [b.shift[n, c, p] for n in range(8)]
        side = [jnp.where(right, sides[n + 3], sides[n]) for n in range(3)]
        v = (b.pair[g, 3] * b.grid[c, p] + b.pair[g, 4] * side[1]
             + b.pair[g, 5] * jnp.where(down, dn, up)
             + b.pair[g, 6] * jnp.where(down, side[2], side[0]))
        b.plane[g, c, p] = v if keep is None else v * keep


def shade_planes(b, scale, g):
    _, ch, ext, rows, half = b.plane.shape
    fz = b.pair[g, 0]
    az = jnp.abs(fz)

    def step(k, acc):
        v = []
        for c in range(ch):
            far = jnp.where(fz > 0, b.plane[g, c, k + 2], b.plane[g, c, k])
            v.append((1.0 - az) * b.plane[g, c, k + 1] + az * far)
        sg = (jnp.maximum(v[0], 0.0) + jnp.log(1.0 + jnp.exp(-jnp.abs(v[0])))) * scale
        b.sigma[g, k] = sg
        b.diff[g, ch, k + 2] = (0.5 + 0.5 * jnp.tanh(0.5 * v[0])) * scale
        for c in range(3):
            b.colour[g, c, k] = 0.5 + 0.5 * jnp.tanh(0.5 * v[c + 1])
        b.ahead[g, k] = acc
        return acc + sg

    return lax.fori_loop(0, ext - 2, step, jnp.zeros((rows, half), jnp.float32))


def local_light(b, total, g):
    _, planes, rows, half = b.sigma.shape
    forward = b.heading[g] == 0

    def step(k, acc):
        sg, ah = b.sigma[g, k], b.ahead[g, k]
        front = jnp.where(forward, ah, total - ah - sg)
        th = jnp.exp(-front)
        gl = th * (1.0 - jnp.exp(-sg))
        b.through[g, k] = th
        b.glow[g, k] = gl
        return tuple(acc[c] + gl * b.colour[g, c, k] for c in range(3))

    zero = jnp.zeros((rows, half), jnp.float32)
    return lax.fori_loop(0, planes, step, (zero,) * 3)


def tiles_out(b, nz, put):
    turned = b.stack[...].T
    for i in range(turned.shape[0] // 8):
        put(i % nz, i // nz, turned[8 * i:8 * i + 8])


def prepare(b, g):
    _, planes, rows, half = b.sigma.shape
    ch = b.grid.shape[0]
    zero = jnp.zeros((rows, half), jnp.float32)
    forward = b.heading[g] == 0
    whole = b.kept[g]
    for c in range(ch + 1):
        for k in (0, 1, planes + 2, planes + 3):
            b.diff[g, c, k] = zero

    def step(k, before):
        pull = [b.pull[g, c] for c in range(3)]
        col = [b.colour[g, c, k] for c in range(3)]
        shade = pull[0] * col[0] + pull[1] * col[1] + pull[2] * col[2]
        th, gl = b.through[g, k], b.glow[g, k]
        share = gl * shade
        later = jnp.where(forward, whole - before - share, before)
        b.diff[g, 0, k + 2] = ((th - gl) * shade - later) * b.diff[g, ch, k + 2]
        for c in range(3):
            b.diff[g, c + 1, k + 2] = pull[c] * gl * (col[c] * (1.0 - col[c]))
        return before + share

    lax.fori_loop(0, planes, step, zero)

    def mix(p, carry):
        fz = b.pair[g, 0]
        mid, up, down = 1.0 - jnp.abs(fz), jnp.maximum(fz, 0.0), jnp.maximum(-fz, 0.0)
        for c in range(ch + 1):
            v = mid * b.diff[g, c, p + 1] + up * b.diff[g, c, p] + down * b.diff[g, c, p + 2]
            if c < ch:
                b.plane[g, c, p] = v
            else:
                b.tail[g, p] = v
        return carry

    lax.fori_loop(0, planes + 2, mix, 0)


def seam_slot(c, p, ch, planes):
    if p == 0:
        return ch * planes + c
    return ch * planes + ch + c if p == planes + 1 else c * planes + p - 1


def seam_of(d, r):
    return jnp.where(d == 0, r[..., r.shape[-1] - 1:], r[..., 0:1])


def gather_seam(b, me, g):
    _, ch, ext, rows, half = b.plane.shape
    slot = iota((rows, SIDE), 1)
    wide = lambda v: jnp.broadcast_to(seam_of(me.dir, v), (rows, SIDE))
    a = jnp.zeros((rows, SIDE), jnp.float32)
    r = a
    for p in range(ext):
        for c in range(ch):
            a = jnp.where(slot == seam_slot(c, p, ch, ext - 2), wide(b.plane[g, c, p]), a)
        r = jnp.where(slot == seam_slot(0, p, ch, ext - 2), wide(b.tail[g, p]), r)
    b.seam[g, 0] = a
    b.seam[g, 1] = r


def spill_seam(b, me):
    _, ch, ext, rows, half = b.plane.shape
    d, t = me.dir, me.tile
    row = iota((rows, SIDE), 0)
    wide = lambda v: jnp.broadcast_to(seam_of(d, v), (rows, SIDE))
    cols = [wide(b.lit[g, 0]) * b.seam[g, 0] - wide(b.lit[g, 1]) * b.seam[g, 1] for g in range(2)]
    bands = []
    for i in range(3):
        w = [jnp.where(d == 0, b.taps[g, 3 * i + 2, :, half - 1:half], b.taps[g, 3 * i, :, 0:1])
             for g in range(2)]
        bands.append(sum(jnp.broadcast_to(w[g], (rows, SIDE)) * cols[g] for g in range(2)))
    up = pltpu.roll(bands[0], rows - 1, 0)
    dn = pltpu.roll(bands[2], 1, 0)
    b.pack[:rows] = (bands[1] + jnp.where(row == rows - 1, 0.0, up) + jnp.where(row == 0, 0.0, dn))
    b.pack[rows:rows + 1] = jnp.where(t == 0, dn[0:1], up[rows - 1:rows])
    b.turn[...] = b.pack[...].T


def spill_plane(b, me, p):
    ch, ext, rows, half = b.out.shape
    tw = half // 2
    t = me.tile
    row, lane = iota((rows, tw), 0), iota((rows, tw), 1)
    for c in range(ch):
        cols = []
        for g in range(2):
            v = b.lit[g, 0] * b.plane[g, c, p]
            cols.append(v if c else v - b.lit[g, 1] * b.tail[g, p])
        bands = []
        for i in range(3):
            u = []
            for j in range(3):
                full = b.taps[0, 3 * i + j] * cols[0] + b.taps[1, 3 * i + j] * cols[1]
                u.append([full[:, :tw], full[:, tw:]])
            l = [pltpu.roll(a, tw - 1, 1) for a in u[0]]
            r = [pltpu.roll(a, 1, 1) for a in u[2]]
            x0 = u[1][0] + jnp.where(lane == tw - 1, l[1], l[0]) + jnp.where(lane == 0, 0.0, r[0])
            x1 = u[1][1] + jnp.where(lane == tw - 1, 0.0, l[1]) + jnp.where(lane == 0, r[0], r[1])
            bands.append([x0, x1])
        for x in range(2):
            at = slice(x * tw, (x + 1) * tw)
            up = pltpu.roll(bands[0][x], rows - 1, 0)
            dn = pltpu.roll(bands[2][x], 1, 0)
            b.out[c, p, :, at] = (bands[1][x] + jnp.where(row == rows - 1, 0.0, up)
                                  + jnp.where(row == 0, 0.0, dn))
            b.line[p, c:c + 1, at] = jnp.where(t == 0, dn[0:1], up[rows - 1:rows])


def gather_spill(b, me, has_prev, has_next, dest):
    ch, ext, rows, half = b.out.shape
    planes = ext - 2
    tw = half // 2
    d, t = me.dir, me.tile
    touch = (1 - t) * (rows - 1)
    seam = (1 - d) * (half - 1)
    row = iota((rows, tw), 0)
    lane = iota((rows, tw), 1)
    spot = iota((1, SIDE), 1)
    b.turn[:ch * planes] = b.rin[...]
    for c in range(ch):
        for k, i, r, has in ((0, 0, ch + c, has_prev), (planes - 1, 1, c, has_next)):
            far = jnp.broadcast_to(b.rzfar[i, r:r + 1, rows:rows + 1], (1, SIDE))
            add = jnp.where(spot < rows, b.rzin[i, r:r + 1], 0.0) + jnp.where(spot == touch, far, 0.0)
            j = c * planes + k
            b.turn[j:j + 1] = b.turn[j:j + 1] + add * has
    col = b.turn[...].T[:rows]
    col = col + jnp.where(iota((rows, SIDE), 0) == touch, jnp.broadcast_to(b.rfar[0:1], (rows, SIDE)), 0.0)
    for c in range(ch):
        for k in range(planes):
            pos = c * planes + k
            extra = b.rline[k, c:c + 1]
            v = b.out[c, k + 1]
            if k == 0:
                extra = extra + b.zline[0, c:c + 1] * has_prev
            if k == planes - 1:
                extra = extra + b.zline[1, c:c + 1] * has_next
            bar = jnp.broadcast_to(col[:, pos:pos + 1], (rows, tw))
            for x in range(2):
                at = slice(x * tw, (x + 1) * tw)
                y = v[:, at] + jnp.where(row == touch, jnp.broadcast_to(extra[:, at], (rows, tw)), 0.0)
                y = y + jnp.where(lane + x * tw == seam, bar, 0.0)
                dest[c, k, :, at] = y


def render_kernel(scale, depth, names, vox, codes, head, cot, grad, img, *scratch):
    b = SimpleNamespace(**dict(zip(names, scratch)))
    sems = scratch[len(names):]
    (lsem, hs, hr, s1, r1, s2, r2, s3, r3, s4, r4, s5, r5, ss, sr) = sems
    me = places()
    nsy, nsx, nz = (lax.axis_size(a) for a in SLAB)
    ng = nsy * nsx
    blocks = ng // 2
    d, t, z = me.dir, me.tile, me.sz
    gi = me.sy * nsx + me.sx
    s = slab_index(me)
    prev, nxt = at_slab(me, -1), at_slab(me, 1)
    flip = lambda p: p._replace(tile=1 - p.tile)
    over = lambda p: p._replace(dir=1 - p.dir)
    near = [prev, me, nxt]
    mate = me._replace(dir=1 - d, sx=nsx - 1 - me.sx)
    ch, ext, rows, half = b.grid.shape
    planes = ext - 2
    wide = b.wing.shape[-1]
    has_prev = (s > 0).astype(jnp.float32)
    has_next = (s < nsy * nsx * nz - 1).astype(jnp.float32)

    mine = pl.ds(pl.multiple_of(d * half, half), half)
    theirs = pl.ds(pl.multiple_of((1 - d) * half, half), half)
    beside = pl.ds(pl.multiple_of(half - d * wide, wide), wide)
    loads = [
        (vox.at[:, :, :, mine], b.grid.at[:, 1:planes + 1]),
        (vox.at[:, :, :, beside], b.wing.at[:, 1:planes + 1]),
        (codes.at[0, :, mine], b.codes.at[0]),
        (head.at[0, :, mine], b.heading.at[0]),
        (cot.at[0, :, :, mine], b.pull.at[0]),
    ]
    loads = [pltpu.make_async_copy(a, c, lsem.at[i]) for i, (a, c) in enumerate(loads)]
    for c in loads:
        c.start()

    far_first = sorted(range(1, nz), key=lambda i: -min(i, nz - i))
    zpeer = [me._replace(sz=lax.rem(z + i, nz)) for i in far_first]
    gpeer, across = [], []
    for i in range(ng):
        g = lax.rem(gi + i, ng)
        p = me._replace(sy=g // nsx, sx=g % nsx)
        across.append(over(p))
        if i:
            gpeer.append(p)
    ready = greet([prev, nxt] + [flip(p) for p in near] + [over(prev), over(nxt)]
          + [over(flip(p)) for p in near] + zpeer + gpeer + across)

    for c in loads[:2]:
        c.wait()
    cut_faces(b, me)
    for c in loads[2:]:
        c.wait()
    weights(b, 0)
    ready()
    rays = [
        (codes.at[0, :, theirs], b.codes.at[1], mate),
        (head.at[0, :, theirs], b.heading.at[1], mate),
        (cot.at[0, :, :, theirs], b.pull.at[1], mate),
    ]
    rays = [push(x, y, hs.at[i], hr.at[i], p) for i, (x, y, p) in enumerate(rays)]
    for c in rays:
        c.start()
    inner = pl.ds(1, planes)
    beyond = [
        (b.brim.at[inner], b.rbrim.at[inner], flip(me)),
        (b.cut.at[0], b.rcut.at[0], nxt),
        (b.cut.at[1], b.rcut.at[1], prev),
        (b.brim.at[planes], b.rbrim.at[0], flip(nxt)),
        (b.brim.at[1], b.rbrim.at[ext - 1], flip(prev)),
        (b.grid.at[:, planes], b.grid.at[:, 0], nxt),
        (b.grid.at[:, 1], b.grid.at[:, ext - 1], prev),
    ]
    beyond = [push(x, y, hs.at[3 + i], hr.at[3 + i], p) for i, (x, y, p) in enumerate(beyond)]
    for c in beyond:
        c.start()
    beyond[0].wait()
    tw = half // 2
    pairs = blocks // 2
    first, late = [], []

    def rows_in(parts):
        for n, v in enumerate(parts):
            b.stack[n * rows:(n + 1) * rows] = v

    def chain(g):
        def inside(p, carry):
            if g == 0:
                sample_plane(b, me, p, (g,), inner_edges(b, me, p), None)
            else:
                sample_again(b, p, g, None)
            return carry

        lax.fori_loop(1, planes + 1, inside, 0)
        sides = [slice(0, tw), slice(tw, half)]
        if g == 0:
            head_f = b.heading[g].astype(jnp.float32)
            rows_in([head_f[:, x] for x in sides for _ in range(2)])

            def put_hd(j, m, v):
                b.hd[g, j, m] = v

            tiles_out(b, nz, put_hd)
            for c in beyond[1:]:
                c.wait()

        def ends(i, carry):
            keep = jnp.where(i == 0, has_prev, has_next)
            if g == 0:
                sample_plane(b, me, i * (ext - 1), (g,), outer_edges(b, me, i), keep)
            else:
                sample_again(b, i * (ext - 1), g, keep)
            return carry

        lax.fori_loop(0, 2, ends, 0)
        total = shade_planes(b, scale, g)
        if g == 1:
            for c in rays[1:]:
                c.wait()
        for c in range(3):
            b.pull[g, c] = b.pull[g, c] * depth
        images = local_light(b, total, g)
        kept = sum(b.pull[g, c] * images[c] for c in range(3))
        b.kept[g] = kept
        sides = [slice(0, tw), slice(tw, half)]
        rows_in([v[:, x] for x in sides for v in (total, kept)])

        def put_dl(j, m, v):
            b.dl[g, j, m] = v

        tiles_out(b, nz, put_dl)
        first.append([push(b.dl.at[g, p.sz], b.rdl.at[g, z], s1.at[g * (nz - 1) + i],
                           r1.at[g * (nz - 1) + i], p) for i, p in enumerate(zpeer)])
        for c in first[g]:
            c.start()
        if g == 1:
            head_f = b.heading[g].astype(jnp.float32)
            rows_in([head_f[:, x] for x in sides for _ in range(2)])

            def put_hd(j, m, v):
                b.hd[g, j, m] = v

            tiles_out(b, nz, put_hd)
        for n, x in enumerate(sides):
            rows_in([v[:, x] for v in images])

            def put_im(j, m, v):
                b.im[g, j, n * pairs + m] = v

            tiles_out(b, nz, put_im)
        late.append([push(b.im.at[g, p.sz], b.rim.at[g, z], s2.at[g * (nz - 1) + i],
                          r2.at[g * (nz - 1) + i], p) for i, p in enumerate(zpeer)])
        if g == 0:
            for c in late[g]:
                c.start()

    chain(0)
    rays[0].wait()
    weights(b, 1)
    chain(1)
    lanes = b.dl.shape[-1]
    spot = iota(b.dl.shape[2:], 2)
    is_d = (spot // rows) % 2 == 0
    roll = lambda a, n: pltpu.roll(a, n % lanes, 2)

    def directed(parts, ahead):
        lows, low = [], jnp.zeros_like(parts[0])
        for p in parts:
            lows.append(low)
            low = low + p
        highs, high = [], jnp.zeros_like(parts[0])
        for p in reversed(parts):
            highs.append(high)
            high = high + p
        highs = highs[::-1]
        before = [jnp.where(ahead, x, y) for x, y in zip(lows, highs)]
        after = [jnp.where(ahead, y, x) for x, y in zip(lows, highs)]
        return before, after, low

    def compose(g):
        b.rdl[g, z] = b.dl[g, z]
        for c in first[g]:
            c.wait()
        ahead = b.hd[g, z] == 0
        tiles = [b.rdl[g, i] for i in range(nz)]
        before, _, dsum = directed(tiles, ahead)
        reach = [jnp.exp(-x) for x in before]
        _, later, lsum = directed([roll(r, rows) * x for r, x in zip(reach, tiles)], ahead)
        b.gm[g, gi] = jnp.where(is_d, dsum, lsum)
        copies = [push(b.gm.at[g, gi], b.gm.at[g, gi], s3.at[g * (ng - 1) + i],
                       r3.at[g * (ng - 1) + i], p) for i, p in enumerate(gpeer)]
        for c in copies:
            c.start()
        for i in range(nz):
            b.zreach[g, i] = reach[i]
            b.zlater[g, i] = later[i]
        return copies

    def conclude(g, copies):
        for c in copies:
            c.wait()
        ahead = b.hd[g, z] == 0
        groups = [b.gm[g, i] for i in range(ng)]
        before, _, _ = directed(groups, ahead)
        reach = [jnp.exp(-x) for x in before]
        _, after, _ = directed([roll(r, rows) * x for r, x in zip(reach, groups)], ahead)
        to_me = jnp.zeros_like(reach[0])
        rest = jnp.zeros_like(reach[0])
        for i in range(ng):
            to_me = jnp.where(gi == i, reach[i], to_me)
            rest = jnp.where(gi == i, after[i], rest)
        to_me_l = roll(to_me, rows)
        for i in range(nz):
            b.ret[g, i] = jnp.where(is_d, to_me * b.zreach[g, i],
                                    rest + to_me_l * b.zlater[g, i])
        copies = [push(b.ret.at[g, p.sz], b.rb.at[g, z], s4.at[g * (nz - 1) + i],
                       r4.at[g * (nz - 1) + i], p) for i, p in enumerate(zpeer)]
        for c in copies:
            c.start()
        b.rb[g, z] = b.ret[g, z]
        return copies

    second0 = compose(0)
    prepare(b, 0)
    gather_seam(b, me, 0)
    b.rim[0, z] = b.im[0, z]
    second1 = compose(1)
    for c in late[1]:
        c.start()
    back0 = conclude(0, second0)
    prepare(b, 1)
    back1 = conclude(1, second1)
    b.rim[1, z] = b.im[1, z]
    gather_seam(b, me, 1)
    for g, back in enumerate((back0, back1)):
        for c in back:
            c.wait()
        for i in range(tw // 8):
            b.tile[8 * i:8 * i + 8] = b.rb[g, i % nz, i // nz]
        turned = b.tile[...].T
        for n in range(4):
            x, q = n // 2, n % 2
            b.lit[g, q, :, x * tw:(x + 1) * tw] = turned[n * rows:(n + 1) * rows]
    faces = []
    for i, (p, to, r, zl) in enumerate(((ext - 1, nxt, b.fp, 0), (0, prev, b.fn, 1))):
        spill_plane(b, me, p)
        faces += [push(b.out.at[:, p], r, ss.at[6 + 2 * i], sr.at[6 + 2 * i], to),
                  push(b.line.at[p], b.zline.at[zl], ss.at[7 + 2 * i], sr.at[7 + 2 * i], flip(to))]
        for c in faces[2 * i:]:
            c.start()
    spill_seam(b, me)
    small = b.turn.at[ch * planes:ch * planes + 8]
    spill = [
        (b.turn.at[0:ch * planes], b.rin, over(me)),
        (b.pack.at[rows:rows + 8], b.rfar, over(flip(me))),
    ]
    for i, p in enumerate((nxt, prev)):
        spill.append((small, b.rzin.at[i], over(p)))
        spill.append((small, b.rzfar.at[i], over(flip(p))))
    spill = [push(x, y, ss.at[i], sr.at[i], p) for i, (x, y, p) in enumerate(spill)]
    for c in spill:
        c.start()

    for c in late[0] + late[1]:
        c.wait()
    quarter = spot // rows
    for g in range(2):
        for x in range(2):
            total = jnp.zeros(b.dl.shape[2:], jnp.float32)
            for i in range(nz):
                src = b.ret[g, i]
                wash = roll(src, -2 * x * rows)
                wash = jnp.where(quarter == 1, roll(src, (1 - 2 * x) * rows), wash)
                wash = jnp.where(quarter == 2, roll(src, (2 - 2 * x) * rows), wash)
                total = total + wash * b.rim[g, i, x * pairs:(x + 1) * pairs]
            b.part[g, x * pairs:(x + 1) * pairs] = total
    half_of_me = gi // blocks
    out = []
    for g in range(2):
        for m in range(blocks):
            q = blocks * d + m
            peer = me._replace(dir=d if g == 0 else 1 - d, sy=q // nsx, sx=q % nsx)
            out.append(push(b.part.at[g, m], b.rpart.at[gi],
                            s5.at[g * blocks + m], r5.at[gi], peer))
    for g in range(2):
        for m in range(blocks):
            copy = out[g * blocks + m]
            if g == 0:
                itself = gi == blocks * d + m

                @pl.when(itself)
                def _():
                    b.rpart[gi] = b.part[0, m]

                @pl.when(jnp.logical_not(itself))
                def _():
                    copy.start()
            else:
                copy.start()

    def spread(p, carry):
        spill_plane(b, me, p)
        return carry

    lax.fori_loop(1, planes + 1, spread, 0)
    lines = push(b.line.at[inner], b.rline, ss.at[10], sr.at[10], flip(me))
    lines.start()
    spill = spill + [faces[1], faces[3], lines]

    for g in range(2):
        for m in range(blocks):
            copy = out[g * blocks + m]
            if g == 0:
                @pl.when(gi != blocks * d + m)
                def _():
                    copy.wait_send()
            else:
                copy.wait_send()
    for i in range(ng):
        arrive = push(b.part.at[0, 0], b.rpart.at[i], s5.at[0], r5.at[i], over(me))

        @pl.when(jnp.logical_or(half_of_me != d, gi != i))
        def _():
            arrive.wait_recv()
    total = b.rpart[0]
    for i in range(1, ng):
        total = total + b.rpart[i]
    for c in range(3):
        img[c] = total[:, c * rows:(c + 1) * rows]
    for c in spill:
        c.wait()
    gather_spill(b, me, has_prev, has_next, grad)
    for c in (faces[0], faces[2]):
        c.wait()
    for c in range(ch):
        grad[c, 0] = grad[c, 0] + b.fp[c] * has_prev
        grad[c, planes - 1] = grad[c, planes - 1] + b.fn[c] * has_next


def per_device(voxels, offsets, heading, cotangent):
    ch, planes, rows, total = voxels.shape
    nsy, nsx, nz = (lax.axis_size(a) for a in SLAB)
    ng = nsy * nsx
    depth = planes * nz * ng
    half = total // 2
    wide = half // 2
    room = shapes(ch, planes, rows, half, wide, nz, ng)
    dma = lambda n: pltpu.SemaphoreType.DMA((n,))
    grad, img = pl.pallas_call(
        functools.partial(render_kernel, 2.0 / depth, float(depth), tuple(room)),
        out_shape=(pltpu.VMEM((ch, planes, rows, half), jnp.float32),
                   pltpu.VMEM((3, 8, rows), jnp.float32)),
        in_specs=[HBM] * 4,
        out_specs=(VM, VM),
        scratch_shapes=list(room.values()) + [
            dma(5), dma(10), dma(10),
            dma(2 * nz - 2), dma(2 * nz - 2), dma(2 * nz - 2), dma(2 * nz - 2),
            dma(2 * ng - 2), dma(2 * ng - 2), dma(2 * nz - 2), dma(2 * nz - 2),
            dma(ng), dma(ng), dma(11), dma(11),
        ],
        compiler_params=pltpu.CompilerParams(
            collective_id=0, has_side_effects=True, vmem_limit_bytes=58 * 1024 * 1024
        ),
    )(voxels, offsets, heading, cotangent)
    image = jnp.swapaxes(img, 1, 2)[None]
    return (image, grad)


def solution(mesh):
    n = mesh.devices.size
    shape = (2, 4, 2, 8, 2) if n == 256 else (2,) * 5
    finer = Mesh(mesh.devices.reshape(shape), AXES)
    return jax.shard_map(
        per_device,
        mesh=finer,
        in_specs=(
            P(None, SLAB, "tile", None),
            P("dir", "tile", None),
            P("dir", "tile", None),
            P("dir", None, "tile", None),
        ),
        out_specs=(P("dir", None, "tile", SLAB), P(None, SLAB, "tile", "dir")),
        check_vma=False,
    )
```
